256 devices in a mesh: gz: 32 (over y, z), gy: 4 (over x), gx: 2 (over core).
Axes of the slice: x: 4, y: 4, z: 8, core: 2. Of those that a mesh axis runs over, the one named last changes fastest.
Arguments:
- right_side: float32 [256, 64, 256], P('gz', 'gy', 'gx'), may hold values from -128 to 128
- diagonal: float32 [256, 64, 256], P('gz', 'gy', 'gx'), may hold values from 0.05 to 1
Outputs:
- solution_field: float32 [256, 64, 256], P('gz', 'gy', 'gx')
- residual: float32 [256, 64, 256], P('gz', 'gy', 'gx')
The draws below stay inside these ranges and needn't reach their ends.
All inputs are finite; a program needn't handle non-finite values.
Results may differ from the reference program's by a relative error of at most 0.03.
Values sent between devices are 32-bit elements.
A program may use at most 64 MiB of HBM per device.

```python
import jax
import jax.numpy as jnp
import numpy as np
from jax import lax

S = 6
OUTER = 5
NZ = 256
NY = 64
NX = 256


def shard_levels(own_key, dims, pieces, low, largest):
    factor_of = 1.0
    for position, blocks in pieces:
        steps = jax.random.uniform(jax.random.fold_in(jax.random.fold_in(own_key, 6), position), (blocks,), jnp.float32, low / len(pieces), largest / len(pieces))
        factor_of = factor_of * jnp.repeat(jnp.exp(steps), dims[position] // blocks).reshape((-1,) + (1,) * (len(dims) - 1 - position))
    return factor_of


def gaussian(own_key, extent, spread, most, split=(), kind=jnp.bfloat16):
    result = spread * jax.random.normal(own_key, extent, jnp.float32)
    if split:
        result = result * shard_levels(own_key, extent, split, -0.22, 0.18)
    return jnp.clip(result, -most, most).astype(kind)


def setup_inputs(seed: int = 0) -> dict:
    key_list = jax.random.split(jax.random.key(seed), 3)
    return {
        "right_side": gaussian(key_list[0], (NZ, NY, NX), 24.0, 128.0, ((0, 32), (1, 4), (2, 2)), jnp.float32),
        "diagonal": jnp.clip(0.05 + 0.95 * jax.random.uniform(key_list[1], (NZ, NY, NX), jnp.float32) ** shard_levels(key_list[1], (NZ, NY, NX), ((0, 32), (1, 4), (2, 2)), -0.2, 0.2), 0.05, 1.0),
    }


center_shift = 19.0
half_width = 19.0


def apply_operator(padded, diagonal):
    extent_z = padded.shape[-3] - 2
    extent_y = padded.shape[-2] - 2
    extent_x = padded.shape[-1] - 2
    running = jnp.zeros(padded[..., 1:-1, 1:-1, 1:-1].shape, jnp.float32)
    for along_z in range(3):
        for along_y in range(3):
            for along_x in range(3):
                if along_z == 1 and along_y == 1 and along_x == 1:
                    continue
                running = running + padded[..., along_z:along_z + extent_z, along_y:along_y + extent_y, along_x:along_x + extent_x]
    return (26.0 + diagonal) * padded[..., 1:-1, 1:-1, 1:-1] - running


def chebyshev_next(images, current, previous):
    scaled = (images - center_shift * current) / half_width
    if previous is None:
        return scaled
    return 2.0 * scaled - previous


def basis_change():
    columns = 2 * S + 1
    matrix = np.zeros((columns, columns), np.float32)
    for offset, length in ((0, S), (S + 1, S - 1)):
        for degree in range(length):
            matrix[offset + degree, offset + degree] = center_shift
            if degree == 0:
                matrix[offset + 1, offset] = half_width
            else:
                matrix[offset + degree + 1, offset + degree] = 0.5 * half_width
                matrix[offset + degree - 1, offset + degree] = 0.5 * half_width
    return matrix


def coefficients(gram_matrix):
    columns = 2 * S + 1
    change = jnp.asarray(basis_change(), dtype=jnp.float32)
    identity = jnp.eye(columns, dtype=jnp.float32)
    dir_coeff = identity[0]
    res_coeff = identity[S + 1]
    sol_coeff = jnp.zeros((columns,), jnp.float32)
    for degree in range(S):
        moved = jnp.dot(change, dir_coeff, precision=lax.Precision.HIGHEST)
        norm_now = jnp.dot(res_coeff, jnp.dot(gram_matrix, res_coeff, precision=lax.Precision.HIGHEST), precision=lax.Precision.HIGHEST)
        curvature = jnp.dot(dir_coeff, jnp.dot(gram_matrix, moved, precision=lax.Precision.HIGHEST), precision=lax.Precision.HIGHEST)
        step_len = norm_now / curvature
        sol_coeff = sol_coeff + step_len * dir_coeff
        res_next = res_coeff - step_len * moved
        norm_next = jnp.dot(res_next, jnp.dot(gram_matrix, res_next, precision=lax.Precision.HIGHEST), precision=lax.Precision.HIGHEST)
        dir_coeff = res_next + (norm_next / norm_now) * dir_coeff
        res_coeff = res_next
    return sol_coeff, res_coeff, dir_coeff


def combine(coeff, basis_set):
    return jnp.tensordot(coeff, basis_set, axes=1, precision=lax.Precision.HIGHEST)


def reference(right_side, diagonal):
    solution = jnp.zeros(right_side.shape, jnp.float32)
    residual = right_side
    direction = right_side
    for outer_step in range(OUTER):
        p_fields = [direction]
        for degree in range(S):
            images = apply_operator(jnp.pad(p_fields[-1], 1), diagonal)
            p_fields.append(chebyshev_next(images, p_fields[-1], p_fields[-2] if degree else None))
        r_fields = [residual]
        for degree in range(S - 1):
            images = apply_operator(jnp.pad(r_fields[-1], 1), diagonal)
            r_fields.append(chebyshev_next(images, r_fields[-1], r_fields[-2] if degree else None))
        basis_set = jnp.stack(p_fields + r_fields)
        flattened = basis_set.reshape(basis_set.shape[0], -1)
        gram_matrix = jnp.dot(flattened, flattened.T, precision=lax.Precision.HIGHEST)
        sol_coeff, res_coeff, dir_coeff = coefficients(gram_matrix)
        solution = solution + combine(sol_coeff, basis_set)
        residual = combine(res_coeff, basis_set)
        direction = combine(dir_coeff, basis_set)
    return solution, residual
```

```python
import functools

import jax
import jax.numpy as jnp
import numpy as np
from jax import lax
from jax.experimental import pallas as pl
from jax.experimental.pallas import tpu as pltpu
from jax.sharding import PartitionSpec as P

S = 6
OUTER = 5
MESH = pl.DeviceIdType.MESH

CENTER = 19.0
HALF = 19.0

BZ = 8
NZE = BZ + 2 * S
ROWS = 40
LO, MID, HI = 8, 16, 24

NPP, NPR, NRR = 2 * S + 1, 2 * S, 2 * S - 1


def weights():
    columns = 2 * S + 1
    total = NPP + NPR + NRR

    def moment(offset, m):
        v = np.zeros(total)
        if m < 2:
            v[offset + m] = 1.0
        else:
            v[offset + m] = 2.0
            v[offset + m % 2] -= 1.0
        return v

    gram = np.zeros((columns, columns, total))
    for i in range(columns):
        for j in range(columns):
            di, dj = (i if i <= S else i - S - 1), (j if j <= S else j - S - 1)
            kinds = (i > S) + (j > S)
            offset = (0, NPP, NPP + NPR)[kinds]
            gram[i, j] = (moment(offset, di + dj) + moment(offset, abs(di - dj))) / 2
    change = np.zeros((columns, columns))
    for offset, length in ((0, S), (S + 1, S - 1)):
        for degree in range(length):
            change[offset + degree, offset + degree] = CENTER
            if degree == 0:
                change[offset + 1, offset] = HALF
            else:
                change[offset + degree + 1, offset + degree] = 0.5 * HALF
                change[offset + degree - 1, offset + degree] = 0.5 * HALF
    moved = np.einsum("ikm,kj->ijm", gram, change)
    out = np.zeros((2, columns, 2, 8, 128), np.float32)
    for which, table in enumerate((gram, moved)):
        for j in range(columns):
            for i in range(columns):
                half, row = (0, i) if i <= S else (1, i - S - 1)
                out[which, j, half, row, :total] = table[i, j]
    return out


def kernel(
    rhs_ref, diag_ref, w_ref, sol_ref, res_ref,
    F, PV, RV, C, M, V0, X, land, S1, S2,
    zs_sem, zr_sem, ys_sem, yr_sem, fs_sem, fr_sem, io_s, io_r, g1_s, g1_r, g2_s, g2_r,
):
    gz = lax.axis_index("gz")
    gy = lax.axis_index("gy")
    gx = lax.axis_index("gx")
    nz = lax.axis_size("gz")
    ny = lax.axis_size("gy")
    yv = 2 * gy + gx
    nyv = 2 * ny
    sib = 1 - gx
    nzp = 8
    py = gz // nzp
    pz = gz % nzp

    own_rows = pl.ds(MID, 8)
    own_z = pl.ds(S, BZ)

    swaps = []
    for f, ref in enumerate((rhs_ref, diag_ref)):
        cp = pltpu.make_async_remote_copy(
            src_ref=ref.at[:, pl.ds(pl.multiple_of(8 * sib, 8), 8), :],
            dst_ref=F.at[f, gx, own_z, own_rows, :],
            send_sem=io_s.at[f], recv_sem=io_r.at[f],
            device_id=(gz, gy, sib), device_id_type=MESH,
        )
        cp.start()
        swaps.append(cp)
        F[f, gx, S:S + BZ, MID:MID + 8, :] = ref[:, pl.ds(pl.multiple_of(8 * gx, 8), 8), :]

    @pl.when(gz == 0)
    def _():
        F[:, :, 0:S, :, :] = jnp.zeros((2, 2, S, ROWS, 128), jnp.float32)

    @pl.when(gz == nz - 1)
    def _():
        F[:, :, S + BZ:NZE, :, :] = jnp.zeros((2, 2, S, ROWS, 128), jnp.float32)

    @pl.when(yv == 0)
    def _():
        F[:, :, :, LO:MID, :] = jnp.zeros((2, 2, NZE, 8, 128), jnp.float32)

    @pl.when(yv == nyv - 1)
    def _():
        F[:, :, :, HI:HI + 8, :] = jnp.zeros((2, 2, NZE, 8, 128), jnp.float32)

    X[...] = jnp.zeros(X.shape, jnp.float32)

    row = lax.broadcasted_iota(jnp.int32, (24, 128), 0) + (8 * yv - 8)
    row_in = jnp.where((row >= 0) & (row < 8 * nyv), 2.0 / HALF, 0.0)
    for z in range(NZE):
        at = gz * BZ + (z - S)
        M[z] = row_in * jnp.where((at >= 0) & (at < nz * BZ), 1.0, 0.0)

    for cp in swaps:
        cp.wait()

    lane = lax.broadcasted_iota(jnp.int32, (24, 128), 1)

    def x_sum(v, rows):
        first = lane[:rows] == 0
        last = lane[:rows] == 127
        a0, a1 = pltpu.roll(v[0], 1, 1), pltpu.roll(v[1], 1, 1)
        b0, b1 = pltpu.roll(v[0], 127, 1), pltpu.roll(v[1], 127, 1)
        zero = jnp.zeros((rows, 128), jnp.float32)
        s0 = v[0] + jnp.where(first, zero, a0) + jnp.where(last, b1, b0)
        s1 = v[1] + jnp.where(first, a0, a1) + jnp.where(last, zero, b1)
        return s0, s1

    def neighbours(dz=0, dy=0):
        t = yv + dy
        return (gz + dz, t // 2, t % 2)

    def z_copy(k):
        src, dst, dz = ((S, S + BZ, -1), (BZ, 0, 1))[k]
        return pltpu.make_async_remote_copy(
            src_ref=F.at[:, :, pl.ds(src, S), own_rows, :],
            dst_ref=F.at[:, :, pl.ds(dst, S), own_rows, :],
            send_sem=zs_sem.at[k], recv_sem=zr_sem.at[k],
            device_id=neighbours(dz=dz), device_id_type=MESH,
        )

    def y_copy(k, planes, send, recv):
        dst, dy = ((HI, -1), (LO, 1))[k]
        return pltpu.make_async_remote_copy(
            src_ref=F.at[:, :, planes, own_rows, :],
            dst_ref=F.at[:, :, planes, pl.ds(dst, 8), :],
            send_sem=send, recv_sem=recv,
            device_id=neighbours(dy=dy), device_id_type=MESH,
        )

    to_z = (gz > 0, gz < nz - 1)
    from_z = (gz < nz - 1, gz > 0)
    to_y = (yv > 0, yv < nyv - 1)
    from_y = (yv < nyv - 1, yv > 0)
    bands = (pl.ds(S + BZ, S), pl.ds(0, S))

    def exchange():
        for k in range(2):
            @pl.when(to_z[k])
            def _(k=k):
                z_copy(k).start()
        for k in range(2):
            @pl.when(to_y[k])
            def _(k=k):
                y_copy(k, own_z, ys_sem.at[k], yr_sem.at[k]).start()
        for b in range(2):
            @pl.when(from_z[b])
            def _(b=b):
                z_copy(b).wait_recv()
                for k in range(2):
                    @pl.when(to_y[k])
                    def _(k=k):
                        y_copy(k, bands[b], fs_sem.at[b, k], fr_sem.at[b, k]).start()
        for k in range(2):
            @pl.when(from_y[k])
            def _(k=k):
                y_copy(k, own_z, ys_sem.at[k], yr_sem.at[k]).wait_recv()
                for b in range(2):
                    @pl.when(from_z[b])
                    def _(b=b):
                        y_copy(k, bands[b], fs_sem.at[b, k], fr_sem.at[b, k]).wait_recv()
        for k in range(2):
            @pl.when(to_z[k])
            def _(k=k):
                z_copy(k).wait_send()

            @pl.when(to_y[k])
            def _(k=k):
                y_copy(k, own_z, ys_sem.at[k], yr_sem.at[k]).wait_send()
                for b in range(2):
                    @pl.when(from_z[b])
                    def _(b=b):
                        y_copy(k, bands[b], fs_sem.at[b, k], fr_sem.at[b, k]).wait_send()

    def power_steps(read, write, degree, z0, z1, rows):
        r0, n = rows
        m0 = r0 - LO
        sums = {}

        def y_sum(z):
            if z not in sums:
                sums[z] = (
                    read(degree - 1, z, r0 - 1, n) + read(degree - 1, z, r0, n) + read(degree - 1, z, r0 + 1, n)
                )
            return sums[z]

        for z in range(z0, z1):
            s0, s1 = x_sum(y_sum(z - 1) + y_sum(z) + y_sum(z + 1), n)
            sums.pop(z - 1, None)
            mask = M[z, m0:m0 + n, :]
            box = jnp.stack([s0 * mask, s1 * mask])
            value = C[:, z, r0:r0 + n, :] * read(degree - 1, z, r0, n) - box
            if degree == 1:
                value = 0.5 * value
            else:
                value = value - read(degree - 2, z, r0, n)
            write(degree, z, r0, n, value)

    def reader(f, V):
        def read(degree, z, r, n):
            if degree == 0:
                return F[f, :, z, r:r + n, :]
            return V[degree - 1, :, z, r:r + n, :]
        return read

    def writer(V):
        def write(degree, z, r, n, value):
            V[degree - 1, :, z, r:r + n, :] = value
        return write

    read_p, read_r = reader(0, PV), reader(1, RV)
    write_p, write_r = writer(PV), writer(RV)

    def own(block, degree, xt):
        if degree == 0:
            return V0[block, xt]
        V = (PV, RV)[block]
        return V[degree - 1, xt, S:S + BZ, MID:MID + 8, :]

    lane8 = lax.broadcasted_iota(jnp.int32, (8, 128), 1)
    sub8 = lax.broadcasted_iota(jnp.int32, (8, 128), 0)

    def all_sublanes(v):
        v = v + pltpu.roll(v, 4, 0)
        v = v + pltpu.roll(v, 2, 0)
        return v + pltpu.roll(v, 1, 0)

    def splat(v, j):
        return jnp.broadcast_to(v[j:j + 1, :], (8, 128))

    def by_row(values):
        out = jnp.zeros((8, 128), jnp.float32)
        for j, value in enumerate(values):
            if value:
                out = jnp.where(sub8 == j, value, out)
        return out

    diag_c = (by_row([CENTER] * S), by_row([CENTER] * (S - 1)))
    from_low = (by_row([0.0, HALF] + [0.5 * HALF] * (S - 1)), by_row([0.0, HALF] + [0.5 * HALF] * (S - 2)))
    from_high = (by_row([0.5 * HALF] * (S - 1)), by_row([0.5 * HALF] * (S - 2)))

    def outer(t, carry):
        par = t % 2
        exchange()

        @pl.when(t == 0)
        def _():
            for z in range(NZE):
                C[:, z, LO:HI + 8, :] = (2.0 / HALF) * (
                    F[1, :, z, LO:HI + 8, :] + (27.0 - CENTER)
                )
                F[1, :, z, LO:HI + 8, :] = F[0, :, z, LO:HI + 8, :]

        for f in range(2):
            V0[f] = F[f, :, S:S + BZ, MID:MID + 8, :]
        for degree in range(1, S + 1):
            rows = (LO, 24) if degree < S else (MID, 8)
            power_steps(read_p, write_p, degree, degree, NZE - degree, rows)
            if degree < S:
                rows = (LO, 24) if degree < S - 1 else (MID, 8)
                power_steps(read_r, write_r, degree, degree + 1, NZE - degree - 1, rows)

        parts = [None] * (NPP + NPR + NRR)

        def add(k, a, b):
            s = jnp.sum(a * b, axis=0)
            parts[k] = s if parts[k] is None else parts[k] + s

        for xt in range(2):
            p, r = own(0, 0, xt), own(1, 0, xt)
            for i in range(S + 1):
                p_next = own(0, i + 1, xt) if i < S else None
                r_next = own(1, i + 1, xt) if i < S - 1 else None
                add(2 * i, p, p)
                if i < S:
                    add(2 * i + 1, p, p_next)
                    add(NPP + 2 * i, p, r)
                    add(NPP + 2 * i + 1, p_next, r)
                    add(NPP + NPR + 2 * i, r, r)
                if i < S - 1:
                    add(NPP + NPR + 2 * i + 1, r, r_next)
                p, r = p_next, r_next
        picked = jnp.zeros((8, 128), jnp.float32)
        for k, part in enumerate(parts):
            picked = jnp.where(lane8 == k, jnp.sum(part, axis=1, keepdims=True), picked)
        local = jnp.sum(picked, axis=0, keepdims=True)

        me1 = 8 * py + yv
        S1[par, me1] = local
        for dy in range(4):
            for dx in range(4):
                for dc in range(2):
                    if dy or dx or dc:
                        to = (((py + dy) % 4) * nzp + pz, (gy + dx) % 4, (gx + dc) % 2)
                        pltpu.make_async_remote_copy(
                            src_ref=S1.at[par, me1], dst_ref=S1.at[par, me1],
                            send_sem=g1_s.at[par], recv_sem=g1_r.at[par],
                            device_id=to, device_id_type=MESH,
                        ).start()
        whole1 = pltpu.make_async_copy(S1.at[par, pl.ds(0, 31)], S1.at[par, pl.ds(0, 31)], g1_r.at[par])
        whole1.wait()
        S2[par, pz] = jnp.sum(S1[par], axis=0)
        for dz in range(1, nzp):
            to = (py * nzp + (pz + dz) % nzp, gy, gx)
            pltpu.make_async_remote_copy(
                src_ref=S2.at[par, pz], dst_ref=S2.at[par, pz],
                send_sem=g2_s.at[par], recv_sem=g2_r.at[par],
                device_id=to, device_id_type=MESH,
            ).start()
        whole2 = pltpu.make_async_copy(S2.at[par, pl.ds(0, 7)], S2.at[par, pl.ds(0, 7)], g2_r.at[par])
        whole2.wait()
        moments = jnp.broadcast_to(jnp.sum(S2[par], axis=0), (8, 128))
        pltpu.make_async_copy(S1.at[par, pl.ds(0, 31)], S1.at[par, pl.ds(0, 31)], g1_s.at[par]).wait()
        pltpu.make_async_copy(S2.at[par, pl.ds(0, 7)], S2.at[par, pl.ds(0, 7)], g2_s.at[par]).wait()

        columns = 2 * S + 1
        table = [
            [
                [
                    jnp.broadcast_to(jnp.sum(w_ref[which, j, half] * moments, axis=1, keepdims=True), (8, 128))
                    for half in range(2)
                ]
                for j in range(columns)
            ]
            for which in range(2)
        ]

        def form(which, v):
            col = [splat(v[0], j) for j in range(S + 1)] + [splat(v[1], j) for j in range(S)]
            total = None
            for half in range(2):
                terms = [table[which][j][half] * col[j] for j in range(columns)]
                while len(terms) > 1:
                    terms = [
                        terms[i] + terms[i + 1] if i + 1 < len(terms) else terms[i] for i in range(0, len(terms), 2)
                    ]
                part = terms[0] * v[half]
                total = part if total is None else total + part
            return all_sublanes(total)

        unit = jnp.where(sub8 == 0, 1.0, 0.0)
        none = jnp.zeros((8, 128), jnp.float32)
        p_c, r_c, x_c = [unit, none], [none, unit], [none, none]
        norm = form(0, r_c)
        for step in range(S):
            q = [
                diag_c[h] * p_c[h] + from_low[h] * pltpu.roll(p_c[h], 1, 0) + from_high[h] * pltpu.roll(p_c[h], 7, 0)
                for h in range(2)
            ]
            length = norm / form(1, p_c)
            x_c = [x_c[h] + length * p_c[h] for h in range(2)]
            r_c = [r_c[h] - length * q[h] for h in range(2)]
            norm_next = form(0, r_c)
            ratio = norm_next / norm
            p_c = [r_c[h] + ratio * p_c[h] for h in range(2)]
            norm = norm_next

        def combine(c, xt):
            total = None
            for block in range(2):
                for degree in range(S + 1 - block):
                    term = splat(c[block], degree)[None] * own(block, degree, xt)
                    total = term if total is None else total + term
            return total

        for xt in range(2):
            F[0, xt, S:S + BZ, MID:MID + 8, :] = combine(p_c, xt)
            F[1, xt, S:S + BZ, MID:MID + 8, :] = combine(r_c, xt)
            X[xt] = X[xt] + combine(x_c, xt)
        return carry

    lax.fori_loop(0, OUTER, outer, 0)

    backs = []
    for f, (src, out) in enumerate(
        ((X.at[sib], sol_ref), (F.at[1, sib, own_z, own_rows, :], res_ref))
    ):
        cp = pltpu.make_async_remote_copy(
            src_ref=src, dst_ref=land.at[f],
            send_sem=io_s.at[2 + f], recv_sem=io_r.at[2 + f],
            device_id=(gz, gy, sib), device_id_type=MESH,
        )
        cp.start()
        backs.append(cp)
    mine = pl.ds(pl.multiple_of(8 * gx, 8), 8)
    sol_ref[:, mine, :] = X[gx]
    res_ref[:, mine, :] = F[1, gx, S:S + BZ, MID:MID + 8, :]
    other = pl.ds(pl.multiple_of(8 * sib, 8), 8)
    for f, out in enumerate((sol_ref, res_ref)):
        backs[f].wait()
        out[:, other, :] = land[f]


def solution(mesh):
    table = weights()

    def local(right_side, diagonal):
        f32 = jnp.float32
        dma = pltpu.SemaphoreType.DMA
        field = (2, NZE, ROWS, 128)
        return pl.pallas_call(
            kernel,
            out_shape=(jax.ShapeDtypeStruct(right_side.shape, f32),) * 2,
            in_specs=[pl.BlockSpec(memory_space=pltpu.VMEM)] * 3,
            out_specs=(pl.BlockSpec(memory_space=pltpu.VMEM),) * 2,
            scratch_shapes=[
                pltpu.VMEM((2,) + field, f32),
                pltpu.VMEM((S,) + field, f32),
                pltpu.VMEM((S - 1,) + field, f32),
                pltpu.VMEM(field, f32),
                pltpu.VMEM((NZE, 24, 128), f32),
                pltpu.VMEM((2, 2, BZ, 8, 128), f32),
                pltpu.VMEM((2, BZ, 8, 128), f32),
                pltpu.VMEM((2, BZ, 8, 128), f32),
                pltpu.VMEM((2, 32, 1, 128), f32),
                pltpu.VMEM((2, 8, 1, 128), f32),
                dma((2,)), dma((2,)), dma((2,)), dma((2,)), dma((2, 2)), dma((2, 2)),
                dma((4,)), dma((4,)), dma((2,)), dma((2,)), dma((2,)), dma((2,)),
            ],
            compiler_params=pltpu.CompilerParams(has_side_effects=True, vmem_limit_bytes=48 * 2**20),
        )(right_side, diagonal, jnp.asarray(table))

    spec = P("gz", "gy", "gx")
    return jax.shard_map(
        local, mesh=mesh, in_specs=(spec, spec), out_specs=(spec, spec), check_vma=False
    )
```

```python
import functools

import jax
import jax.numpy as jnp
import numpy as np
from jax import lax
from jax.experimental import pallas as pl
from jax.experimental.pallas import tpu as pltpu
from jax.sharding import PartitionSpec as P

S = 6
INNER = (6,) * 5
MESH = pl.DeviceIdType.MESH

CENTER = 19.0
HALF = 19.0

BZ = 8
NZE = BZ + 2 * S
ROWS = 40
LO, MID, HI = 8, 16, 24

NPP, NPR, NRR = 2 * S + 1, 2 * S, 2 * S - 1

PARTS = 3 if S == 8 else 2


def place(i):
    if i > S:
        return 1, i - S - 1
    return (0, i) if i < 8 else (2, i - 8)


def weights():
    columns = 2 * S + 1
    total = NPP + NPR + NRR

    def moment(offset, m):
        v = np.zeros(total)
        if m < 2:
            v[offset + m] = 1.0
        else:
            v[offset + m] = 2.0
            v[offset + m % 2] -= 1.0
        return v

    gram = np.zeros((columns, columns, total))
    for i in range(columns):
        for j in range(columns):
            di, dj = (i if i <= S else i - S - 1), (j if j <= S else j - S - 1)
            kinds = (i > S) + (j > S)
            offset = (0, NPP, NPP + NPR)[kinds]
            gram[i, j] = (moment(offset, di + dj) + moment(offset, abs(di - dj))) / 2
    change = np.zeros((columns, columns))
    for offset, length in ((0, S), (S + 1, S - 1)):
        for degree in range(length):
            change[offset + degree, offset + degree] = CENTER
            if degree == 0:
                change[offset + 1, offset] = HALF
            else:
                change[offset + degree + 1, offset + degree] = 0.5 * HALF
                change[offset + degree - 1, offset + degree] = 0.5 * HALF
    moved = np.einsum("ikm,kj->ijm", gram, change)
    out = np.zeros((2, columns, PARTS, 8, 128), np.float32)
    for which, table in enumerate((gram, moved)):
        for j in range(columns):
            for i in range(columns):
                half, row = place(i)
                out[which, j, half, row, :total] = table[i, j]
    return out


def kernel(
    rhs_ref, diag_ref, w_hbm, sol_ref, res_ref,
    F, PV, RV, C, M, V0, X, XC, land, S1, S2, w_ref,
    in_sem, zs_sem, zr_sem, ys_sem, yr_sem, cs_sem, cr_sem, fs_sem, fr_sem, io_s, io_r, g1_s, g1_r, g2_s, g2_r,
):
    gz = lax.axis_index("gz")
    gy = lax.axis_index("gy")
    gx = lax.axis_index("gx")
    nz = lax.axis_size("gz")
    ny = lax.axis_size("gy")
    yv = 2 * gy + gx
    nyv = 2 * ny
    sib = 1 - gx
    nzp = 8
    py = gz // nzp
    pz = gz % nzp

    own_rows = pl.ds(MID, 8)
    own_z = pl.ds(S, BZ)
    mine = pl.ds(pl.multiple_of(8 * gx, 8), 8)
    other = pl.ds(pl.multiple_of(8 * sib, 8), 8)

    loads = []
    for f, ref in enumerate((rhs_ref, diag_ref)):
        loads.append(pltpu.make_async_copy(ref.at[:, other, :], land.at[f], in_sem.at[f]))
    for f, ref in enumerate((rhs_ref, diag_ref)):
        loads.append(pltpu.make_async_copy(ref.at[:, mine, :], F.at[f, gx, own_z, own_rows, :], in_sem.at[2 + f]))
    loads.append(pltpu.make_async_copy(w_hbm, w_ref, in_sem.at[4]))
    for cp in loads:
        cp.start()

    plane = [
        (((py + dy) % 4) * nzp + pz, (gy + dx) % 4, (gx + dc) % 2)
        for dy in range(4) for dx in range(4) for dc in range(2) if dy or dx or dc
    ]
    line = [(py * nzp + (pz + dz) % nzp, gy, gx) for dz in range(1, nzp)]
    off_gy = gy + 2 * gx - 1
    has_off = (off_gy >= 0) & (off_gy < ny)
    to_z = (gz > 0, gz < nz - 1)
    from_z = (gz < nz - 1, gz > 0)

    barrier = pltpu.get_barrier_semaphore()
    for to in plane + line:
        pl.semaphore_signal(barrier, inc=1, device_id=to, device_id_type=MESH)
    for k, dz in enumerate((-1, 1)):
        @pl.when(to_z[k])
        def _(dz=dz):
            pl.semaphore_signal(barrier, inc=1, device_id=(gz + dz, gy, gx), device_id_type=MESH)

        @pl.when(to_z[k] & has_off)
        def _(dz=dz):
            pl.semaphore_signal(barrier, inc=1, device_id=(gz + dz, off_gy, sib), device_id_type=MESH)

    @pl.when(gz == 0)
    def _():
        F[:, :, 0:S, :, :] = jnp.zeros((2, 2, S, ROWS, 128), jnp.float32)

    @pl.when(gz == nz - 1)
    def _():
        F[:, :, S + BZ:NZE, :, :] = jnp.zeros((2, 2, S, ROWS, 128), jnp.float32)

    @pl.when(yv == 0)
    def _():
        F[:, :, :, LO:MID, :] = jnp.zeros((2, 2, NZE, 8, 128), jnp.float32)

    @pl.when(yv == nyv - 1)
    def _():
        F[:, :, :, HI:HI + 8, :] = jnp.zeros((2, 2, NZE, 8, 128), jnp.float32)

    X[...] = jnp.zeros(X.shape, jnp.float32)

    row = lax.broadcasted_iota(jnp.int32, (24, 128), 0) + (8 * yv - 8)
    row_in = jnp.where((row >= 0) & (row < 8 * nyv), 2.0 / HALF, 0.0)
    for z in range(NZE):
        at = gz * BZ + (z - S)
        M[z] = row_in * jnp.where((at >= 0) & (at < nz * BZ), 1.0, 0.0)

    nz_near = jnp.where(gz > 0, 1, 0) + jnp.where(gz < nz - 1, 1, 0)
    pl.semaphore_wait(barrier, len(plane) + len(line) + nz_near * jnp.where(has_off, 2, 1))
    swaps = []
    for f in range(2):
        loads[f].wait()
        cp = pltpu.make_async_remote_copy(
            src_ref=land.at[f],
            dst_ref=F.at[f, gx, own_z, own_rows, :],
            send_sem=io_s.at[f], recv_sem=io_r.at[f],
            device_id=(gz, gy, sib), device_id_type=MESH,
        )
        cp.start()
        swaps.append(cp)
    for cp in loads[2:] + swaps:
        cp.wait()

    lane = lax.broadcasted_iota(jnp.int32, (24, 128), 1)

    def x_sum(v, rows):
        first = lane[:rows] == 0
        last = lane[:rows] == 127
        a0, a1 = pltpu.roll(v[0], 1, 1), pltpu.roll(v[1], 1, 1)
        b0, b1 = pltpu.roll(v[0], 127, 1), pltpu.roll(v[1], 127, 1)
        zero = jnp.zeros((rows, 128), jnp.float32)
        s0 = v[0] + jnp.where(first, zero, a0) + jnp.where(last, b1, b0)
        s1 = v[1] + jnp.where(first, a0, a1) + jnp.where(last, zero, b1)
        return s0, s1

    off_rows = pl.ds(pl.multiple_of(LO + 16 * sib, 8), 8)
    sib_rows = pl.ds(pl.multiple_of(LO + 16 * gx, 8), 8)
    bands = (pl.ds(S + BZ, S), pl.ds(0, S))
    edges = (pl.ds(S, S), pl.ds(BZ, S))
    near = (gz - 1, gz + 1)

    def remote(src_planes, dst_planes, dst_rows, send, recv, to):
        return pltpu.make_async_remote_copy(
            src_ref=F.at[:, :, src_planes, own_rows, :], dst_ref=F.at[:, :, dst_planes, dst_rows, :],
            send_sem=send, recv_sem=recv, device_id=to, device_id_type=MESH,
        )

    def z_copy(k):
        return remote(edges[k], bands[k], own_rows, zs_sem.at[k], zr_sem.at[k], (near[k], gy, gx))

    def corner(k):
        return remote(edges[k], bands[k], off_rows, cs_sem.at[k], cr_sem.at[k], (near[k], off_gy, sib))

    def forward(k):
        return remote(bands[k], bands[k], sib_rows, fs_sem.at[k], fr_sem.at[k], (gz, gy, sib))

    y_off = remote(own_z, own_z, off_rows, ys_sem.at[0], yr_sem.at[0], (gz, off_gy, sib))
    y_sib = remote(own_z, own_z, sib_rows, ys_sem.at[1], yr_sem.at[1], (gz, gy, sib))

    def exchange_start():
        for k in range(2):
            @pl.when(to_z[k])
            def _(k=k):
                z_copy(k).start()

        @pl.when(has_off)
        def _():
            y_off.start()
        for k in range(2):
            @pl.when(to_z[k] & has_off)
            def _(k=k):
                corner(k).start()
        y_sib.start()

    def exchange_finish():
        for k in range(2):
            @pl.when(from_z[k])
            def _(k=k):
                z_copy(k).wait_recv()
                forward(k).start()
        y_sib.wait_recv()

        @pl.when(has_off)
        def _():
            y_off.wait_recv()
        for k in range(2):
            @pl.when(from_z[k])
            def _(k=k):
                forward(k).wait_recv()

            @pl.when(from_z[k] & has_off)
            def _(k=k):
                corner(k).wait_recv()
        y_sib.wait_send()

        @pl.when(has_off)
        def _():
            y_off.wait_send()
        for k in range(2):
            @pl.when(to_z[k])
            def _(k=k):
                z_copy(k).wait_send()

            @pl.when(to_z[k] & has_off)
            def _(k=k):
                corner(k).wait_send()

            @pl.when(from_z[k])
            def _(k=k):
                forward(k).wait_send()

    def power_steps(read, write, degree, z0, z1, rows):
        r0, n = rows
        m0 = r0 - LO
        sums = {}

        def y_sum(z):
            if z not in sums:
                sums[z] = (
                    read(degree - 1, z, r0 - 1, n) + read(degree - 1, z, r0, n) + read(degree - 1, z, r0 + 1, n)
                )
            return sums[z]

        for z in range(z0, z1):
            s0, s1 = x_sum(y_sum(z - 1) + y_sum(z) + y_sum(z + 1), n)
            sums.pop(z - 1, None)
            mask = M[z, m0:m0 + n, :]
            box = jnp.stack([s0 * mask, s1 * mask])
            value = C[:, z, r0:r0 + n, :] * read(degree - 1, z, r0, n) - box
            if degree == 1:
                value = 0.5 * value
            else:
                value = value - read(degree - 2, z, r0, n)
            write(degree, z, r0, n, value)

    def reader(f, V):
        def read(degree, z, r, n):
            if degree == 0:
                return F[f, :, z, r:r + n, :]
            return V[degree - 1, :, z, r:r + n, :]
        return read

    def writer(V):
        def write(degree, z, r, n, value):
            V[degree - 1, :, z, r:r + n, :] = value
        return write

    read_p, read_r = reader(0, PV), reader(1, RV)
    write_p, write_r = writer(PV), writer(RV)

    def own(block, degree, xt):
        if degree == 0:
            return V0[block, xt]
        V = (PV, RV)[block]
        return V[degree - 1, xt, S:S + BZ, MID:MID + 8, :]

    lane8 = lax.broadcasted_iota(jnp.int32, (8, 128), 1)
    sub8 = lax.broadcasted_iota(jnp.int32, (8, 128), 0)

    def all_sublanes(v):
        v = v + pltpu.roll(v, 4, 0)
        v = v + pltpu.roll(v, 2, 0)
        return v + pltpu.roll(v, 1, 0)

    def splat(v, j):
        return jnp.broadcast_to(v[j:j + 1, :], (8, 128))

    def by_row(values):
        out = jnp.zeros((8, 128), jnp.float32)
        for j, value in enumerate(values):
            if value:
                out = jnp.where(sub8 == j, value, out)
        return out

    diag_c = (by_row([CENTER] * S), by_row([CENTER] * (S - 1)))
    from_low = (by_row([0.0, HALF] + [0.5 * HALF] * (S - 1)), by_row([0.0, HALF] + [0.5 * HALF] * (S - 2)))
    from_high = (by_row([0.5 * HALF] * (S - 1)), by_row([0.5 * HALF] * (S - 2)))

    def combine(c, xt):
        total = None
        for block in range(2):
            for degree in range(S + 1 - block):
                half, row = place(degree + block * (S + 1))
                term = splat(c[half], row)[None] * own(block, degree, xt)
                total = term if total is None else total + term
        return total

    def outer(t, carry):
        par = t % 2
        exchange_start()

        @pl.when(t > 0)
        def _():
            for xt in range(2):
                X[xt] = X[xt] + combine([XC[h] for h in range(PARTS)], xt)
        exchange_finish()

        @pl.when(t == 0)
        def _():
            for z in range(NZE):
                C[:, z, LO:HI + 8, :] = (2.0 / HALF) * (
                    F[1, :, z, LO:HI + 8, :] + (27.0 - CENTER)
                )
                F[1, :, z, LO:HI + 8, :] = F[0, :, z, LO:HI + 8, :]

        for f in range(2):
            V0[f] = F[f, :, S:S + BZ, MID:MID + 8, :]
        for degree in range(1, S + 1):
            rows = (LO, 24) if degree < S else (MID, 8)
            power_steps(read_p, write_p, degree, degree, NZE - degree, rows)
            if degree < S:
                rows = (LO, 24) if degree < S - 1 else (MID, 8)
                power_steps(read_r, write_r, degree, degree + 1, NZE - degree - 1, rows)

        parts = [None] * (NPP + NPR + NRR)

        def add(k, a, b):
            s = jnp.sum(a * b, axis=0)
            parts[k] = s if parts[k] is None else parts[k] + s

        for xt in range(2):
            p, r = own(0, 0, xt), own(1, 0, xt)
            for i in range(S + 1):
                p_next = own(0, i + 1, xt) if i < S else None
                r_next = own(1, i + 1, xt) if i < S - 1 else None
                add(2 * i, p, p)
                if i < S:
                    add(2 * i + 1, p, p_next)
                    add(NPP + 2 * i, p, r)
                    add(NPP + 2 * i + 1, p_next, r)
                    add(NPP + NPR + 2 * i, r, r)
                if i < S - 1:
                    add(NPP + NPR + 2 * i + 1, r, r_next)
                p, r = p_next, r_next
        picked = jnp.zeros((8, 128), jnp.float32)
        for k, part in enumerate(parts):
            picked = jnp.where(lane8 == k, jnp.sum(part, axis=1, keepdims=True), picked)
        local = jnp.sum(picked, axis=0, keepdims=True)

        me1 = 8 * py + yv
        S1[par, me1] = local
        for to in plane:
            pltpu.make_async_remote_copy(
                src_ref=S1.at[par, me1], dst_ref=S1.at[par, me1],
                send_sem=g1_s.at[par], recv_sem=g1_r.at[par],
                device_id=to, device_id_type=MESH,
            ).start()
        whole1 = pltpu.make_async_copy(S1.at[par, pl.ds(0, 31)], S1.at[par, pl.ds(0, 31)], g1_r.at[par])
        whole1.wait()
        S2[par, pz] = jnp.sum(S1[par], axis=0)
        for to in line:
            pltpu.make_async_remote_copy(
                src_ref=S2.at[par, pz], dst_ref=S2.at[par, pz],
                send_sem=g2_s.at[par], recv_sem=g2_r.at[par],
                device_id=to, device_id_type=MESH,
            ).start()
        whole2 = pltpu.make_async_copy(S2.at[par, pl.ds(0, 7)], S2.at[par, pl.ds(0, 7)], g2_r.at[par])
        whole2.wait()
        moments = jnp.broadcast_to(jnp.sum(S2[par], axis=0), (8, 128))
        pltpu.make_async_copy(S1.at[par, pl.ds(0, 31)], S1.at[par, pl.ds(0, 31)], g1_s.at[par]).wait()
        pltpu.make_async_copy(S2.at[par, pl.ds(0, 7)], S2.at[par, pl.ds(0, 7)], g2_s.at[par]).wait()

        columns = 2 * S + 1
        table = [
            [
                [
                    jnp.broadcast_to(jnp.sum(w_ref[which, j, half] * moments, axis=1, keepdims=True), (8, 128))
                    for half in range(PARTS)
                ]
                for j in range(columns)
            ]
            for which in range(2)
        ]

        def form(which, v):
            col = [splat(v[place(j)[0]], place(j)[1]) for j in range(columns)]
            total = None
            for half in range(PARTS):
                terms = [table[which][j][half] * col[j] for j in range(columns)]
                while len(terms) > 1:
                    terms = [
                        terms[i] + terms[i + 1] if i + 1 < len(terms) else terms[i] for i in range(0, len(terms), 2)
                    ]
                part = terms[0] * v[half]
                total = part if total is None else total + part
            return all_sublanes(total)

        unit = jnp.where(sub8 == 0, 1.0, 0.0)
        none = jnp.zeros((8, 128), jnp.float32)
        p_c, r_c, x_c = ([unit] + [none] * (PARTS - 1), [none, unit] + [none] * (PARTS - 2), [none] * PARTS)
        norm = form(0, r_c)
        for step in range(S):
            q = [
                diag_c[h] * p_c[h] + from_low[h] * pltpu.roll(p_c[h], 1, 0) + from_high[h] * pltpu.roll(p_c[h], 7, 0)
                for h in range(2)
            ]
            if PARTS == 3:
                q.append(jnp.where(sub8 == 0, 0.5 * HALF * splat(p_c[0], 7), 0.0))
            length = norm / form(1, p_c)
            r_next = [r_c[h] - length * q[h] for h in range(PARTS)]
            norm_next = form(0, r_next)
            ratio = norm_next / norm
            new = (
                [x_c[h] + length * p_c[h] for h in range(PARTS)] + r_next
                + [r_next[h] + ratio * p_c[h] for h in range(PARTS)] + [norm_next]
            )
            count = sum(inner > step for inner in INNER)
            if count < len(INNER):
                keep = jnp.full((8, 128), t, jnp.int32) < count
                new = [jnp.where(keep, a, b) for a, b in zip(new, x_c + r_c + p_c + [norm])]
            x_c, r_c, p_c, norm = new[:PARTS], new[PARTS:2 * PARTS], new[2 * PARTS:3 * PARTS], new[-1]

        for xt in range(2):
            F[0, xt, S:S + BZ, MID:MID + 8, :] = combine(p_c, xt)
            F[1, xt, S:S + BZ, MID:MID + 8, :] = combine(r_c, xt)
        for h in range(PARTS):
            XC[h] = x_c[h]
        return carry

    lax.fori_loop(0, len(INNER), outer, 0)

    def back(f, src):
        return pltpu.make_async_remote_copy(
            src_ref=src, dst_ref=land.at[f],
            send_sem=io_s.at[2 + f], recv_sem=io_r.at[2 + f],
            device_id=(gz, gy, sib), device_id_type=MESH,
        )

    res_back = back(1, F.at[1, sib, own_z, own_rows, :])
    res_back.start()
    for xt in range(2):
        X[xt] = X[xt] + combine([XC[h] for h in range(PARTS)], xt)
    sol_back = back(0, X.at[sib])
    sol_back.start()
    res_ref[:, mine, :] = F[1, gx, S:S + BZ, MID:MID + 8, :]
    sol_ref[:, mine, :] = X[gx]
    for f, (cp, out) in enumerate(((sol_back, sol_ref), (res_back, res_ref))):
        cp.wait()
        out[:, other, :] = land[f]


def solution(mesh):
    table = weights()

    def local(right_side, diagonal):
        f32 = jnp.float32
        dma = pltpu.SemaphoreType.DMA
        field = (2, NZE, ROWS, 128)
        return pl.pallas_call(
            kernel,
            out_shape=(jax.ShapeDtypeStruct(right_side.shape, f32),) * 2,
            in_specs=[pl.BlockSpec(memory_space=pltpu.HBM)] * 3,
            out_specs=(pl.BlockSpec(memory_space=pltpu.VMEM),) * 2,
            scratch_shapes=[
                pltpu.VMEM((2,) + field, f32),
                pltpu.VMEM((S,) + field, f32),
                pltpu.VMEM((S - 1,) + field, f32),
                pltpu.VMEM(field, f32),
                pltpu.VMEM((NZE, 24, 128), f32),
                pltpu.VMEM((2, 2, BZ, 8, 128), f32),
                pltpu.VMEM((2, BZ, 8, 128), f32),
                pltpu.VMEM((PARTS, 8, 128), f32),
                pltpu.VMEM((2, BZ, 8, 128), f32),
                pltpu.VMEM((2, 32, 1, 128), f32),
                pltpu.VMEM((2, 8, 1, 128), f32),
                pltpu.VMEM(table.shape, f32),
                dma((5,)), dma((2,)), dma((2,)), dma((2,)), dma((2,)), dma((2,)), dma((2,)), dma((2,)), dma((2,)),
                dma((4,)), dma((4,)), dma((2,)), dma((2,)), dma((2,)), dma((2,)),
            ],
            compiler_params=pltpu.CompilerParams(collective_id=0, has_side_effects=True, vmem_limit_bytes=67043328),
        )(right_side, diagonal, jnp.asarray(table))

    spec = P("gz", "gy", "gx")
    return jax.shard_map(
        local, mesh=mesh, in_specs=(spec, spec), out_specs=(spec, spec), check_vma=False
    )
```

```python
import functools

import jax
import jax.numpy as jnp
import numpy as np
from jax import lax
from jax.experimental import pallas as pl
from jax.experimental.pallas import tpu as pltpu
from jax.sharding import PartitionSpec as P

S = 8
INNER = (8, 8, 7, 7)
MESH = pl.DeviceIdType.MESH

CENTER = 19.0
HALF = 19.0

BZ = 8
NZE = BZ + 2 * S
ROWS = 40
LO, MID, HI = 8, 16, 24

NPP, NPR, NRR = 2 * S + 1, 2 * S, 2 * S - 1

PARTS = 3 if S == 8 else 2


def place(i):
    if i > S:
        return 1, i - S - 1
    return (0, i) if i < 8 else (2, i - 8)


def weights():
    columns = 2 * S + 1
    total = NPP + NPR + NRR

    def moment(offset, m):
        v = np.zeros(total)
        if m < 2:
            v[offset + m] = 1.0
        else:
            v[offset + m] = 2.0
            v[offset + m % 2] -= 1.0
        return v

    gram = np.zeros((columns, columns, total))
    for i in range(columns):
        for j in range(columns):
            di, dj = (i if i <= S else i - S - 1), (j if j <= S else j - S - 1)
            kinds = (i > S) + (j > S)
            offset = (0, NPP, NPP + NPR)[kinds]
            gram[i, j] = (moment(offset, di + dj) + moment(offset, abs(di - dj))) / 2
    change = np.zeros((columns, columns))
    for offset, length in ((0, S), (S + 1, S - 1)):
        for degree in range(length):
            change[offset + degree, offset + degree] = CENTER
            if degree == 0:
                change[offset + 1, offset] = HALF
            else:
                change[offset + degree + 1, offset + degree] = 0.5 * HALF
                change[offset + degree - 1, offset + degree] = 0.5 * HALF
    moved = np.einsum("ikm,kj->ijm", gram, change)
    out = np.zeros((2, columns, PARTS, 8, 128), np.float32)
    for which, table in enumerate((gram, moved)):
        for j in range(columns):
            for i in range(columns):
                half, row = place(i)
                out[which, j, half, row, :total] = table[i, j]
    return out


def kernel(
    rhs_ref, diag_ref, w_hbm, sol_ref, res_ref,
    F, PV, RV, C, M, V0, X, XC, land, S1, S2, w_ref,
    in_sem, zs_sem, zr_sem, ys_sem, yr_sem, cs_sem, cr_sem, fs_sem, fr_sem, io_s, io_r, g1_s, g1_r, g2_s, g2_r,
):
    gz = lax.axis_index("gz")
    gy = lax.axis_index("gy")
    gx = lax.axis_index("gx")
    nz = lax.axis_size("gz")
    ny = lax.axis_size("gy")
    yv = 2 * gy + gx
    nyv = 2 * ny
    sib = 1 - gx
    nzp = 8
    py = gz // nzp
    pz = gz % nzp

    own_rows = pl.ds(MID, 8)
    own_z = pl.ds(S, BZ)
    mine = pl.ds(pl.multiple_of(8 * gx, 8), 8)
    other = pl.ds(pl.multiple_of(8 * sib, 8), 8)

    loads = []
    for f, ref in enumerate((rhs_ref, diag_ref)):
        loads.append(pltpu.make_async_copy(ref.at[:, other, :], land.at[f], in_sem.at[f]))
    for f, ref in enumerate((rhs_ref, diag_ref)):
        loads.append(pltpu.make_async_copy(ref.at[:, mine, :], F.at[f, gx, own_z, own_rows, :], in_sem.at[2 + f]))
    loads.append(pltpu.make_async_copy(w_hbm, w_ref, in_sem.at[4]))
    for cp in loads:
        cp.start()

    plane = [
        (((py + dy) % 4) * nzp + pz, (gy + dx) % 4, (gx + dc) % 2)
        for dy in range(4) for dx in range(4) for dc in range(2) if dy or dx or dc
    ]
    line = [(py * nzp + (pz + dz) % nzp, gy, gx) for dz in range(1, nzp)]
    off_gy = gy + 2 * gx - 1
    has_off = (off_gy >= 0) & (off_gy < ny)
    to_z = (gz > 0, gz < nz - 1)
    from_z = (gz < nz - 1, gz > 0)

    barrier = pltpu.get_barrier_semaphore()
    for to in plane + line:
        pl.semaphore_signal(barrier, inc=1, device_id=to, device_id_type=MESH)
    for k, dz in enumerate((-1, 1)):
        @pl.when(to_z[k])
        def _(dz=dz):
            pl.semaphore_signal(barrier, inc=1, device_id=(gz + dz, gy, gx), device_id_type=MESH)

        @pl.when(to_z[k] & has_off)
        def _(dz=dz):
            pl.semaphore_signal(barrier, inc=1, device_id=(gz + dz, off_gy, sib), device_id_type=MESH)

    @pl.when(gz == 0)
    def _():
        F[:, :, 0:S, :, :] = jnp.zeros((2, 2, S, ROWS, 128), jnp.float32)

    @pl.when(gz == nz - 1)
    def _():
        F[:, :, S + BZ:NZE, :, :] = jnp.zeros((2, 2, S, ROWS, 128), jnp.float32)

    @pl.when(yv == 0)
    def _():
        F[:, :, :, LO:MID, :] = jnp.zeros((2, 2, NZE, 8, 128), jnp.float32)

    @pl.when(yv == nyv - 1)
    def _():
        F[:, :, :, HI:HI + 8, :] = jnp.zeros((2, 2, NZE, 8, 128), jnp.float32)

    X[...] = jnp.zeros(X.shape, jnp.float32)

    row = lax.broadcasted_iota(jnp.int32, (24, 128), 0) + (8 * yv - 8)
    row_in = jnp.where((row >= 0) & (row < 8 * nyv), 2.0 / HALF, 0.0)
    for z in range(NZE):
        at = gz * BZ + (z - S)
        M[z] = row_in * jnp.where((at >= 0) & (at < nz * BZ), 1.0, 0.0)

    nz_near = jnp.where(gz > 0, 1, 0) + jnp.where(gz < nz - 1, 1, 0)
    pl.semaphore_wait(barrier, len(plane) + len(line) + nz_near * jnp.where(has_off, 2, 1))
    swaps = []
    for f in range(2):
        loads[f].wait()
        cp = pltpu.make_async_remote_copy(
            src_ref=land.at[f],
            dst_ref=F.at[f, gx, own_z, own_rows, :],
            send_sem=io_s.at[f], recv_sem=io_r.at[f],
            device_id=(gz, gy, sib), device_id_type=MESH,
        )
        cp.start()
        swaps.append(cp)
    for cp in loads[2:] + swaps:
        cp.wait()

    lane = lax.broadcasted_iota(jnp.int32, (24, 128), 1)

    def x_sum(v, rows):
        first = lane[:rows] == 0
        last = lane[:rows] == 127
        a0, a1 = pltpu.roll(v[0], 1, 1), pltpu.roll(v[1], 1, 1)
        b0, b1 = pltpu.roll(v[0], 127, 1), pltpu.roll(v[1], 127, 1)
        zero = jnp.zeros((rows, 128), jnp.float32)
        s0 = v[0] + jnp.where(first, zero, a0) + jnp.where(last, b1, b0)
        s1 = v[1] + jnp.where(first, a0, a1) + jnp.where(last, zero, b1)
        return s0, s1

    off_rows = pl.ds(pl.multiple_of(LO + 16 * sib, 8), 8)
    sib_rows = pl.ds(pl.multiple_of(LO + 16 * gx, 8), 8)
    bands = (pl.ds(S + BZ, S), pl.ds(0, S))
    edges = (pl.ds(S, S), pl.ds(BZ, S))
    near = (gz - 1, gz + 1)

    def remote(src_planes, dst_planes, dst_rows, send, recv, to):
        return pltpu.make_async_remote_copy(
            src_ref=F.at[:, :, src_planes, own_rows, :], dst_ref=F.at[:, :, dst_planes, dst_rows, :],
            send_sem=send, recv_sem=recv, device_id=to, device_id_type=MESH,
        )

    def z_copy(k):
        return remote(edges[k], bands[k], own_rows, zs_sem.at[k], zr_sem.at[k], (near[k], gy, gx))

    def corner(k):
        return remote(edges[k], bands[k], off_rows, cs_sem.at[k], cr_sem.at[k], (near[k], off_gy, sib))

    def forward(k):
        return remote(bands[k], bands[k], sib_rows, fs_sem.at[k], fr_sem.at[k], (gz, gy, sib))

    y_off = remote(own_z, own_z, off_rows, ys_sem.at[0], yr_sem.at[0], (gz, off_gy, sib))
    y_sib = remote(own_z, own_z, sib_rows, ys_sem.at[1], yr_sem.at[1], (gz, gy, sib))

    def exchange_start():
        for k in range(2):
            @pl.when(to_z[k])
            def _(k=k):
                z_copy(k).start()

        @pl.when(has_off)
        def _():
            y_off.start()
        for k in range(2):
            @pl.when(to_z[k] & has_off)
            def _(k=k):
                corner(k).start()
        y_sib.start()

    def exchange_finish():
        for k in range(2):
            @pl.when(from_z[k])
            def _(k=k):
                z_copy(k).wait_recv()
                forward(k).start()
        y_sib.wait_recv()

        @pl.when(has_off)
        def _():
            y_off.wait_recv()
        for k in range(2):
            @pl.when(from_z[k])
            def _(k=k):
                forward(k).wait_recv()

            @pl.when(from_z[k] & has_off)
            def _(k=k):
                corner(k).wait_recv()
        y_sib.wait_send()

        @pl.when(has_off)
        def _():
            y_off.wait_send()
        for k in range(2):
            @pl.when(to_z[k])
            def _(k=k):
                z_copy(k).wait_send()

            @pl.when(to_z[k] & has_off)
            def _(k=k):
                corner(k).wait_send()

            @pl.when(from_z[k])
            def _(k=k):
                forward(k).wait_send()

    def power_steps(read, write, degree, z0, z1, rows):
        r0, n = rows
        m0 = r0 - LO
        sums = {}

        def y_sum(z):
            if z not in sums:
                sums[z] = (
                    read(degree - 1, z, r0 - 1, n) + read(degree - 1, z, r0, n) + read(degree - 1, z, r0 + 1, n)
                )
            return sums[z]

        for z in range(z0, z1):
            s0, s1 = x_sum(y_sum(z - 1) + y_sum(z) + y_sum(z + 1), n)
            sums.pop(z - 1, None)
            mask = M[z, m0:m0 + n, :]
            box = jnp.stack([s0 * mask, s1 * mask])
            value = C[:, z, r0:r0 + n, :] * read(degree - 1, z, r0, n) - box
            if degree == 1:
                value = 0.5 * value
            else:
                value = value - read(degree - 2, z, r0, n)
            write(degree, z, r0, n, value)

    def reader(f, V):
        def read(degree, z, r, n):
            if degree == 0:
                return F[f, :, z, r:r + n, :]
            return V[degree - 1, :, z, r:r + n, :]
        return read

    def writer(V):
        def write(degree, z, r, n, value):
            V[degree - 1, :, z, r:r + n, :] = value
        return write

    read_p, read_r = reader(0, PV), reader(1, RV)
    write_p, write_r = writer(PV), writer(RV)

    def own(block, degree, xt):
        if degree == 0:
            return V0[block, xt]
        V = (PV, RV)[block]
        return V[degree - 1, xt, S:S + BZ, MID:MID + 8, :]

    lane8 = lax.broadcasted_iota(jnp.int32, (8, 128), 1)
    sub8 = lax.broadcasted_iota(jnp.int32, (8, 128), 0)

    def all_sublanes(v):
        v = v + pltpu.roll(v, 4, 0)
        v = v + pltpu.roll(v, 2, 0)
        return v + pltpu.roll(v, 1, 0)

    def splat(v, j):
        return jnp.broadcast_to(v[j:j + 1, :], (8, 128))

    def by_row(values):
        out = jnp.zeros((8, 128), jnp.float32)
        for j, value in enumerate(values):
            if value:
                out = jnp.where(sub8 == j, value, out)
        return out

    diag_c = (by_row([CENTER] * S), by_row([CENTER] * (S - 1)))
    from_low = (by_row([0.0, HALF] + [0.5 * HALF] * (S - 1)), by_row([0.0, HALF] + [0.5 * HALF] * (S - 2)))
    from_high = (by_row([0.5 * HALF] * (S - 1)), by_row([0.5 * HALF] * (S - 2)))

    def combine(c, xt):
        total = None
        for block in range(2):
            for degree in range(S + 1 - block):
                half, row = place(degree + block * (S + 1))
                term = splat(c[half], row)[None] * own(block, degree, xt)
                total = term if total is None else total + term
        return total

    def outer(t, carry):
        par = t % 2
        exchange_start()

        @pl.when(t > 0)
        def _():
            for xt in range(2):
                X[xt] = X[xt] + combine([XC[h] for h in range(PARTS)], xt)
        exchange_finish()

        @pl.when(t == 0)
        def _():
            for z in range(NZE):
                C[:, z, LO:HI + 8, :] = (2.0 / HALF) * (
                    F[1, :, z, LO:HI + 8, :] + (27.0 - CENTER)
                )
                F[1, :, z, LO:HI + 8, :] = F[0, :, z, LO:HI + 8, :]

        for f in range(2):
            V0[f] = F[f, :, S:S + BZ, MID:MID + 8, :]
        for degree in range(1, S + 1):
            rows = (LO, 24) if degree < S else (MID, 8)
            power_steps(read_p, write_p, degree, degree, NZE - degree, rows)
            if degree < S:
                rows = (LO, 24) if degree < S - 1 else (MID, 8)
                power_steps(read_r, write_r, degree, degree + 1, NZE - degree - 1, rows)

        parts = [None] * (NPP + NPR + NRR)

        def add(k, a, b):
            s = jnp.sum(a * b, axis=0)
            parts[k] = s if parts[k] is None else parts[k] + s

        for xt in range(2):
            p, r = own(0, 0, xt), own(1, 0, xt)
            for i in range(S + 1):
                p_next = own(0, i + 1, xt) if i < S else None
                r_next = own(1, i + 1, xt) if i < S - 1 else None
                add(2 * i, p, p)
                if i < S:
                    add(2 * i + 1, p, p_next)
                    add(NPP + 2 * i, p, r)
                    add(NPP + 2 * i + 1, p_next, r)
                    add(NPP + NPR + 2 * i, r, r)
                if i < S - 1:
                    add(NPP + NPR + 2 * i + 1, r, r_next)
                p, r = p_next, r_next
        picked = jnp.zeros((8, 128), jnp.float32)
        for k, part in enumerate(parts):
            picked = jnp.where(lane8 == k, jnp.sum(part, axis=1, keepdims=True), picked)
        local = jnp.sum(picked, axis=0, keepdims=True)

        me1 = 8 * py + yv
        S1[par, me1] = local
        for to in plane:
            pltpu.make_async_remote_copy(
                src_ref=S1.at[par, me1], dst_ref=S1.at[par, me1],
                send_sem=g1_s.at[par], recv_sem=g1_r.at[par],
                device_id=to, device_id_type=MESH,
            ).start()
        whole1 = pltpu.make_async_copy(S1.at[par, pl.ds(0, 31)], S1.at[par, pl.ds(0, 31)], g1_r.at[par])
        whole1.wait()
        S2[par, pz] = jnp.sum(S1[par], axis=0)
        for to in line:
            pltpu.make_async_remote_copy(
                src_ref=S2.at[par, pz], dst_ref=S2.at[par, pz],
                send_sem=g2_s.at[par], recv_sem=g2_r.at[par],
                device_id=to, device_id_type=MESH,
            ).start()
        whole2 = pltpu.make_async_copy(S2.at[par, pl.ds(0, 7)], S2.at[par, pl.ds(0, 7)], g2_r.at[par])
        whole2.wait()
        moments = jnp.broadcast_to(jnp.sum(S2[par], axis=0), (8, 128))
        pltpu.make_async_copy(S1.at[par, pl.ds(0, 31)], S1.at[par, pl.ds(0, 31)], g1_s.at[par]).wait()
        pltpu.make_async_copy(S2.at[par, pl.ds(0, 7)], S2.at[par, pl.ds(0, 7)], g2_s.at[par]).wait()

        columns = 2 * S + 1
        table = [
            [
                [
                    jnp.broadcast_to(jnp.sum(w_ref[which, j, half] * moments, axis=1, keepdims=True), (8, 128))
                    for half in range(PARTS)
                ]
                for j in range(columns)
            ]
            for which in range(2)
        ]

        def form(which, v):
            col = [splat(v[place(j)[0]], place(j)[1]) for j in range(columns)]
            total = None
            for half in range(PARTS):
                terms = [table[which][j][half] * col[j] for j in range(columns)]
                while len(terms) > 1:
                    terms = [
                        terms[i] + terms[i + 1] if i + 1 < len(terms) else terms[i] for i in range(0, len(terms), 2)
                    ]
                part = terms[0] * v[half]
                total = part if total is None else total + part
            return all_sublanes(total)

        unit = jnp.where(sub8 == 0, 1.0, 0.0)
        none = jnp.zeros((8, 128), jnp.float32)
        p_c, r_c, x_c = ([unit] + [none] * (PARTS - 1), [none, unit] + [none] * (PARTS - 2), [none] * PARTS)
        norm = form(0, r_c)
        for step in range(S):
            q = [
                diag_c[h] * p_c[h] + from_low[h] * pltpu.roll(p_c[h], 1, 0) + from_high[h] * pltpu.roll(p_c[h], 7, 0)
                for h in range(2)
            ]
            if PARTS == 3:
                q.append(jnp.where(sub8 == 0, 0.5 * HALF * splat(p_c[0], 7), 0.0))
            length = norm / form(1, p_c)
            r_next = [r_c[h] - length * q[h] for h in range(PARTS)]
            norm_next = form(0, r_next)
            ratio = norm_next / norm
            new = (
                [x_c[h] + length * p_c[h] for h in range(PARTS)] + r_next
                + [r_next[h] + ratio * p_c[h] for h in range(PARTS)] + [norm_next]
            )
            count = sum(inner > step for inner in INNER)
            if count < len(INNER):
                keep = jnp.full((8, 128), t, jnp.int32) < count
                new = [jnp.where(keep, a, b) for a, b in zip(new, x_c + r_c + p_c + [norm])]
            x_c, r_c, p_c, norm = new[:PARTS], new[PARTS:2 * PARTS], new[2 * PARTS:3 * PARTS], new[-1]

        for xt in range(2):
            F[0, xt, S:S + BZ, MID:MID + 8, :] = combine(p_c, xt)
            F[1, xt, S:S + BZ, MID:MID + 8, :] = combine(r_c, xt)
        for h in range(PARTS):
            XC[h] = x_c[h]
        return carry

    lax.fori_loop(0, len(INNER), outer, 0)

    def back(f, src):
        return pltpu.make_async_remote_copy(
            src_ref=src, dst_ref=land.at[f],
            send_sem=io_s.at[2 + f], recv_sem=io_r.at[2 + f],
            device_id=(gz, gy, sib), device_id_type=MESH,
        )

    res_back = back(1, F.at[1, sib, own_z, own_rows, :])
    res_back.start()
    for xt in range(2):
        X[xt] = X[xt] + combine([XC[h] for h in range(PARTS)], xt)
    sol_back = back(0, X.at[sib])
    sol_back.start()
    res_ref[:, mine, :] = F[1, gx, S:S + BZ, MID:MID + 8, :]
    sol_ref[:, mine, :] = X[gx]
    for f, (cp, out) in enumerate(((sol_back, sol_ref), (res_back, res_ref))):
        cp.wait()
        out[:, other, :] = land[f]


def solution(mesh):
    table = weights()

    def local(right_side, diagonal):
        f32 = jnp.float32
        dma = pltpu.SemaphoreType.DMA
        field = (2, NZE, ROWS, 128)
        return pl.pallas_call(
            kernel,
            out_shape=(jax.ShapeDtypeStruct(right_side.shape, f32),) * 2,
            in_specs=[pl.BlockSpec(memory_space=pltpu.HBM)] * 3,
            out_specs=(pl.BlockSpec(memory_space=pltpu.VMEM),) * 2,
            scratch_shapes=[
                pltpu.VMEM((2,) + field, f32),
                pltpu.VMEM((S,) + field, f32),
                pltpu.VMEM((S - 1,) + field, f32),
                pltpu.VMEM(field, f32),
                pltpu.VMEM((NZE, 24, 128), f32),
                pltpu.VMEM((2, 2, BZ, 8, 128), f32),
                pltpu.VMEM((2, BZ, 8, 128), f32),
                pltpu.VMEM((PARTS, 8, 128), f32),
                pltpu.VMEM((2, BZ, 8, 128), f32),
                pltpu.VMEM((2, 32, 1, 128), f32),
                pltpu.VMEM((2, 8, 1, 128), f32),
                pltpu.VMEM(table.shape, f32),
                dma((5,)), dma((2,)), dma((2,)), dma((2,)), dma((2,)), dma((2,)), dma((2,)), dma((2,)), dma((2,)),
                dma((4,)), dma((4,)), dma((2,)), dma((2,)), dma((2,)), dma((2,)),
            ],
            compiler_params=pltpu.CompilerParams(collective_id=0, has_side_effects=True, vmem_limit_bytes=67043328),
        )(right_side, diagonal, jnp.asarray(table))

    spec = P("gz", "gy", "gx")
    return jax.shard_map(
        local, mesh=mesh, in_specs=(spec, spec), out_specs=(spec, spec), check_vma=False
    )
```

```python
import functools

import jax
import jax.numpy as jnp
import numpy as np
from jax import lax
from jax.experimental import pallas as pl
from jax.experimental.pallas import tpu as pltpu
from jax.sharding import PartitionSpec as P

S = 8
INNER = (8, 8, 7, 7)
MESH = pl.DeviceIdType.MESH

CENTER = 19.0
HALF = 19.0

BZ = 8
NZE = BZ + 2 * S
ROWS = 40
LO, MID, HI = 8, 16, 24

NPP, NPR, NRR = 2 * S + 1, 2 * S, 2 * S - 1

PARTS = 3 if S == 8 else 2


def place(i):
    if i > S:
        return 1, i - S - 1
    return (0, i) if i < 8 else (2, i - 8)


def weights():
    columns = 2 * S + 1
    total = NPP + NPR + NRR

    def moment(offset, m):
        v = np.zeros(total)
        if m < 2:
            v[offset + m] = 1.0
        else:
            v[offset + m] = 2.0
            v[offset + m % 2] -= 1.0
        return v

    gram = np.zeros((columns, columns, total))
    for i in range(columns):
        for j in range(columns):
            di, dj = (i if i <= S else i - S - 1), (j if j <= S else j - S - 1)
            kinds = (i > S) + (j > S)
            offset = (0, NPP, NPP + NPR)[kinds]
            gram[i, j] = (moment(offset, di + dj) + moment(offset, abs(di - dj))) / 2
    out = np.zeros((columns, PARTS, 8, 128), np.float32)
    for j in range(columns):
        for i in range(columns):
            half, row = place(i)
            out[j, half, row, :total] = gram[i, j]
    return out


def kernel(
    rhs_ref, diag_ref, w_hbm, sol_ref, res_ref,
    F, PV, RV, C, M, V0, X, XC, land, S1, S2, w_ref,
    in_sem, zs_sem, zr_sem, ys_sem, yr_sem, cs_sem, cr_sem, fs_sem, fr_sem, io_s, io_r, g1_s, g1_r, g2_s, g2_r,
):
    gz = lax.axis_index("gz")
    gy = lax.axis_index("gy")
    gx = lax.axis_index("gx")
    nz = lax.axis_size("gz")
    ny = lax.axis_size("gy")
    yv = 2 * gy + gx
    nyv = 2 * ny
    sib = 1 - gx
    nzp = 8
    py = gz // nzp
    pz = gz % nzp

    own_rows = pl.ds(MID, 8)
    own_z = pl.ds(S, BZ)
    mine = pl.ds(pl.multiple_of(8 * gx, 8), 8)
    other = pl.ds(pl.multiple_of(8 * sib, 8), 8)

    loads = []
    for f, ref in enumerate((rhs_ref, diag_ref)):
        loads.append(pltpu.make_async_copy(ref.at[:, other, :], land.at[f], in_sem.at[f]))
    for f, ref in enumerate((rhs_ref, diag_ref)):
        loads.append(pltpu.make_async_copy(ref.at[:, mine, :], F.at[f, gx, own_z, own_rows, :], in_sem.at[2 + f]))
    loads.append(pltpu.make_async_copy(w_hbm, w_ref, in_sem.at[4]))
    for cp in loads:
        cp.start()

    plane = [
        (((py + dy) % 4) * nzp + pz, (gy + dx) % 4, (gx + dc) % 2)
        for dy in range(4) for dx in range(4) for dc in range(2) if dy or dx or dc
    ]
    line = [(py * nzp + (pz + dz) % nzp, gy, gx) for dz in range(1, nzp)]
    off_gy = gy + 2 * gx - 1
    has_off = (off_gy >= 0) & (off_gy < ny)
    to_z = (gz > 0, gz < nz - 1)
    from_z = (gz < nz - 1, gz > 0)

    barrier = pltpu.get_barrier_semaphore()
    for to in plane + line:
        pl.semaphore_signal(barrier, inc=1, device_id=to, device_id_type=MESH)
    for k, dz in enumerate((-1, 1)):
        @pl.when(to_z[k])
        def _(dz=dz):
            pl.semaphore_signal(barrier, inc=1, device_id=(gz + dz, gy, gx), device_id_type=MESH)

        @pl.when(to_z[k] & has_off)
        def _(dz=dz):
            pl.semaphore_signal(barrier, inc=1, device_id=(gz + dz, off_gy, sib), device_id_type=MESH)

    @pl.when(gz == 0)
    def _():
        F[:, :, 0:S, :, :] = jnp.zeros((2, 2, S, ROWS, 128), jnp.float32)

    @pl.when(gz == nz - 1)
    def _():
        F[:, :, S + BZ:NZE, :, :] = jnp.zeros((2, 2, S, ROWS, 128), jnp.float32)

    @pl.when(yv == 0)
    def _():
        F[:, :, :, LO:MID, :] = jnp.zeros((2, 2, NZE, 8, 128), jnp.float32)

    @pl.when(yv == nyv - 1)
    def _():
        F[:, :, :, HI:HI + 8, :] = jnp.zeros((2, 2, NZE, 8, 128), jnp.float32)

    X[...] = jnp.zeros(X.shape, jnp.float32)

    row = lax.broadcasted_iota(jnp.int32, (24, 128), 0) + (8 * yv - 8)
    row_in = jnp.where((row >= 0) & (row < 8 * nyv), 2.0 / HALF, 0.0)
    for z in range(NZE):
        at = gz * BZ + (z - S)
        M[z] = row_in * jnp.where((at >= 0) & (at < nz * BZ), 1.0, 0.0)

    nz_near = jnp.where(gz > 0, 1, 0) + jnp.where(gz < nz - 1, 1, 0)
    pl.semaphore_wait(barrier, len(plane) + len(line) + nz_near * jnp.where(has_off, 2, 1))
    swaps = []
    for f in range(2):
        loads[f].wait()
        cp = pltpu.make_async_remote_copy(
            src_ref=land.at[f],
            dst_ref=F.at[f, gx, own_z, own_rows, :],
            send_sem=io_s.at[f], recv_sem=io_r.at[f],
            device_id=(gz, gy, sib), device_id_type=MESH,
        )
        cp.start()
        swaps.append(cp)
    for cp in loads[2:] + swaps:
        cp.wait()

    lane = lax.broadcasted_iota(jnp.int32, (24, 128), 1)

    def x_sum(v, rows):
        first = lane[:rows] == 0
        last = lane[:rows] == 127
        a0, a1 = pltpu.roll(v[0], 1, 1), pltpu.roll(v[1], 1, 1)
        b0, b1 = pltpu.roll(v[0], 127, 1), pltpu.roll(v[1], 127, 1)
        zero = jnp.zeros((rows, 128), jnp.float32)
        s0 = v[0] + jnp.where(first, zero, a0) + jnp.where(last, b1, b0)
        s1 = v[1] + jnp.where(first, a0, a1) + jnp.where(last, zero, b1)
        return s0, s1

    off_rows = pl.ds(pl.multiple_of(LO + 16 * sib, 8), 8)
    sib_rows = pl.ds(pl.multiple_of(LO + 16 * gx, 8), 8)
    bands = (pl.ds(S + BZ, S), pl.ds(0, S))
    edges = (pl.ds(S, S), pl.ds(BZ, S))
    near = (gz - 1, gz + 1)

    def remote(src_planes, dst_planes, dst_rows, send, recv, to):
        return pltpu.make_async_remote_copy(
            src_ref=F.at[:, :, src_planes, own_rows, :], dst_ref=F.at[:, :, dst_planes, dst_rows, :],
            send_sem=send, recv_sem=recv, device_id=to, device_id_type=MESH,
        )

    def z_copy(k):
        return remote(edges[k], bands[k], own_rows, zs_sem.at[k], zr_sem.at[k], (near[k], gy, gx))

    def corner(k):
        return remote(edges[k], bands[k], off_rows, cs_sem.at[k], cr_sem.at[k], (near[k], off_gy, sib))

    def forward(k):
        return remote(bands[k], bands[k], sib_rows, fs_sem.at[k], fr_sem.at[k], (gz, gy, sib))

    y_off = remote(own_z, own_z, off_rows, ys_sem.at[0], yr_sem.at[0], (gz, off_gy, sib))
    y_sib = remote(own_z, own_z, sib_rows, ys_sem.at[1], yr_sem.at[1], (gz, gy, sib))

    def exchange_start():
        for k in range(2):
            @pl.when(to_z[k])
            def _(k=k):
                z_copy(k).start()

        @pl.when(has_off)
        def _():
            y_off.start()
        for k in range(2):
            @pl.when(to_z[k] & has_off)
            def _(k=k):
                corner(k).start()
        y_sib.start()

    def exchange_finish():
        for k in range(2):
            @pl.when(from_z[k])
            def _(k=k):
                z_copy(k).wait_recv()
                forward(k).start()
        y_sib.wait_recv()

        @pl.when(has_off)
        def _():
            y_off.wait_recv()
        for k in range(2):
            @pl.when(from_z[k])
            def _(k=k):
                forward(k).wait_recv()

            @pl.when(from_z[k] & has_off)
            def _(k=k):
                corner(k).wait_recv()
        y_sib.wait_send()

        @pl.when(has_off)
        def _():
            y_off.wait_send()
        for k in range(2):
            @pl.when(to_z[k])
            def _(k=k):
                z_copy(k).wait_send()

            @pl.when(to_z[k] & has_off)
            def _(k=k):
                corner(k).wait_send()

            @pl.when(from_z[k])
            def _(k=k):
                forward(k).wait_send()

    def power_steps(read, write, degree, z0, z1, rows):
        r0, n = rows
        m0 = r0 - LO
        sums = {}

        def y_sum(z):
            if z not in sums:
                sums[z] = (
                    read(degree - 1, z, r0 - 1, n) + read(degree - 1, z, r0, n) + read(degree - 1, z, r0 + 1, n)
                )
            return sums[z]

        for z in range(z0, z1):
            s0, s1 = x_sum(y_sum(z - 1) + y_sum(z) + y_sum(z + 1), n)
            sums.pop(z - 1, None)
            mask = M[z, m0:m0 + n, :]
            box = jnp.stack([s0 * mask, s1 * mask])
            value = C[:, z, r0:r0 + n, :] * read(degree - 1, z, r0, n) - box
            if degree == 1:
                value = 0.5 * value
            else:
                value = value - read(degree - 2, z, r0, n)
            write(degree, z, r0, n, value)

    def reader(f, V):
        def read(degree, z, r, n):
            if degree == 0:
                return F[f, :, z, r:r + n, :]
            return V[degree - 1, :, z, r:r + n, :]
        return read

    def writer(V):
        def write(degree, z, r, n, value):
            V[degree - 1, :, z, r:r + n, :] = value
        return write

    read_p, read_r = reader(0, PV), reader(1, RV)
    write_p, write_r = writer(PV), writer(RV)

    def own(block, degree, xt):
        if degree == 0:
            return V0[block, xt]
        V = (PV, RV)[block]
        return V[degree - 1, xt, S:S + BZ, MID:MID + 8, :]

    lane8 = lax.broadcasted_iota(jnp.int32, (8, 128), 1)
    sub8 = lax.broadcasted_iota(jnp.int32, (8, 128), 0)

    def all_sublanes(v):
        v = v + pltpu.roll(v, 4, 0)
        v = v + pltpu.roll(v, 2, 0)
        return v + pltpu.roll(v, 1, 0)

    def exact_sum(pairs):
        while len(pairs) > 1:
            joined = []
            for (a, ea), (b, eb) in zip(pairs[::2], pairs[1::2]):
                t = a + b
                back = t - a
                err = (a - (t - back)) + (b - back)
                joined.append((t, err if ea is None else err + (ea + eb)))
            pairs = joined
        return pairs[0]

    def splat(v, j):
        return jnp.broadcast_to(v[j:j + 1, :], (8, 128))

    def by_row(values):
        out = jnp.zeros((8, 128), jnp.float32)
        for j, value in enumerate(values):
            if value:
                out = jnp.where(sub8 == j, value, out)
        return out

    diag_c = (by_row([CENTER] * S), by_row([CENTER] * (S - 1)))
    from_low = (by_row([0.0, HALF] + [0.5 * HALF] * (S - 1)), by_row([0.0, HALF] + [0.5 * HALF] * (S - 2)))
    from_high = (by_row([0.5 * HALF] * (S - 1)), by_row([0.5 * HALF] * (S - 2)))

    def combine(c, xt):
        total = None
        for block in range(2):
            for degree in range(S + 1 - block):
                half, row = place(degree + block * (S + 1))
                term = splat(c[half], row)[None] * own(block, degree, xt)
                total = term if total is None else total + term
        return total

    def outer(t, carry):
        par = t % 2
        exchange_start()

        @pl.when(t > 0)
        def _():
            for xt in range(2):
                X[xt] = X[xt] + combine([XC[h] for h in range(PARTS)], xt)
        exchange_finish()

        @pl.when(t == 0)
        def _():
            for z in range(NZE):
                C[:, z, LO:HI + 8, :] = (2.0 / HALF) * (
                    F[1, :, z, LO:HI + 8, :] + (27.0 - CENTER)
                )
                F[1, :, z, LO:HI + 8, :] = F[0, :, z, LO:HI + 8, :]

        for f in range(2):
            V0[f] = F[f, :, S:S + BZ, MID:MID + 8, :]
        for degree in range(1, S + 1):
            rows = (LO, 24) if degree < S else (MID, 8)
            power_steps(read_p, write_p, degree, degree, NZE - degree, rows)
            if degree < S:
                rows = (LO, 24) if degree < S - 1 else (MID, 8)
                power_steps(read_r, write_r, degree, degree + 1, NZE - degree - 1, rows)

        parts = [None] * (NPP + NPR + NRR)

        def add(k, a, b):
            s = jnp.sum(a * b, axis=0)
            parts[k] = s if parts[k] is None else parts[k] + s

        for xt in range(2):
            p, r = own(0, 0, xt), own(1, 0, xt)
            for i in range(S + 1):
                p_next = own(0, i + 1, xt) if i < S else None
                r_next = own(1, i + 1, xt) if i < S - 1 else None
                add(2 * i, p, p)
                if i < S:
                    add(2 * i + 1, p, p_next)
                    add(NPP + 2 * i, p, r)
                    add(NPP + 2 * i + 1, p_next, r)
                    add(NPP + NPR + 2 * i, r, r)
                if i < S - 1:
                    add(NPP + NPR + 2 * i + 1, r, r_next)
                p, r = p_next, r_next
        picked = jnp.zeros((8, 128), jnp.float32)
        for k, part in enumerate(parts):
            picked = jnp.where(lane8 == k, jnp.sum(part, axis=1, keepdims=True), picked)
        local = jnp.sum(picked, axis=0, keepdims=True)

        me1 = 8 * py + yv
        S1[par, me1] = local
        for to in plane:
            pltpu.make_async_remote_copy(
                src_ref=S1.at[par, me1], dst_ref=S1.at[par, me1],
                send_sem=g1_s.at[par], recv_sem=g1_r.at[par],
                device_id=to, device_id_type=MESH,
            ).start()
        whole1 = pltpu.make_async_copy(S1.at[par, pl.ds(0, 31)], S1.at[par, pl.ds(0, 31)], g1_r.at[par])
        whole1.wait()
        S2[par, pz] = jnp.concatenate(exact_sum([(S1[par, i], None) for i in range(32)]), axis=0)
        for to in line:
            pltpu.make_async_remote_copy(
                src_ref=S2.at[par, pz], dst_ref=S2.at[par, pz],
                send_sem=g2_s.at[par], recv_sem=g2_r.at[par],
                device_id=to, device_id_type=MESH,
            ).start()
        whole2 = pltpu.make_async_copy(S2.at[par, pl.ds(0, 7)], S2.at[par, pl.ds(0, 7)], g2_r.at[par])
        whole2.wait()
        high, low = exact_sum([(S2[par, i, 0:1], S2[par, i, 1:2]) for i in range(nzp)])
        lead = high.astype(jnp.bfloat16).astype(jnp.float32)
        rest = (high - lead) + low
        lead, rest = jnp.broadcast_to(lead, (8, 128)), jnp.broadcast_to(rest, (8, 128))
        pltpu.make_async_copy(S1.at[par, pl.ds(0, 31)], S1.at[par, pl.ds(0, 31)], g1_s.at[par]).wait()
        pltpu.make_async_copy(S2.at[par, pl.ds(0, 7)], S2.at[par, pl.ds(0, 7)], g2_s.at[par]).wait()

        columns = 2 * S + 1

        def lanes(v):
            return jnp.broadcast_to(jnp.sum(v, axis=1, keepdims=True), (8, 128))

        table = [
            [lanes(w_ref[j, half] * lead) + lanes(w_ref[j, half] * rest) for half in range(PARTS)]
            for j in range(columns)
        ]

        def form(u, v):
            col = [splat(v[place(j)[0]], place(j)[1]) for j in range(columns)]
            total = None
            for half in range(PARTS):
                terms = [table[j][half] * col[j] for j in range(columns)]
                while len(terms) > 1:
                    terms = [
                        terms[i] + terms[i + 1] if i + 1 < len(terms) else terms[i] for i in range(0, len(terms), 2)
                    ]
                part = terms[0] * u[half]
                total = part if total is None else total + part
            return all_sublanes(total)

        unit = jnp.where(sub8 == 0, 1.0, 0.0)
        none = jnp.zeros((8, 128), jnp.float32)
        p_c, r_c, x_c = ([unit] + [none] * (PARTS - 1), [none, unit] + [none] * (PARTS - 2), [none] * PARTS)
        norm = form(r_c, r_c)
        for step in range(S):
            q = [
                diag_c[h] * p_c[h] + from_low[h] * pltpu.roll(p_c[h], 1, 0) + from_high[h] * pltpu.roll(p_c[h], 7, 0)
                for h in range(2)
            ]
            if PARTS == 3:
                q.append(jnp.where(sub8 == 0, 0.5 * HALF * splat(p_c[0], 7), 0.0))
            length = norm / form(p_c, q)
            r_next = [r_c[h] - length * q[h] for h in range(PARTS)]
            norm_next = form(r_next, r_next)
            ratio = norm_next / norm
            new = (
                [x_c[h] + length * p_c[h] for h in range(PARTS)] + r_next
                + [r_next[h] + ratio * p_c[h] for h in range(PARTS)] + [norm_next]
            )
            count = sum(inner > step for inner in INNER)
            if count < len(INNER):
                keep = jnp.full((8, 128), t, jnp.int32) < count
                new = [jnp.where(keep, a, b) for a, b in zip(new, x_c + r_c + p_c + [norm])]
            x_c, r_c, p_c, norm = new[:PARTS], new[PARTS:2 * PARTS], new[2 * PARTS:3 * PARTS], new[-1]

        for xt in range(2):
            F[0, xt, S:S + BZ, MID:MID + 8, :] = combine(p_c, xt)
            F[1, xt, S:S + BZ, MID:MID + 8, :] = combine(r_c, xt)
        for h in range(PARTS):
            XC[h] = x_c[h]
        return carry

    lax.fori_loop(0, len(INNER), outer, 0)

    def back(f, src):
        return pltpu.make_async_remote_copy(
            src_ref=src, dst_ref=land.at[f],
            send_sem=io_s.at[2 + f], recv_sem=io_r.at[2 + f],
            device_id=(gz, gy, sib), device_id_type=MESH,
        )

    res_back = back(1, F.at[1, sib, own_z, own_rows, :])
    res_back.start()
    for xt in range(2):
        X[xt] = X[xt] + combine([XC[h] for h in range(PARTS)], xt)
    sol_back = back(0, X.at[sib])
    sol_back.start()
    res_ref[:, mine, :] = F[1, gx, S:S + BZ, MID:MID + 8, :]
    sol_ref[:, mine, :] = X[gx]
    for f, (cp, out) in enumerate(((sol_back, sol_ref), (res_back, res_ref))):
        cp.wait()
        out[:, other, :] = land[f]


def solution(mesh):
    table = weights()

    def local(right_side, diagonal):
        f32 = jnp.float32
        dma = pltpu.SemaphoreType.DMA
        field = (2, NZE, ROWS, 128)
        return pl.pallas_call(
            kernel,
            out_shape=(jax.ShapeDtypeStruct(right_side.shape, f32),) * 2,
            in_specs=[pl.BlockSpec(memory_space=pltpu.HBM)] * 3,
            out_specs=(pl.BlockSpec(memory_space=pltpu.VMEM),) * 2,
            scratch_shapes=[
                pltpu.VMEM((2,) + field, f32),
                pltpu.VMEM((S,) + field, f32),
                pltpu.VMEM((S - 1,) + field, f32),
                pltpu.VMEM(field, f32),
                pltpu.VMEM((NZE, 24, 128), f32),
                pltpu.VMEM((2, 2, BZ, 8, 128), f32),
                pltpu.VMEM((2, BZ, 8, 128), f32),
                pltpu.VMEM((PARTS, 8, 128), f32),
                pltpu.VMEM((2, BZ, 8, 128), f32),
                pltpu.VMEM((2, 32, 1, 128), f32),
                pltpu.VMEM((2, 8, 2, 128), f32),
                pltpu.VMEM(table.shape, f32),
                dma((5,)), dma((2,)), dma((2,)), dma((2,)), dma((2,)), dma((2,)), dma((2,)), dma((2,)), dma((2,)),
                dma((4,)), dma((4,)), dma((2,)), dma((2,)), dma((2,)), dma((2,)),
            ],
            compiler_params=pltpu.CompilerParams(collective_id=0, has_side_effects=True, vmem_limit_bytes=67043328),
        )(right_side, diagonal, jnp.asarray(table))

    spec = P("gz", "gy", "gx")
    return jax.shard_map(
        local, mesh=mesh, in_specs=(spec, spec), out_specs=(spec, spec), check_vma=False
    )
```

```python
import functools

import jax
import jax.numpy as jnp
import numpy as np
from jax import lax
from jax.experimental import pallas as pl
from jax.experimental.pallas import tpu as pltpu
from jax.sharding import PartitionSpec as P

S = 8
INNER = (8, 8, 7, 7)
MESH = pl.DeviceIdType.MESH

CENTER = 19.0
HALF = 19.0

BZ = 8
NZE = BZ + 2 * S
ROWS = 40
LO, MID, HI = 8, 16, 24

NPP, NPR, NRR = 2 * S + 1, 2 * S, 2 * S - 1

PARTS = 3 if S == 8 else 2


def place(i):
    if i > S:
        return 1, i - S - 1
    return (0, i) if i < 8 else (2, i - 8)


def weights():
    columns = 2 * S + 1
    total = NPP + NPR + NRR

    def moment(offset, m):
        v = np.zeros(total)
        if m < 2:
            v[offset + m] = 1.0
        else:
            v[offset + m] = 2.0
            v[offset + m % 2] -= 1.0
        return v

    gram = np.zeros((columns, columns, total))
    for i in range(columns):
        for j in range(columns):
            di, dj = (i if i <= S else i - S - 1), (j if j <= S else j - S - 1)
            kinds = (i > S) + (j > S)
            offset = (0, NPP, NPP + NPR)[kinds]
            gram[i, j] = (moment(offset, di + dj) + moment(offset, abs(di - dj))) / 2
    out = np.zeros((columns, PARTS, 8, 128), np.float32)
    for j in range(columns):
        for i in range(columns):
            half, row = place(i)
            out[j, half, row, :total] = gram[i, j]
    return out


def kernel(
    rhs_ref, diag_ref, w_hbm, sol_ref, res_ref,
    F, PV, RV, C, M, V0, X, XC, land, S1, S2, w_ref,
    in_sem, zs_sem, zr_sem, ys_sem, yr_sem, cs_sem, cr_sem, fs_sem, fr_sem, io_s, io_r, g1_s, g1_r, g2_s, g2_r,
):
    gz = lax.axis_index("gz")
    gy = lax.axis_index("gy")
    gx = lax.axis_index("gx")
    nz = lax.axis_size("gz")
    ny = lax.axis_size("gy")
    yv = 2 * gy + gx
    nyv = 2 * ny
    sib = 1 - gx
    nzp = 8
    py = gz // nzp
    pz = gz % nzp

    own_rows = pl.ds(MID, 8)
    own_z = pl.ds(S, BZ)
    mine = pl.ds(pl.multiple_of(8 * gx, 8), 8)
    other = pl.ds(pl.multiple_of(8 * sib, 8), 8)

    loads = []
    for f, ref in enumerate((rhs_ref, diag_ref)):
        loads.append(pltpu.make_async_copy(ref.at[:, other, :], land.at[f], in_sem.at[f]))
    for f, ref in enumerate((rhs_ref, diag_ref)):
        loads.append(pltpu.make_async_copy(ref.at[:, mine, :], F.at[f, gx, own_z, own_rows, :], in_sem.at[2 + f]))
    loads.append(pltpu.make_async_copy(w_hbm, w_ref, in_sem.at[4]))
    for cp in loads:
        cp.start()

    plane = [
        (((py + dy) % 4) * nzp + pz, (gy + dx) % 4, (gx + dc) % 2)
        for dy in range(4) for dx in range(4) for dc in range(2) if dy or dx or dc
    ]
    line = [(py * nzp + (pz + dz) % nzp, gy, gx) for dz in range(1, nzp)]
    off_gy = gy + 2 * gx - 1
    has_off = (off_gy >= 0) & (off_gy < ny)
    to_z = (gz > 0, gz < nz - 1)
    from_z = (gz < nz - 1, gz > 0)

    barrier = pltpu.get_barrier_semaphore()
    for to in plane + line:
        pl.semaphore_signal(barrier, inc=1, device_id=to, device_id_type=MESH)
    for k, dz in enumerate((-1, 1)):
        @pl.when(to_z[k])
        def _(dz=dz):
            pl.semaphore_signal(barrier, inc=1, device_id=(gz + dz, gy, gx), device_id_type=MESH)

        @pl.when(to_z[k] & has_off)
        def _(dz=dz):
            pl.semaphore_signal(barrier, inc=1, device_id=(gz + dz, off_gy, sib), device_id_type=MESH)

    @pl.when(gz == 0)
    def _():
        F[:, :, 0:S, :, :] = jnp.zeros((2, 2, S, ROWS, 128), jnp.float32)

    @pl.when(gz == nz - 1)
    def _():
        F[:, :, S + BZ:NZE, :, :] = jnp.zeros((2, 2, S, ROWS, 128), jnp.float32)

    @pl.when(yv == 0)
    def _():
        F[:, :, :, LO:MID, :] = jnp.zeros((2, 2, NZE, 8, 128), jnp.float32)

    @pl.when(yv == nyv - 1)
    def _():
        F[:, :, :, HI:HI + 8, :] = jnp.zeros((2, 2, NZE, 8, 128), jnp.float32)

    X[...] = jnp.zeros(X.shape, jnp.float32)

    row = lax.broadcasted_iota(jnp.int32, (24, 128), 0) + (8 * yv - 8)
    row_in = jnp.where((row >= 0) & (row < 8 * nyv), 2.0 / HALF, 0.0)
    for z in range(NZE):
        at = gz * BZ + (z - S)
        M[z] = row_in * jnp.where((at >= 0) & (at < nz * BZ), 1.0, 0.0)

    nz_near = jnp.where(gz > 0, 1, 0) + jnp.where(gz < nz - 1, 1, 0)
    pl.semaphore_wait(barrier, len(plane) + len(line) + nz_near * jnp.where(has_off, 2, 1))
    swaps = []
    for f in range(2):
        loads[f].wait()
        cp = pltpu.make_async_remote_copy(
            src_ref=land.at[f],
            dst_ref=F.at[f, gx, own_z, own_rows, :],
            send_sem=io_s.at[f], recv_sem=io_r.at[f],
            device_id=(gz, gy, sib), device_id_type=MESH,
        )
        cp.start()
        swaps.append(cp)
    for cp in loads[2:] + swaps:
        cp.wait()

    lane = lax.broadcasted_iota(jnp.int32, (24, 128), 1)

    def x_sum(v, rows):
        first = lane[:rows] == 0
        last = lane[:rows] == 127
        a0, a1 = pltpu.roll(v[0], 1, 1), pltpu.roll(v[1], 1, 1)
        b0, b1 = pltpu.roll(v[0], 127, 1), pltpu.roll(v[1], 127, 1)
        zero = jnp.zeros((rows, 128), jnp.float32)
        s0 = v[0] + jnp.where(first, zero, a0) + jnp.where(last, b1, b0)
        s1 = v[1] + jnp.where(first, a0, a1) + jnp.where(last, zero, b1)
        return s0, s1

    off_rows = pl.ds(pl.multiple_of(LO + 16 * sib, 8), 8)
    sib_rows = pl.ds(pl.multiple_of(LO + 16 * gx, 8), 8)
    near = (gz - 1, gz + 1)

    def bands(k, f):
        return (pl.ds(S + BZ, S - f), pl.ds(f, S - f))[k]

    def edges(k, f):
        return (pl.ds(S, S - f), pl.ds(BZ + f, S - f))[k]

    def remote(f, src_planes, dst_planes, dst_rows, send, recv, to):
        return pltpu.make_async_remote_copy(
            src_ref=F.at[f, :, src_planes, own_rows, :], dst_ref=F.at[f, :, dst_planes, dst_rows, :],
            send_sem=send, recv_sem=recv, device_id=to, device_id_type=MESH,
        )

    def z_copy(k, f):
        return remote(f, edges(k, f), bands(k, f), own_rows, zs_sem.at[k, f], zr_sem.at[k, f], (near[k], gy, gx))

    def corner(k, f):
        return remote(
            f, edges(k, f), bands(k, f), off_rows, cs_sem.at[k, f], cr_sem.at[k, f], (near[k], off_gy, sib)
        )

    def forward(k, f):
        return remote(f, bands(k, f), bands(k, f), sib_rows, fs_sem.at[k, f], fr_sem.at[k, f], (gz, gy, sib))

    def y_off(f):
        return remote(f, own_z, own_z, off_rows, ys_sem.at[0, f], yr_sem.at[0, f], (gz, off_gy, sib))

    def y_sib(f):
        return remote(f, own_z, own_z, sib_rows, ys_sem.at[1, f], yr_sem.at[1, f], (gz, gy, sib))

    def exchange_start():
        for k in range(2):
            @pl.when(to_z[k])
            def _(k=k):
                for f in range(2):
                    z_copy(k, f).start()

        @pl.when(has_off)
        def _():
            for f in range(2):
                y_off(f).start()
        for k in range(2):
            @pl.when(to_z[k] & has_off)
            def _(k=k):
                for f in range(2):
                    corner(k, f).start()
        for f in range(2):
            y_sib(f).start()

    def exchange_finish():
        for f in range(2):
            for k in range(2):
                @pl.when(from_z[k])
                def _(k=k, f=f):
                    z_copy(k, f).wait_recv()
                    forward(k, f).start()
        for f in range(2):
            y_sib(f).wait_recv()

        @pl.when(has_off)
        def _():
            for f in range(2):
                y_off(f).wait_recv()
        for k in range(2):
            @pl.when(from_z[k])
            def _(k=k):
                for f in range(2):
                    forward(k, f).wait_recv()

            @pl.when(from_z[k] & has_off)
            def _(k=k):
                for f in range(2):
                    corner(k, f).wait_recv()

    def exchange_sent():
        for f in range(2):
            y_sib(f).wait_send()

        @pl.when(has_off)
        def _():
            for f in range(2):
                y_off(f).wait_send()
        for k in range(2):
            @pl.when(to_z[k])
            def _(k=k):
                for f in range(2):
                    z_copy(k, f).wait_send()

            @pl.when(to_z[k] & has_off)
            def _(k=k):
                for f in range(2):
                    corner(k, f).wait_send()

            @pl.when(from_z[k])
            def _(k=k):
                for f in range(2):
                    forward(k, f).wait_send()

    def power_steps(read, write, degree, z0, z1, rows):
        r0, n = rows
        m0 = r0 - LO
        sums = {}

        def y_sum(z):
            if z not in sums:
                sums[z] = (
                    read(degree - 1, z, r0 - 1, n) + read(degree - 1, z, r0, n) + read(degree - 1, z, r0 + 1, n)
                )
            return sums[z]

        for z in range(z0, z1):
            s0, s1 = x_sum(y_sum(z - 1) + y_sum(z) + y_sum(z + 1), n)
            sums.pop(z - 1, None)
            mask = M[z, m0:m0 + n, :]
            box = jnp.stack([s0 * mask, s1 * mask])
            value = C[:, z, r0:r0 + n, :] * read(degree - 1, z, r0, n) - box
            if degree == 1:
                value = 0.5 * value
            else:
                value = value - read(degree - 2, z, r0, n)
            write(degree, z, r0, n, value)

    def reader(f, V):
        def read(degree, z, r, n):
            if degree == 0:
                return F[f, :, z, r:r + n, :]
            return V[degree - 1, :, z, r:r + n, :]
        return read

    def writer(V):
        def write(degree, z, r, n, value):
            V[degree - 1, :, z, r:r + n, :] = value
        return write

    read_p, read_r = reader(0, PV), reader(1, RV)
    write_p, write_r = writer(PV), writer(RV)

    def own(block, degree, xt):
        if degree == 0:
            return V0[block, xt]
        V = (PV, RV)[block]
        return V[degree - 1, xt, S:S + BZ, MID:MID + 8, :]

    lane8 = lax.broadcasted_iota(jnp.int32, (8, 128), 1)
    sub8 = lax.broadcasted_iota(jnp.int32, (8, 128), 0)

    def all_sublanes(v):
        v = v + pltpu.roll(v, 4, 0)
        v = v + pltpu.roll(v, 2, 0)
        return v + pltpu.roll(v, 1, 0)

    def exact_sum(pairs):
        while len(pairs) > 1:
            joined = []
            for (a, ea), (b, eb) in zip(pairs[::2], pairs[1::2]):
                t = a + b
                back = t - a
                err = (a - (t - back)) + (b - back)
                joined.append((t, err if ea is None else err + (ea + eb)))
            pairs = joined
        return pairs[0]

    def splat(v, j):
        return jnp.broadcast_to(v[j:j + 1, :], (8, 128))

    def by_row(values):
        out = jnp.zeros((8, 128), jnp.float32)
        for j, value in enumerate(values):
            if value:
                out = jnp.where(sub8 == j, value, out)
        return out

    diag_c = (by_row([CENTER] * S), by_row([CENTER] * (S - 1)))
    from_low = (by_row([0.0, HALF] + [0.5 * HALF] * (S - 1)), by_row([0.0, HALF] + [0.5 * HALF] * (S - 2)))
    from_high = (by_row([0.5 * HALF] * (S - 1)), by_row([0.5 * HALF] * (S - 2)))

    def combine(c, xt):
        total = None
        for block in range(2):
            for degree in range(S + 1 - block):
                half, row = place(degree + block * (S + 1))
                term = splat(c[half], row)[None] * own(block, degree, xt)
                total = term if total is None else total + term
        return total

    def outer(t, carry):
        par = t % 2
        exchange_start()

        @pl.when(t > 0)
        def _():
            for xt in range(2):
                X[xt] = X[xt] + combine([XC[h] for h in range(PARTS)], xt)
        exchange_finish()

        @pl.when(t == 0)
        def _():
            exchange_sent()
            for z in range(NZE):
                C[:, z, LO:HI + 8, :] = (2.0 / HALF) * (
                    F[1, :, z, LO:HI + 8, :] + (27.0 - CENTER)
                )
                F[1, :, z, LO:HI + 8, :] = F[0, :, z, LO:HI + 8, :]

        for f in range(2):
            V0[f] = F[f, :, S:S + BZ, MID:MID + 8, :]
        def window(margin):
            return (LO, 24) if margin > 4 else (MID - 4, 16) if margin else (MID, 8)

        for degree in range(1, S + 1):
            power_steps(read_p, write_p, degree, degree, NZE - degree, window(S - degree))
            if degree < S:
                power_steps(read_r, write_r, degree, degree + 1, NZE - degree - 1, window(S - 1 - degree))

        parts = [None] * (NPP + NPR + NRR)

        def add(k, a, b):
            s = jnp.sum(a * b, axis=0)
            parts[k] = s if parts[k] is None else parts[k] + s

        for xt in range(2):
            p, r = own(0, 0, xt), own(1, 0, xt)
            for i in range(S + 1):
                p_next = own(0, i + 1, xt) if i < S else None
                r_next = own(1, i + 1, xt) if i < S - 1 else None
                add(2 * i, p, p)
                if i < S:
                    add(2 * i + 1, p, p_next)
                    add(NPP + 2 * i, p, r)
                    add(NPP + 2 * i + 1, p_next, r)
                    add(NPP + NPR + 2 * i, r, r)
                if i < S - 1:
                    add(NPP + NPR + 2 * i + 1, r, r_next)
                p, r = p_next, r_next
        picked = jnp.zeros((8, 128), jnp.float32)
        for k, part in enumerate(parts):
            picked = jnp.where(lane8 == k, jnp.sum(part, axis=1, keepdims=True), picked)
        local = jnp.sum(picked, axis=0, keepdims=True)

        me1 = 8 * py + yv
        @pl.when(t > 0)
        def _():
            exchange_sent()
        S1[par, me1] = local
        for to in plane:
            pltpu.make_async_remote_copy(
                src_ref=S1.at[par, me1], dst_ref=S1.at[par, me1],
                send_sem=g1_s.at[par], recv_sem=g1_r.at[par],
                device_id=to, device_id_type=MESH,
            ).start()
        whole1 = pltpu.make_async_copy(S1.at[par, pl.ds(0, 31)], S1.at[par, pl.ds(0, 31)], g1_r.at[par])
        whole1.wait()
        S2[par, pz] = jnp.concatenate(exact_sum([(S1[par, i], None) for i in range(32)]), axis=0)
        for to in line:
            pltpu.make_async_remote_copy(
                src_ref=S2.at[par, pz], dst_ref=S2.at[par, pz],
                send_sem=g2_s.at[par], recv_sem=g2_r.at[par],
                device_id=to, device_id_type=MESH,
            ).start()
        whole2 = pltpu.make_async_copy(S2.at[par, pl.ds(0, 7)], S2.at[par, pl.ds(0, 7)], g2_r.at[par])
        whole2.wait()
        high, low = exact_sum([(S2[par, i, 0:1], S2[par, i, 1:2]) for i in range(nzp)])
        lead = high.astype(jnp.bfloat16).astype(jnp.float32)
        rest = (high - lead) + low
        lead, rest = jnp.broadcast_to(lead, (8, 128)), jnp.broadcast_to(rest, (8, 128))
        pltpu.make_async_copy(S1.at[par, pl.ds(0, 31)], S1.at[par, pl.ds(0, 31)], g1_s.at[par]).wait()
        pltpu.make_async_copy(S2.at[par, pl.ds(0, 7)], S2.at[par, pl.ds(0, 7)], g2_s.at[par]).wait()

        columns = 2 * S + 1

        def lanes(v):
            return jnp.broadcast_to(jnp.sum(v, axis=1, keepdims=True), (8, 128))

        table = [
            [lanes(w_ref[j, half] * lead) + lanes(w_ref[j, half] * rest) for half in range(PARTS)]
            for j in range(columns)
        ]

        def form(u, v):
            col = [splat(v[place(j)[0]], place(j)[1]) for j in range(columns)]
            total = None
            for half in range(PARTS):
                terms = [table[j][half] * col[j] for j in range(columns)]
                while len(terms) > 1:
                    terms = [
                        terms[i] + terms[i + 1] if i + 1 < len(terms) else terms[i] for i in range(0, len(terms), 2)
                    ]
                part = terms[0] * u[half]
                total = part if total is None else total + part
            return all_sublanes(total)

        unit = jnp.where(sub8 == 0, 1.0, 0.0)
        none = jnp.zeros((8, 128), jnp.float32)
        p_c, r_c, x_c = ([unit] + [none] * (PARTS - 1), [none, unit] + [none] * (PARTS - 2), [none] * PARTS)
        norm = form(r_c, r_c)
        for step in range(S):
            q = [
                diag_c[h] * p_c[h] + from_low[h] * pltpu.roll(p_c[h], 1, 0) + from_high[h] * pltpu.roll(p_c[h], 7, 0)
                for h in range(2)
            ]
            if PARTS == 3:
                q.append(jnp.where(sub8 == 0, 0.5 * HALF * splat(p_c[0], 7), 0.0))
            length = norm / form(p_c, q)
            r_next = [r_c[h] - length * q[h] for h in range(PARTS)]
            norm_next = form(r_next, r_next)
            ratio = norm_next / norm
            new = (
                [x_c[h] + length * p_c[h] for h in range(PARTS)] + r_next
                + [r_next[h] + ratio * p_c[h] for h in range(PARTS)] + [norm_next]
            )
            count = sum(inner > step for inner in INNER)
            if count < len(INNER):
                keep = jnp.full((8, 128), t, jnp.int32) < count
                new = [jnp.where(keep, a, b) for a, b in zip(new, x_c + r_c + p_c + [norm])]
            x_c, r_c, p_c, norm = new[:PARTS], new[PARTS:2 * PARTS], new[2 * PARTS:3 * PARTS], new[-1]

        for xt in range(2):
            F[0, xt, S:S + BZ, MID:MID + 8, :] = combine(p_c, xt)
            F[1, xt, S:S + BZ, MID:MID + 8, :] = combine(r_c, xt)
        for h in range(PARTS):
            XC[h] = x_c[h]
        return carry

    lax.fori_loop(0, len(INNER), outer, 0)

    def back(f, src):
        return pltpu.make_async_remote_copy(
            src_ref=src, dst_ref=land.at[f],
            send_sem=io_s.at[2 + f], recv_sem=io_r.at[2 + f],
            device_id=(gz, gy, sib), device_id_type=MESH,
        )

    res_back = back(1, F.at[1, sib, own_z, own_rows, :])
    res_back.start()
    for xt in range(2):
        X[xt] = X[xt] + combine([XC[h] for h in range(PARTS)], xt)
    sol_back = back(0, X.at[sib])
    sol_back.start()
    res_ref[:, mine, :] = F[1, gx, S:S + BZ, MID:MID + 8, :]
    sol_ref[:, mine, :] = X[gx]
    for f, (cp, out) in enumerate(((sol_back, sol_ref), (res_back, res_ref))):
        cp.wait()
        out[:, other, :] = land[f]


def solution(mesh):
    table = weights()

    def local(right_side, diagonal):
        f32 = jnp.float32
        dma = pltpu.SemaphoreType.DMA
        field = (2, NZE, ROWS, 128)
        return pl.pallas_call(
            kernel,
            out_shape=(jax.ShapeDtypeStruct(right_side.shape, f32),) * 2,
            in_specs=[pl.BlockSpec(memory_space=pltpu.HBM)] * 3,
            out_specs=(pl.BlockSpec(memory_space=pltpu.VMEM),) * 2,
            scratch_shapes=[
                pltpu.VMEM((2,) + field, f32),
                pltpu.VMEM((S,) + field, f32),
                pltpu.VMEM((S - 1,) + field, f32),
                pltpu.VMEM(field, f32),
                pltpu.VMEM((NZE, 24, 128), f32),
                pltpu.VMEM((2, 2, BZ, 8, 128), f32),
                pltpu.VMEM((2, BZ, 8, 128), f32),
                pltpu.VMEM((PARTS, 8, 128), f32),
                pltpu.VMEM((2, BZ, 8, 128), f32),
                pltpu.VMEM((2, 32, 1, 128), f32),
                pltpu.VMEM((2, 8, 2, 128), f32),
                pltpu.VMEM(table.shape, f32),
                dma((5,)), dma((2, 2)), dma((2, 2)), dma((2, 2)), dma((2, 2)), dma((2, 2)), dma((2, 2)), dma((2, 2)), dma((2, 2)),
                dma((4,)), dma((4,)), dma((2,)), dma((2,)), dma((2,)), dma((2,)),
            ],
            compiler_params=pltpu.CompilerParams(collective_id=0, has_side_effects=True, vmem_limit_bytes=48 * 2**20),
        )(*(pltpu.with_memory_space_constraint(v, pltpu.HBM) for v in (right_side, diagonal, jnp.asarray(table))))

    spec = P("gz", "gy", "gx")
    return jax.shard_map(
        local, mesh=mesh, in_specs=(spec, spec), out_specs=(spec, spec), check_vma=False
    )
```

```python
import functools

import jax
import jax.numpy as jnp
import numpy as np
from jax import lax
from jax.experimental import pallas as pl
from jax.experimental.pallas import tpu as pltpu
from jax.sharding import PartitionSpec as P

S = 8
INNER = (8, 8, 7, 7)
MESH = pl.DeviceIdType.MESH

CENTER = 19.0
HALF = 19.0

BZ = 8
NZE = BZ + 2 * S
ROWS = 40
LO, MID, HI = 8, 16, 24

NPP, NPR, NRR = 2 * S + 1, 2 * S, 2 * S - 1

PARTS = 3 if S == 8 else 2


def place(i):
    if i > S:
        return 1, i - S - 1
    return (0, i) if i < 8 else (2, i - 8)


def weights():
    columns = 2 * S + 1
    total = NPP + NPR + NRR

    def moment(offset, m):
        v = np.zeros(total)
        if m < 2:
            v[offset + m] = 1.0
        else:
            v[offset + m] = 2.0
            v[offset + m % 2] -= 1.0
        return v

    gram = np.zeros((columns, columns, total))
    for i in range(columns):
        for j in range(columns):
            di, dj = (i if i <= S else i - S - 1), (j if j <= S else j - S - 1)
            kinds = (i > S) + (j > S)
            offset = (0, NPP, NPP + NPR)[kinds]
            gram[i, j] = (moment(offset, di + dj) + moment(offset, abs(di - dj))) / 2
    out = np.zeros((columns, PARTS, 8, 128), np.float32)
    for j in range(columns):
        for i in range(columns):
            half, row = place(i)
            out[j, half, row, :total] = gram[i, j]
    return out


def kernel(
    rhs_ref, diag_ref, w_hbm, sol_ref, res_ref,
    F, PV, RV, C, M, V0, X, XC, land, S1, S2, w_ref,
    in_sem, zs_sem, zr_sem, ys_sem, yr_sem, cs_sem, cr_sem, fs_sem, fr_sem, io_s, io_r, g1_s, g1_r, g2_s, g2_r,
):
    gz = lax.axis_index("gz")
    gy = lax.axis_index("gy")
    gx = lax.axis_index("gx")
    nz = lax.axis_size("gz")
    ny = lax.axis_size("gy")
    yv = 2 * gy + gx
    nyv = 2 * ny
    sib = 1 - gx
    nzp = 8
    py = gz // nzp
    pz = gz % nzp

    own_rows = pl.ds(MID, 8)
    own_z = pl.ds(S, BZ)
    mine = pl.ds(pl.multiple_of(8 * gx, 8), 8)
    other = pl.ds(pl.multiple_of(8 * sib, 8), 8)

    loads = []
    for f, ref in enumerate((rhs_ref, diag_ref)):
        loads.append(pltpu.make_async_copy(ref.at[:, other, :], land.at[f], in_sem.at[f]))
    for f, ref in enumerate((rhs_ref, diag_ref)):
        loads.append(pltpu.make_async_copy(ref.at[:, mine, :], F.at[f, gx, own_z, own_rows, :], in_sem.at[2 + f]))
    loads.append(pltpu.make_async_copy(w_hbm, w_ref, in_sem.at[4]))
    for cp in loads:
        cp.start()

    plane = [
        (((py + dy) % 4) * nzp + pz, (gy + dx) % 4, (gx + dc) % 2)
        for dy in range(4) for dx in range(4) for dc in range(2) if dy or dx or dc
    ]
    line = [(py * nzp + (pz + dz) % nzp, gy, gx) for dz in range(1, nzp)]
    off_gy = gy + 2 * gx - 1
    has_off = (off_gy >= 0) & (off_gy < ny)
    to_z = (gz > 0, gz < nz - 1)
    from_z = (gz < nz - 1, gz > 0)

    barrier = pltpu.get_barrier_semaphore()
    for to in plane + line:
        pl.semaphore_signal(barrier, inc=1, device_id=to, device_id_type=MESH)
    for k, dz in enumerate((-1, 1)):
        @pl.when(to_z[k])
        def _(dz=dz):
            pl.semaphore_signal(barrier, inc=1, device_id=(gz + dz, gy, gx), device_id_type=MESH)

        @pl.when(to_z[k] & has_off)
        def _(dz=dz):
            pl.semaphore_signal(barrier, inc=1, device_id=(gz + dz, off_gy, sib), device_id_type=MESH)

    @pl.when(gz == 0)
    def _():
        F[:, :, 0:S, :, :] = jnp.zeros((2, 2, S, ROWS, 128), jnp.float32)

    @pl.when(gz == nz - 1)
    def _():
        F[:, :, S + BZ:NZE, :, :] = jnp.zeros((2, 2, S, ROWS, 128), jnp.float32)

    @pl.when(yv == 0)
    def _():
        F[:, :, :, LO:MID, :] = jnp.zeros((2, 2, NZE, 8, 128), jnp.float32)

    @pl.when(yv == nyv - 1)
    def _():
        F[:, :, :, HI:HI + 8, :] = jnp.zeros((2, 2, NZE, 8, 128), jnp.float32)

    X[...] = jnp.zeros(X.shape, jnp.float32)

    row = lax.broadcasted_iota(jnp.int32, (24, 128), 0) + (8 * yv - 8)
    row_in = jnp.where((row >= 0) & (row < 8 * nyv), 2.0 / HALF, 0.0)
    for z in range(NZE):
        at = gz * BZ + (z - S)
        M[z] = row_in * jnp.where((at >= 0) & (at < nz * BZ), 1.0, 0.0)

    nz_near = jnp.where(gz > 0, 1, 0) + jnp.where(gz < nz - 1, 1, 0)
    pl.semaphore_wait(barrier, len(plane) + len(line) + nz_near * jnp.where(has_off, 2, 1))
    swaps = []
    for f in range(2):
        loads[f].wait()
        cp = pltpu.make_async_remote_copy(
            src_ref=land.at[f],
            dst_ref=F.at[f, gx, own_z, own_rows, :],
            send_sem=io_s.at[f], recv_sem=io_r.at[f],
            device_id=(gz, gy, sib), device_id_type=MESH,
        )
        cp.start()
        swaps.append(cp)
    for cp in loads[2:] + swaps:
        cp.wait()

    lane = lax.broadcasted_iota(jnp.int32, (24, 128), 1)

    def x_sum(v, rows):
        both = v[0] + v[1]
        s0 = both + jnp.where(lane[:rows] == 0, 0.0, pltpu.roll(v[1], 1, 1))
        s1 = both + jnp.where(lane[:rows] == 127, 0.0, pltpu.roll(v[0], 127, 1))
        return s0, s1

    def reorder(pair, order):
        n = pair[0].shape[0]
        wide = jnp.concatenate([pair[0].reshape(8 * n, 128), pair[1].reshape(8 * n, 128)], axis=1)
        out = jnp.dot(wide, order, precision=lax.Precision.HIGHEST, preferred_element_type=jnp.float32)
        return [out[:, 128 * h:128 * (h + 1)].reshape(n, 8, 128) for h in range(2)]

    at_i = lax.broadcasted_iota(jnp.int32, (256, 256), 0)
    at_j = lax.broadcasted_iota(jnp.int32, (256, 256), 1)
    to_stored = jnp.where(at_i == 2 * (at_j & 127) + (at_j >> 7), 1.0, 0.0)
    to_natural = jnp.where(at_j == 2 * (at_i & 127) + (at_i >> 7), 1.0, 0.0)
    for f in range(2):
        halves = reorder(F[f, :, S:S + BZ, MID:MID + 8, :], to_stored)
        for xt in range(2):
            F[f, xt, S:S + BZ, MID:MID + 8, :] = halves[xt]

    off_rows = pl.ds(pl.multiple_of(LO + 16 * sib, 8), 8)
    sib_rows = pl.ds(pl.multiple_of(LO + 16 * gx, 8), 8)
    near = (gz - 1, gz + 1)

    def bands(k, f):
        return (pl.ds(S + BZ, S - f), pl.ds(f, S - f))[k]

    def edges(k, f):
        return (pl.ds(S, S - f), pl.ds(BZ + f, S - f))[k]

    def remote(f, src_planes, dst_planes, dst_rows, send, recv, to):
        return pltpu.make_async_remote_copy(
            src_ref=F.at[f, :, src_planes, own_rows, :], dst_ref=F.at[f, :, dst_planes, dst_rows, :],
            send_sem=send, recv_sem=recv, device_id=to, device_id_type=MESH,
        )

    def z_copy(k, f):
        return remote(f, edges(k, f), bands(k, f), own_rows, zs_sem.at[k, f], zr_sem.at[k, f], (near[k], gy, gx))

    def corner(k, f):
        return remote(
            f, edges(k, f), bands(k, f), off_rows, cs_sem.at[k, f], cr_sem.at[k, f], (near[k], off_gy, sib)
        )

    def forward(k, f):
        return remote(f, bands(k, f), bands(k, f), sib_rows, fs_sem.at[k, f], fr_sem.at[k, f], (gz, gy, sib))

    def y_off(f):
        return remote(f, own_z, own_z, off_rows, ys_sem.at[0, f], yr_sem.at[0, f], (gz, off_gy, sib))

    def y_sib(f):
        return remote(f, own_z, own_z, sib_rows, ys_sem.at[1, f], yr_sem.at[1, f], (gz, gy, sib))

    def exchange_start():
        for k in range(2):
            @pl.when(to_z[k])
            def _(k=k):
                for f in range(2):
                    z_copy(k, f).start()

        @pl.when(has_off)
        def _():
            for f in range(2):
                y_off(f).start()
        for k in range(2):
            @pl.when(to_z[k] & has_off)
            def _(k=k):
                for f in range(2):
                    corner(k, f).start()
        for f in range(2):
            y_sib(f).start()

    def exchange_finish():
        for f in range(2):
            for k in range(2):
                @pl.when(from_z[k])
                def _(k=k, f=f):
                    z_copy(k, f).wait_recv()
                    forward(k, f).start()
        for f in range(2):
            y_sib(f).wait_recv()

        @pl.when(has_off)
        def _():
            for f in range(2):
                y_off(f).wait_recv()
        for k in range(2):
            @pl.when(from_z[k])
            def _(k=k):
                for f in range(2):
                    forward(k, f).wait_recv()

            @pl.when(from_z[k] & has_off)
            def _(k=k):
                for f in range(2):
                    corner(k, f).wait_recv()

    def exchange_sent():
        for f in range(2):
            y_sib(f).wait_send()

        @pl.when(has_off)
        def _():
            for f in range(2):
                y_off(f).wait_send()
        for k in range(2):
            @pl.when(to_z[k])
            def _(k=k):
                for f in range(2):
                    z_copy(k, f).wait_send()

            @pl.when(to_z[k] & has_off)
            def _(k=k):
                for f in range(2):
                    corner(k, f).wait_send()

            @pl.when(from_z[k])
            def _(k=k):
                for f in range(2):
                    forward(k, f).wait_send()

    def power_steps(read, write, degree, z0, z1, rows):
        r0, n = rows
        m0 = r0 - LO
        sums = {}

        def y_sum(z):
            if z not in sums:
                sums[z] = (
                    read(degree - 1, z, r0 - 1, n) + read(degree - 1, z, r0, n) + read(degree - 1, z, r0 + 1, n)
                )
            return sums[z]

        shared = None
        for z in range(z0, z1):
            if shared is None:
                shared = y_sum(z) + y_sum(z + 1)
                s0, s1 = x_sum(shared + y_sum(z - 1), n)
            else:
                s0, s1 = x_sum(shared + y_sum(z + 1), n)
                shared = None
            sums.pop(z - 1, None)
            mask = M[z, m0:m0 + n, :]
            box = jnp.stack([s0 * mask, s1 * mask])
            value = C[:, z, r0:r0 + n, :] * read(degree - 1, z, r0, n) - box
            if degree == 1:
                value = 0.5 * value
            else:
                value = value - read(degree - 2, z, r0, n)
            write(degree, z, r0, n, value)

    def reader(f, V):
        def read(degree, z, r, n):
            if degree == 0:
                return F[f, :, z, r:r + n, :]
            return V[degree - 1, :, z, r:r + n, :]
        return read

    def writer(V):
        def write(degree, z, r, n, value):
            V[degree - 1, :, z, r:r + n, :] = value
        return write

    read_p, read_r = reader(0, PV), reader(1, RV)
    write_p, write_r = writer(PV), writer(RV)

    def own(block, degree, xt):
        if degree == 0:
            return V0[block, xt]
        V = (PV, RV)[block]
        return V[degree - 1, xt, S:S + BZ, MID:MID + 8, :]

    lane8 = lax.broadcasted_iota(jnp.int32, (8, 128), 1)
    sub8 = lax.broadcasted_iota(jnp.int32, (8, 128), 0)

    def all_sublanes(v):
        v = v + pltpu.roll(v, 4, 0)
        v = v + pltpu.roll(v, 2, 0)
        return v + pltpu.roll(v, 1, 0)

    def exact_sum(pairs):
        while len(pairs) > 1:
            joined = []
            for (a, ea), (b, eb) in zip(pairs[::2], pairs[1::2]):
                t = a + b
                back = t - a
                err = (a - (t - back)) + (b - back)
                joined.append((t, err if ea is None else err + (ea + eb)))
            pairs = joined
        return pairs[0]

    def splat(v, j):
        return jnp.broadcast_to(v[j:j + 1, :], (8, 128))

    def by_row(values):
        out = jnp.zeros((8, 128), jnp.float32)
        for j, value in enumerate(values):
            if value:
                out = jnp.where(sub8 == j, value, out)
        return out

    diag_c = (by_row([CENTER] * S), by_row([CENTER] * (S - 1)))
    from_low = (by_row([0.0, HALF] + [0.5 * HALF] * (S - 1)), by_row([0.0, HALF] + [0.5 * HALF] * (S - 2)))
    from_high = (by_row([0.5 * HALF] * (S - 1)), by_row([0.5 * HALF] * (S - 2)))

    def combine(c, xt):
        total = None
        for block in range(2):
            for degree in range(S + 1 - block):
                half, row = place(degree + block * (S + 1))
                term = splat(c[half], row)[None] * own(block, degree, xt)
                total = term if total is None else total + term
        return total

    def outer(t, carry):
        par = t % 2
        exchange_start()

        @pl.when(t > 0)
        def _():
            for xt in range(2):
                X[xt] = X[xt] + combine([XC[h] for h in range(PARTS)], xt)
        exchange_finish()

        @pl.when(t == 0)
        def _():
            exchange_sent()
            for z in range(NZE):
                C[:, z, LO:HI + 8, :] = (2.0 / HALF) * (
                    F[1, :, z, LO:HI + 8, :] + (27.0 - CENTER)
                )
                F[1, :, z, LO:HI + 8, :] = F[0, :, z, LO:HI + 8, :]

        for f in range(2):
            V0[f] = F[f, :, S:S + BZ, MID:MID + 8, :]
        def window(margin):
            return (LO, 24) if margin > 4 else (MID - 4, 16) if margin else (MID, 8)

        for degree in range(1, S + 1):
            power_steps(read_p, write_p, degree, degree, NZE - degree, window(S - degree))
            if degree < S:
                power_steps(read_r, write_r, degree, degree + 1, NZE - degree - 1, window(S - 1 - degree))

        parts = [None] * (NPP + NPR + NRR)

        def add(k, a, b):
            s = jnp.sum(a * b, axis=0)
            parts[k] = s if parts[k] is None else parts[k] + s

        for xt in range(2):
            p, r = own(0, 0, xt), own(1, 0, xt)
            for i in range(S + 1):
                p_next = own(0, i + 1, xt) if i < S else None
                r_next = own(1, i + 1, xt) if i < S - 1 else None
                add(2 * i, p, p)
                if i < S:
                    add(2 * i + 1, p, p_next)
                    add(NPP + 2 * i, p, r)
                    add(NPP + 2 * i + 1, p_next, r)
                    add(NPP + NPR + 2 * i, r, r)
                if i < S - 1:
                    add(NPP + NPR + 2 * i + 1, r, r_next)
                p, r = p_next, r_next
        picked = jnp.zeros((8, 128), jnp.float32)
        for k, part in enumerate(parts):
            picked = jnp.where(lane8 == k, jnp.sum(part, axis=1, keepdims=True), picked)
        local = jnp.sum(picked, axis=0, keepdims=True)

        me1 = 8 * py + yv
        @pl.when(t > 0)
        def _():
            exchange_sent()
        S1[par, me1] = local
        for to in plane:
            pltpu.make_async_remote_copy(
                src_ref=S1.at[par, me1], dst_ref=S1.at[par, me1],
                send_sem=g1_s.at[par], recv_sem=g1_r.at[par],
                device_id=to, device_id_type=MESH,
            ).start()
        whole1 = pltpu.make_async_copy(S1.at[par, pl.ds(0, 31)], S1.at[par, pl.ds(0, 31)], g1_r.at[par])
        whole1.wait()
        S2[par, pz] = jnp.concatenate(exact_sum([(S1[par, i], None) for i in range(32)]), axis=0)
        for to in line:
            pltpu.make_async_remote_copy(
                src_ref=S2.at[par, pz], dst_ref=S2.at[par, pz],
                send_sem=g2_s.at[par], recv_sem=g2_r.at[par],
                device_id=to, device_id_type=MESH,
            ).start()
        whole2 = pltpu.make_async_copy(S2.at[par, pl.ds(0, 7)], S2.at[par, pl.ds(0, 7)], g2_r.at[par])
        whole2.wait()
        high, low = exact_sum([(S2[par, i, 0:1], S2[par, i, 1:2]) for i in range(nzp)])
        lead = high.astype(jnp.bfloat16).astype(jnp.float32)
        rest = (high - lead) + low
        lead, rest = jnp.broadcast_to(lead, (8, 128)), jnp.broadcast_to(rest, (8, 128))
        pltpu.make_async_copy(S1.at[par, pl.ds(0, 31)], S1.at[par, pl.ds(0, 31)], g1_s.at[par]).wait()
        pltpu.make_async_copy(S2.at[par, pl.ds(0, 7)], S2.at[par, pl.ds(0, 7)], g2_s.at[par]).wait()

        columns = 2 * S + 1

        def lanes(v):
            return jnp.broadcast_to(jnp.sum(v, axis=1, keepdims=True), (8, 128))

        table = [
            [lanes(w_ref[j, half] * lead) + lanes(w_ref[j, half] * rest) for half in range(PARTS)]
            for j in range(columns)
        ]

        def form(u, v):
            col = [splat(v[place(j)[0]], place(j)[1]) for j in range(columns)]
            total = None
            for half in range(PARTS):
                terms = [table[j][half] * col[j] for j in range(columns)]
                while len(terms) > 1:
                    terms = [
                        terms[i] + terms[i + 1] if i + 1 < len(terms) else terms[i] for i in range(0, len(terms), 2)
                    ]
                part = terms[0] * u[half]
                total = part if total is None else total + part
            return all_sublanes(total)

        unit = jnp.where(sub8 == 0, 1.0, 0.0)
        none = jnp.zeros((8, 128), jnp.float32)
        p_c, r_c, x_c = ([unit] + [none] * (PARTS - 1), [none, unit] + [none] * (PARTS - 2), [none] * PARTS)
        norm = form(r_c, r_c)
        for step in range(S):
            q = [
                diag_c[h] * p_c[h] + from_low[h] * pltpu.roll(p_c[h], 1, 0) + from_high[h] * pltpu.roll(p_c[h], 7, 0)
                for h in range(2)
            ]
            if PARTS == 3:
                q.append(jnp.where(sub8 == 0, 0.5 * HALF * splat(p_c[0], 7), 0.0))
            length = norm / form(p_c, q)
            r_next = [r_c[h] - length * q[h] for h in range(PARTS)]
            norm_next = form(r_next, r_next)
            ratio = norm_next / norm
            new = (
                [x_c[h] + length * p_c[h] for h in range(PARTS)] + r_next
                + [r_next[h] + ratio * p_c[h] for h in range(PARTS)] + [norm_next]
            )
            count = sum(inner > step for inner in INNER)
            if count < len(INNER):
                keep = jnp.full((8, 128), t, jnp.int32) < count
                new = [jnp.where(keep, a, b) for a, b in zip(new, x_c + r_c + p_c + [norm])]
            x_c, r_c, p_c, norm = new[:PARTS], new[PARTS:2 * PARTS], new[2 * PARTS:3 * PARTS], new[-1]

        for xt in range(2):
            F[0, xt, S:S + BZ, MID:MID + 8, :] = combine(p_c, xt)
            F[1, xt, S:S + BZ, MID:MID + 8, :] = combine(r_c, xt)
        for h in range(PARTS):
            XC[h] = x_c[h]
        return carry

    lax.fori_loop(0, len(INNER), outer, 0)

    def back(f, src):
        return pltpu.make_async_remote_copy(
            src_ref=src, dst_ref=land.at[f],
            send_sem=io_s.at[2 + f], recv_sem=io_r.at[2 + f],
            device_id=(gz, gy, sib), device_id_type=MESH,
        )

    halves = reorder(F[1, :, S:S + BZ, MID:MID + 8, :], to_natural)
    for xt in range(2):
        F[1, xt, S:S + BZ, MID:MID + 8, :] = halves[xt]
    res_back = back(1, F.at[1, sib, own_z, own_rows, :])
    res_back.start()
    halves = reorder([X[xt] + combine([XC[h] for h in range(PARTS)], xt) for xt in range(2)], to_natural)
    for xt in range(2):
        X[xt] = halves[xt]
    sol_back = back(0, X.at[sib])
    sol_back.start()
    res_ref[:, mine, :] = F[1, gx, S:S + BZ, MID:MID + 8, :]
    sol_ref[:, mine, :] = X[gx]
    for f, (cp, out) in enumerate(((sol_back, sol_ref), (res_back, res_ref))):
        cp.wait()
        out[:, other, :] = land[f]


def solution(mesh):
    table = weights()

    def local(right_side, diagonal):
        f32 = jnp.float32
        dma = pltpu.SemaphoreType.DMA
        field = (2, NZE, ROWS, 128)
        return pl.pallas_call(
            kernel,
            out_shape=(jax.ShapeDtypeStruct(right_side.shape, f32),) * 2,
            in_specs=[pl.BlockSpec(memory_space=pltpu.HBM)] * 3,
            out_specs=(pl.BlockSpec(memory_space=pltpu.VMEM),) * 2,
            scratch_shapes=[
                pltpu.VMEM((2,) + field, f32),
                pltpu.VMEM((S,) + field, f32),
                pltpu.VMEM((S - 1,) + field, f32),
                pltpu.VMEM(field, f32),
                pltpu.VMEM((NZE, 24, 128), f32),
                pltpu.VMEM((2, 2, BZ, 8, 128), f32),
                pltpu.VMEM((2, BZ, 8, 128), f32),
                pltpu.VMEM((PARTS, 8, 128), f32),
                pltpu.VMEM((2, BZ, 8, 128), f32),
                pltpu.VMEM((2, 32, 1, 128), f32),
                pltpu.VMEM((2, 8, 2, 128), f32),
                pltpu.VMEM(table.shape, f32),
                dma((5,)), dma((2, 2)), dma((2, 2)), dma((2, 2)), dma((2, 2)), dma((2, 2)), dma((2, 2)), dma((2, 2)), dma((2, 2)),
                dma((4,)), dma((4,)), dma((2,)), dma((2,)), dma((2,)), dma((2,)),
            ],
            compiler_params=pltpu.CompilerParams(collective_id=0, has_side_effects=True, vmem_limit_bytes=48 * 2**20),
        )(*(pltpu.with_memory_space_constraint(v, pltpu.HBM) for v in (right_side, diagonal, jnp.asarray(table))))

    spec = P("gz", "gy", "gx")
    return jax.shard_map(
        local, mesh=mesh, in_specs=(spec, spec), out_specs=(spec, spec), check_vma=False
    )
```

```python
import functools

import jax
import jax.numpy as jnp
import numpy as np
from jax import lax
from jax.experimental import pallas as pl
from jax.experimental.pallas import tpu as pltpu
from jax.sharding import PartitionSpec as P

S = 8
INNER = (8, 8, 7, 7)
MESH = pl.DeviceIdType.MESH

CENTER = 19.0
HALF = 19.0

BZ = 8
NZE = BZ + 2 * S
ROWS = 40
LO, MID, HI = 8, 16, 24

NPP, NPR, NRR = 2 * S + 1, 2 * S, 2 * S - 1

PARTS = 3 if S == 8 else 2


def place(i):
    if i > S:
        return 1, i - S - 1
    return (0, i) if i < 8 else (2, i - 8)


def weights():
    columns = 2 * S + 1
    total = NPP + NPR + NRR

    def moment(offset, m):
        v = np.zeros(total)
        if m < 2:
            v[offset + m] = 1.0
        else:
            v[offset + m] = 2.0
            v[offset + m % 2] -= 1.0
        return v

    gram = np.zeros((columns, columns, total))
    for i in range(columns):
        for j in range(columns):
            di, dj = (i if i <= S else i - S - 1), (j if j <= S else j - S - 1)
            kinds = (i > S) + (j > S)
            offset = (0, NPP, NPP + NPR)[kinds]
            gram[i, j] = (moment(offset, di + dj) + moment(offset, abs(di - dj))) / 2
    out = np.zeros((columns, PARTS, 8, 128), np.float32)
    for j in range(columns):
        for i in range(columns):
            half, row = place(i)
            out[j, half, row, :total] = gram[i, j]
    return out


def kernel(
    rhs_ref, diag_ref, w_hbm, sol_ref, res_ref,
    F, PV, RV, C, M, V0, X, XC, land, S1, S2, w_ref,
    in_sem, zs_sem, zr_sem, ys_sem, yr_sem, cs_sem, cr_sem, fs_sem, fr_sem, io_s, io_r, g1_s, g1_r, g2_s, g2_r,
):
    gz = lax.axis_index("gz")
    gy = lax.axis_index("gy")
    gx = lax.axis_index("gx")
    nz = lax.axis_size("gz")
    ny = lax.axis_size("gy")
    yv = 2 * gy + gx
    nyv = 2 * ny
    sib = 1 - gx
    nzp = 8
    py = gz // nzp
    pz = gz % nzp

    own_rows = pl.ds(MID, 8)
    own_z = pl.ds(S, BZ)
    mine = pl.ds(pl.multiple_of(8 * gx, 8), 8)
    other = pl.ds(pl.multiple_of(8 * sib, 8), 8)

    loads = []
    for f, ref in enumerate((rhs_ref, diag_ref)):
        loads.append(pltpu.make_async_copy(ref.at[:, other, :], land.at[f], in_sem.at[f]))
    for f, ref in enumerate((rhs_ref, diag_ref)):
        loads.append(pltpu.make_async_copy(ref.at[:, mine, :], F.at[f, gx, own_z, own_rows, :], in_sem.at[2 + f]))
    loads.append(pltpu.make_async_copy(w_hbm, w_ref, in_sem.at[4]))
    for cp in loads:
        cp.start()

    plane = [
        (((py + dy) % 4) * nzp + pz, (gy + dx) % 4, (gx + dc) % 2)
        for dy in range(4) for dx in range(4) for dc in range(2) if dy or dx or dc
    ]
    line = [(py * nzp + (pz + dz) % nzp, gy, gx) for dz in range(1, nzp)]
    off_gy = gy + 2 * gx - 1
    has_off = (off_gy >= 0) & (off_gy < ny)
    to_z = (gz > 0, gz < nz - 1)
    from_z = (gz < nz - 1, gz > 0)

    barrier = pltpu.get_barrier_semaphore()
    for to in plane + line:
        pl.semaphore_signal(barrier, inc=1, device_id=to, device_id_type=MESH)
    for k, dz in enumerate((-1, 1)):
        @pl.when(to_z[k])
        def _(dz=dz):
            pl.semaphore_signal(barrier, inc=1, device_id=(gz + dz, gy, gx), device_id_type=MESH)

        @pl.when(to_z[k] & has_off)
        def _(dz=dz):
            pl.semaphore_signal(barrier, inc=1, device_id=(gz + dz, off_gy, sib), device_id_type=MESH)

    @pl.when(gz == 0)
    def _():
        F[:, :, 0:S, :, :] = jnp.zeros((2, 2, S, ROWS, 128), jnp.float32)

    @pl.when(gz == nz - 1)
    def _():
        F[:, :, S + BZ:NZE, :, :] = jnp.zeros((2, 2, S, ROWS, 128), jnp.float32)

    @pl.when(yv == 0)
    def _():
        F[:, :, :, LO:MID, :] = jnp.zeros((2, 2, NZE, 8, 128), jnp.float32)

    @pl.when(yv == nyv - 1)
    def _():
        F[:, :, :, HI:HI + 8, :] = jnp.zeros((2, 2, NZE, 8, 128), jnp.float32)

    X[...] = jnp.zeros(X.shape, jnp.float32)

    row = lax.broadcasted_iota(jnp.int32, (ROWS, 128), 0) + (8 * yv - MID)
    row_in = jnp.where((row >= 0) & (row < 8 * nyv), 2.0 / HALF, 0.0)
    for z in range(NZE):
        at = gz * BZ + (z - S)
        M[z] = row_in * jnp.where((at >= 0) & (at < nz * BZ), 1.0, 0.0)

    nz_near = jnp.where(gz > 0, 1, 0) + jnp.where(gz < nz - 1, 1, 0)
    pl.semaphore_wait(barrier, len(plane) + len(line) + nz_near * jnp.where(has_off, 2, 1))
    swaps = []
    for f in range(2):
        loads[f].wait()
        cp = pltpu.make_async_remote_copy(
            src_ref=land.at[f],
            dst_ref=F.at[f, gx, own_z, own_rows, :],
            send_sem=io_s.at[f], recv_sem=io_r.at[f],
            device_id=(gz, gy, sib), device_id_type=MESH,
        )
        cp.start()
        swaps.append(cp)
    for cp in loads[2:] + swaps:
        cp.wait()

    lane = lax.broadcasted_iota(jnp.int32, (24, 128), 1)

    def x_sum(v, rows):
        both = v[0] + v[1]
        s0 = both + jnp.where(lane[:rows] == 0, 0.0, pltpu.roll(v[1], 1, 1))
        s1 = both + jnp.where(lane[:rows] == 127, 0.0, pltpu.roll(v[0], 127, 1))
        return s0, s1

    def reorder(pair, order):
        n = pair[0].shape[0]
        wide = jnp.concatenate([pair[0].reshape(8 * n, 128), pair[1].reshape(8 * n, 128)], axis=1)
        out = jnp.dot(wide, order, precision=lax.Precision.HIGHEST, preferred_element_type=jnp.float32)
        return [out[:, 128 * h:128 * (h + 1)].reshape(n, 8, 128) for h in range(2)]

    at_i = lax.broadcasted_iota(jnp.int32, (256, 256), 0)
    at_j = lax.broadcasted_iota(jnp.int32, (256, 256), 1)
    to_stored = jnp.where(at_i == 2 * (at_j & 127) + (at_j >> 7), 1.0, 0.0)
    to_natural = jnp.where(at_j == 2 * (at_i & 127) + (at_i >> 7), 1.0, 0.0)
    for f in range(2):
        halves = reorder(F[f, :, S:S + BZ, MID:MID + 8, :], to_stored)
        for xt in range(2):
            F[f, xt, S:S + BZ, MID:MID + 8, :] = halves[xt]

    off_rows = pl.ds(pl.multiple_of(LO + 16 * sib, 8), 8)
    sib_rows = pl.ds(pl.multiple_of(LO + 16 * gx, 8), 8)
    near = (gz - 1, gz + 1)

    def bands(k, f):
        return (pl.ds(S + BZ, S - f), pl.ds(f, S - f))[k]

    def edges(k, f):
        return (pl.ds(S, S - f), pl.ds(BZ + f, S - f))[k]

    def remote(f, src_planes, dst_planes, dst_rows, send, recv, to):
        return pltpu.make_async_remote_copy(
            src_ref=F.at[f, :, src_planes, own_rows, :], dst_ref=F.at[f, :, dst_planes, dst_rows, :],
            send_sem=send, recv_sem=recv, device_id=to, device_id_type=MESH,
        )

    def z_copy(k, f):
        return remote(f, edges(k, f), bands(k, f), own_rows, zs_sem.at[k, f], zr_sem.at[k, f], (near[k], gy, gx))

    def corner(k, f):
        return remote(
            f, edges(k, f), bands(k, f), off_rows, cs_sem.at[k, f], cr_sem.at[k, f], (near[k], off_gy, sib)
        )

    def forward(k, f):
        return remote(f, bands(k, f), bands(k, f), sib_rows, fs_sem.at[k, f], fr_sem.at[k, f], (gz, gy, sib))

    def y_off(f):
        return remote(f, own_z, own_z, off_rows, ys_sem.at[0, f], yr_sem.at[0, f], (gz, off_gy, sib))

    def y_sib(f):
        return remote(f, own_z, own_z, sib_rows, ys_sem.at[1, f], yr_sem.at[1, f], (gz, gy, sib))

    def exchange_start():
        for k in range(2):
            @pl.when(to_z[k])
            def _(k=k):
                for f in range(2):
                    z_copy(k, f).start()

        @pl.when(has_off)
        def _():
            for f in range(2):
                y_off(f).start()
        for k in range(2):
            @pl.when(to_z[k] & has_off)
            def _(k=k):
                for f in range(2):
                    corner(k, f).start()
        for f in range(2):
            y_sib(f).start()

    def exchange_finish():
        for f in range(2):
            for k in range(2):
                @pl.when(from_z[k])
                def _(k=k, f=f):
                    z_copy(k, f).wait_recv()
                    forward(k, f).start()
        for f in range(2):
            y_sib(f).wait_recv()
        for k in range(2):
            @pl.when(from_z[k])
            def _(k=k):
                for f in range(2):
                    forward(k, f).wait_recv()

    def exchange_last():
        @pl.when(has_off)
        def _():
            for f in range(2):
                y_off(f).wait_recv()
        for k in range(2):
            @pl.when(from_z[k] & has_off)
            def _(k=k):
                for f in range(2):
                    corner(k, f).wait_recv()

    def exchange_sent():
        for f in range(2):
            y_sib(f).wait_send()

        @pl.when(has_off)
        def _():
            for f in range(2):
                y_off(f).wait_send()
        for k in range(2):
            @pl.when(to_z[k])
            def _(k=k):
                for f in range(2):
                    z_copy(k, f).wait_send()

            @pl.when(to_z[k] & has_off)
            def _(k=k):
                for f in range(2):
                    corner(k, f).wait_send()

            @pl.when(from_z[k])
            def _(k=k):
                for f in range(2):
                    forward(k, f).wait_send()

    def power_steps(read, write, degree, z0, z1, rows):
        r0, n = rows
        sums = {}

        def y_sum(z):
            if z not in sums:
                sums[z] = (
                    read(degree - 1, z, r0 - 1, n) + read(degree - 1, z, r0, n) + read(degree - 1, z, r0 + 1, n)
                )
            return sums[z]

        shared = None
        for z in range(z0, z1):
            if shared is None:
                shared = y_sum(z) + y_sum(z + 1)
                s0, s1 = x_sum(shared + y_sum(z - 1), n)
            else:
                s0, s1 = x_sum(shared + y_sum(z + 1), n)
                shared = None
            sums.pop(z - 1, None)
            mask = M[z, r0:r0 + n, :]
            box = jnp.stack([s0 * mask, s1 * mask])
            value = C[:, z, r0:r0 + n, :] * read(degree - 1, z, r0, n) - box
            if degree == 1:
                value = 0.5 * value
            else:
                value = value - read(degree - 2, z, r0, n)
            write(degree, z, r0, n, value)

    def reader(f, V):
        def read(degree, z, r, n):
            if degree == 0:
                return F[f, :, z, r:r + n, :]
            return V[degree - 1, :, z, r:r + n, :]
        return read

    def writer(V):
        def write(degree, z, r, n, value):
            V[degree - 1, :, z, r:r + n, :] = value
        return write

    read_p, read_r = reader(0, PV), reader(1, RV)
    write_p, write_r = writer(PV), writer(RV)

    def own(block, degree, xt):
        if degree == 0:
            return V0[block, xt]
        V = (PV, RV)[block]
        return V[degree - 1, xt, S:S + BZ, MID:MID + 8, :]

    lane8 = lax.broadcasted_iota(jnp.int32, (8, 128), 1)
    sub8 = lax.broadcasted_iota(jnp.int32, (8, 128), 0)

    def all_sublanes(v):
        v = v + pltpu.roll(v, 4, 0)
        v = v + pltpu.roll(v, 2, 0)
        return v + pltpu.roll(v, 1, 0)

    def exact_sum(pairs):
        while len(pairs) > 1:
            joined = []
            for (a, ea), (b, eb) in zip(pairs[::2], pairs[1::2]):
                t = a + b
                back = t - a
                err = (a - (t - back)) + (b - back)
                joined.append((t, err if ea is None else err + (ea + eb)))
            pairs = joined
        return pairs[0]

    def splat(v, j):
        return jnp.broadcast_to(v[j:j + 1, :], (8, 128))

    def by_row(values):
        out = jnp.zeros((8, 128), jnp.float32)
        for j, value in enumerate(values):
            if value:
                out = jnp.where(sub8 == j, value, out)
        return out

    diag_c = (by_row([CENTER] * S), by_row([CENTER] * (S - 1)))
    from_low = (by_row([0.0, HALF] + [0.5 * HALF] * (S - 1)), by_row([0.0, HALF] + [0.5 * HALF] * (S - 2)))
    from_high = (by_row([0.5 * HALF] * (S - 1)), by_row([0.5 * HALF] * (S - 2)))

    def combine(c, xt):
        total = None
        for block in range(2):
            for degree in range(S + 1 - block):
                half, row = place(degree + block * (S + 1))
                term = splat(c[half], row)[None] * own(block, degree, xt)
                total = term if total is None else total + term
        return total

    def outer(t, carry):
        par = t % 2
        exchange_start()

        @pl.when(t > 0)
        def _():
            for xt in range(2):
                X[xt] = X[xt] + combine([XC[h] for h in range(PARTS)], xt)
        exchange_finish()

        @pl.when(t == 0)
        def _():
            exchange_last()
            exchange_sent()
            for z in range(NZE):
                C[:, z, LO:HI + 8, :] = (2.0 / HALF) * (
                    F[1, :, z, LO:HI + 8, :] + (27.0 - CENTER)
                )
                F[1, :, z, LO:HI + 8, :] = F[0, :, z, LO:HI + 8, :]

        for f in range(2):
            V0[f] = F[f, :, S:S + BZ, MID:MID + 8, :]
        def early_rows(core, m):
            n = 8 * ((2 * m + 7) // 8)
            return (MID + m - n if core else MID + 8 - m, n)

        def late_rows(core, m):
            return (MID + m if core else MID - m, 8)

        def powers(rows, core):
            for degree in range(1, S + 1):
                for f, (read, write) in enumerate(((read_p, write_p), (read_r, write_r))):
                    m = S - f - degree
                    if m >= 0 and rows(core, m)[1]:
                        power_steps(read, write, degree, degree + f, NZE - degree - f, rows(core, m))

        for core in range(2):
            @pl.when(gx == core)
            def _(core=core):
                powers(early_rows, core)

                @pl.when(t > 0)
                def _():
                    exchange_last()
                powers(late_rows, core)

        parts = [None] * (NPP + NPR + NRR)

        def add(k, a, b):
            s = jnp.sum(a * b, axis=0)
            parts[k] = s if parts[k] is None else parts[k] + s

        for xt in range(2):
            p, r = own(0, 0, xt), own(1, 0, xt)
            for i in range(S + 1):
                p_next = own(0, i + 1, xt) if i < S else None
                r_next = own(1, i + 1, xt) if i < S - 1 else None
                add(2 * i, p, p)
                if i < S:
                    add(2 * i + 1, p, p_next)
                    add(NPP + 2 * i, p, r)
                    add(NPP + 2 * i + 1, p_next, r)
                    add(NPP + NPR + 2 * i, r, r)
                if i < S - 1:
                    add(NPP + NPR + 2 * i + 1, r, r_next)
                p, r = p_next, r_next
        picked = jnp.zeros((8, 128), jnp.float32)
        for k, part in enumerate(parts):
            picked = jnp.where(lane8 == k, jnp.sum(part, axis=1, keepdims=True), picked)
        local = jnp.sum(picked, axis=0, keepdims=True)

        me1 = 8 * py + yv
        @pl.when(t > 0)
        def _():
            exchange_sent()
        S1[par, me1] = local
        for to in plane:
            pltpu.make_async_remote_copy(
                src_ref=S1.at[par, me1], dst_ref=S1.at[par, me1],
                send_sem=g1_s.at[par], recv_sem=g1_r.at[par],
                device_id=to, device_id_type=MESH,
            ).start()
        whole1 = pltpu.make_async_copy(S1.at[par, pl.ds(0, 31)], S1.at[par, pl.ds(0, 31)], g1_r.at[par])
        whole1.wait()
        S2[par, pz] = jnp.concatenate(exact_sum([(S1[par, i], None) for i in range(32)]), axis=0)
        for to in line:
            pltpu.make_async_remote_copy(
                src_ref=S2.at[par, pz], dst_ref=S2.at[par, pz],
                send_sem=g2_s.at[par], recv_sem=g2_r.at[par],
                device_id=to, device_id_type=MESH,
            ).start()
        whole2 = pltpu.make_async_copy(S2.at[par, pl.ds(0, 7)], S2.at[par, pl.ds(0, 7)], g2_r.at[par])
        whole2.wait()
        high, low = exact_sum([(S2[par, i, 0:1], S2[par, i, 1:2]) for i in range(nzp)])
        lead = high.astype(jnp.bfloat16).astype(jnp.float32)
        rest = (high - lead) + low
        lead, rest = jnp.broadcast_to(lead, (8, 128)), jnp.broadcast_to(rest, (8, 128))
        pltpu.make_async_copy(S1.at[par, pl.ds(0, 31)], S1.at[par, pl.ds(0, 31)], g1_s.at[par]).wait()
        pltpu.make_async_copy(S2.at[par, pl.ds(0, 7)], S2.at[par, pl.ds(0, 7)], g2_s.at[par]).wait()

        columns = 2 * S + 1

        def lanes(v):
            return jnp.broadcast_to(jnp.sum(v, axis=1, keepdims=True), (8, 128))

        table = [
            [lanes(w_ref[j, half] * lead) + lanes(w_ref[j, half] * rest) for half in range(PARTS)]
            for j in range(columns)
        ]

        def form(u, v, top_p, top_r):
            used = list(range(top_p + 1)) + [S + 1 + j for j in range(top_r + 1)]
            total = None
            for half in sorted({place(j)[0] for j in used}):
                terms = [table[j][half] * splat(v[place(j)[0]], place(j)[1]) for j in used]
                while len(terms) > 1:
                    terms = [
                        terms[i] + terms[i + 1] if i + 1 < len(terms) else terms[i] for i in range(0, len(terms), 2)
                    ]
                part = terms[0] * u[half]
                total = part if total is None else total + part
            return all_sublanes(total)

        unit = jnp.where(sub8 == 0, 1.0, 0.0)
        none = jnp.zeros((8, 128), jnp.float32)
        p_c, r_c, x_c = ([unit] + [none] * (PARTS - 1), [none, unit] + [none] * (PARTS - 2), [none] * PARTS)
        norm = form(r_c, r_c, -1, 0)
        for step in range(S):
            q = [
                diag_c[h] * p_c[h] + from_low[h] * pltpu.roll(p_c[h], 1, 0) + from_high[h] * pltpu.roll(p_c[h], 7, 0)
                for h in range(2)
            ]
            if PARTS == 3:
                q.append(jnp.where(sub8 == 0, 0.5 * HALF * splat(p_c[0], 7), 0.0))
            length = norm / form(p_c, q, step + 1, step)
            r_next = [r_c[h] - length * q[h] for h in range(PARTS)]
            norm_next = form(r_next, r_next, step + 1, min(step, S - 1))
            ratio = norm_next / norm
            new = (
                [x_c[h] + length * p_c[h] for h in range(PARTS)] + r_next
                + [r_next[h] + ratio * p_c[h] for h in range(PARTS)] + [norm_next]
            )
            count = sum(inner > step for inner in INNER)
            if count < len(INNER):
                keep = jnp.full((8, 128), t, jnp.int32) < count
                new = [jnp.where(keep, a, b) for a, b in zip(new, x_c + r_c + p_c + [norm])]
            x_c, r_c, p_c, norm = new[:PARTS], new[PARTS:2 * PARTS], new[2 * PARTS:3 * PARTS], new[-1]

        for xt in range(2):
            F[0, xt, S:S + BZ, MID:MID + 8, :] = combine(p_c, xt)
            F[1, xt, S:S + BZ, MID:MID + 8, :] = combine(r_c, xt)
        for h in range(PARTS):
            XC[h] = x_c[h]
        return carry

    lax.fori_loop(0, len(INNER), outer, 0)

    def back(f, src):
        return pltpu.make_async_remote_copy(
            src_ref=src, dst_ref=land.at[f],
            send_sem=io_s.at[2 + f], recv_sem=io_r.at[2 + f],
            device_id=(gz, gy, sib), device_id_type=MESH,
        )

    halves = reorder(F[1, :, S:S + BZ, MID:MID + 8, :], to_natural)
    for xt in range(2):
        F[1, xt, S:S + BZ, MID:MID + 8, :] = halves[xt]
    res_back = back(1, F.at[1, sib, own_z, own_rows, :])
    res_back.start()
    halves = reorder([X[xt] + combine([XC[h] for h in range(PARTS)], xt) for xt in range(2)], to_natural)
    for xt in range(2):
        X[xt] = halves[xt]
    sol_back = back(0, X.at[sib])
    sol_back.start()
    res_ref[:, mine, :] = F[1, gx, S:S + BZ, MID:MID + 8, :]
    sol_ref[:, mine, :] = X[gx]
    for f, (cp, out) in enumerate(((sol_back, sol_ref), (res_back, res_ref))):
        cp.wait()
        out[:, other, :] = land[f]


def solution(mesh):
    table = weights()

    def local(right_side, diagonal):
        f32 = jnp.float32
        dma = pltpu.SemaphoreType.DMA
        field = (2, NZE, ROWS, 128)
        return pl.pallas_call(
            kernel,
            out_shape=(jax.ShapeDtypeStruct(right_side.shape, f32),) * 2,
            in_specs=[pl.BlockSpec(memory_space=pltpu.HBM)] * 3,
            out_specs=(pl.BlockSpec(memory_space=pltpu.VMEM),) * 2,
            scratch_shapes=[
                pltpu.VMEM((2,) + field, f32),
                pltpu.VMEM((S,) + field, f32),
                pltpu.VMEM((S - 1,) + field, f32),
                pltpu.VMEM(field, f32),
                pltpu.VMEM((NZE, ROWS, 128), f32),
                pltpu.VMEM((2, 2, BZ, 8, 128), f32),
                pltpu.VMEM((2, BZ, 8, 128), f32),
                pltpu.VMEM((PARTS, 8, 128), f32),
                pltpu.VMEM((2, BZ, 8, 128), f32),
                pltpu.VMEM((2, 32, 1, 128), f32),
                pltpu.VMEM((2, 8, 2, 128), f32),
                pltpu.VMEM(table.shape, f32),
                dma((5,)), dma((2, 2)), dma((2, 2)), dma((2, 2)), dma((2, 2)), dma((2, 2)), dma((2, 2)), dma((2, 2)), dma((2, 2)),
                dma((4,)), dma((4,)), dma((2,)), dma((2,)), dma((2,)), dma((2,)),
            ],
            compiler_params=pltpu.CompilerParams(collective_id=0, has_side_effects=True, vmem_limit_bytes=48 * 2**20),
        )(*(pltpu.with_memory_space_constraint(v, pltpu.HBM) for v in (right_side, diagonal, jnp.asarray(table))))

    spec = P("gz", "gy", "gx")
    return jax.shard_map(
        local, mesh=mesh, in_specs=(spec, spec), out_specs=(spec, spec), check_vma=False
    )
```

```python
import functools

import jax
import jax.numpy as jnp
import numpy as np
from jax import lax
from jax.experimental import pallas as pl
from jax.experimental.pallas import tpu as pltpu
from jax.sharding import PartitionSpec as P

S = 8
INNER = (8, 8, 7, 7)
MESH = pl.DeviceIdType.MESH

CENTER = 19.0
HALF = 19.0

BZ = 8
NZE = BZ + 2 * S
ROWS = 40
LO, MID, HI = 8, 16, 24

NPP, NPR, NRR = 2 * S + 1, 2 * S, 2 * S - 1

PARTS = 3 if S == 8 else 2


def place(i):
    if i > S:
        return 1, i - S - 1
    return (0, i) if i < 8 else (2, i - 8)


def weights():
    columns = 2 * S + 1
    total = NPP + NPR + NRR

    def moment(offset, m):
        v = np.zeros(total)
        if m < 2:
            v[offset + m] = 1.0
        else:
            v[offset + m] = 2.0
            v[offset + m % 2] -= 1.0
        return v

    gram = np.zeros((columns, columns, total))
    for i in range(columns):
        for j in range(columns):
            di, dj = (i if i <= S else i - S - 1), (j if j <= S else j - S - 1)
            kinds = (i > S) + (j > S)
            offset = (0, NPP, NPP + NPR)[kinds]
            gram[i, j] = (moment(offset, di + dj) + moment(offset, abs(di - dj))) / 2
    out = np.zeros((columns, PARTS, 8, 128), np.float32)
    for j in range(columns):
        for i in range(columns):
            half, row = place(i)
            out[j, half, row, :total] = gram[i, j]
    return out


def kernel(
    rhs_ref, diag_ref, w_hbm, sol_ref, res_ref,
    F, PV, RV, C, M, V0, X, XC, land, S1, S2, w_ref,
    in_sem, zs_sem, zr_sem, ys_sem, yr_sem, cs_sem, cr_sem, fs_sem, fr_sem, io_s, io_r, g1_s, g1_r, g2_s, g2_r,
):
    gz = lax.axis_index("gz")
    gy = lax.axis_index("gy")
    gx = lax.axis_index("gx")
    nz = lax.axis_size("gz")
    ny = lax.axis_size("gy")
    yv = 2 * gy + gx
    nyv = 2 * ny
    sib = 1 - gx
    nzp = 8
    py = gz // nzp
    pz = gz % nzp

    own_rows = pl.ds(MID, 8)
    own_z = pl.ds(S, BZ)
    mine = pl.ds(pl.multiple_of(8 * gx, 8), 8)
    other = pl.ds(pl.multiple_of(8 * sib, 8), 8)

    loads = []
    for f, ref in enumerate((rhs_ref, diag_ref)):
        loads.append(pltpu.make_async_copy(ref.at[:, other, :], land.at[f], in_sem.at[f]))
    for f, ref in enumerate((rhs_ref, diag_ref)):
        loads.append(pltpu.make_async_copy(ref.at[:, mine, :], F.at[f, gx, own_z, own_rows, :], in_sem.at[2 + f]))
    loads.append(pltpu.make_async_copy(w_hbm, w_ref, in_sem.at[4]))
    for cp in loads:
        cp.start()

    plane = [
        (((py + dy) % 4) * nzp + pz, (gy + dx) % 4, gx)
        for dy in (2, 1, 3, 0) for dx in (2, 1, 3, 0) if dy or dx
    ]
    line = [(py * nzp + (pz + dz) % nzp, gy, (gx + dc) % 2) for dz in (4, 3, 5, 2, 6, 1, 7, 0) for dc in range(2) if dz or dc]
    off_gy = gy + 2 * gx - 1
    has_off = (off_gy >= 0) & (off_gy < ny)
    to_z = (gz > 0, gz < nz - 1)
    from_z = (gz < nz - 1, gz > 0)

    barrier = pltpu.get_barrier_semaphore()
    for to in plane + line:
        pl.semaphore_signal(barrier, inc=1, device_id=to, device_id_type=MESH)
    @pl.when(has_off)
    def _():
        pl.semaphore_signal(barrier, inc=1, device_id=(gz, off_gy, sib), device_id_type=MESH)
    for k, dz in enumerate((-1, 1)):
        @pl.when(to_z[k])
        def _(dz=dz):
            pl.semaphore_signal(barrier, inc=1, device_id=(gz + dz, gy, gx), device_id_type=MESH)

        @pl.when(to_z[k] & has_off)
        def _(dz=dz):
            pl.semaphore_signal(barrier, inc=1, device_id=(gz + dz, off_gy, sib), device_id_type=MESH)

    @pl.when(gz == 0)
    def _():
        F[:, :, 0:S, :, :] = jnp.zeros((2, 2, S, ROWS, 128), jnp.float32)

    @pl.when(gz == nz - 1)
    def _():
        F[:, :, S + BZ:NZE, :, :] = jnp.zeros((2, 2, S, ROWS, 128), jnp.float32)

    @pl.when(yv == 0)
    def _():
        F[:, :, :, LO:MID, :] = jnp.zeros((2, 2, NZE, 8, 128), jnp.float32)

    @pl.when(yv == nyv - 1)
    def _():
        F[:, :, :, HI:HI + 8, :] = jnp.zeros((2, 2, NZE, 8, 128), jnp.float32)

    X[...] = jnp.zeros(X.shape, jnp.float32)

    row = lax.broadcasted_iota(jnp.int32, (ROWS, 128), 0) + (8 * yv - MID)
    row_in = jnp.where((row >= 0) & (row < 8 * nyv), 2.0 / HALF, 0.0)
    for z in range(NZE):
        at = gz * BZ + (z - S)
        M[z] = row_in * jnp.where((at >= 0) & (at < nz * BZ), 1.0, 0.0)

    nz_near = jnp.where(gz > 0, 1, 0) + jnp.where(gz < nz - 1, 1, 0)
    pl.semaphore_wait(barrier, len(plane) + len(line) + nz_near + jnp.where(has_off, nz_near + 1, 0))
    swaps = []
    for f in range(2):
        loads[f].wait()
        cp = pltpu.make_async_remote_copy(
            src_ref=land.at[f],
            dst_ref=F.at[f, gx, own_z, own_rows, :],
            send_sem=io_s.at[f], recv_sem=io_r.at[f],
            device_id=(gz, gy, sib), device_id_type=MESH,
        )
        cp.start()
        swaps.append(cp)
    for cp in loads[2:] + swaps:
        cp.wait()

    lane = lax.broadcasted_iota(jnp.int32, (24, 128), 1)

    def x_sum(v, rows):
        both = v[0] + v[1]
        s0 = both + jnp.where(lane[:rows] == 0, 0.0, pltpu.roll(v[1], 1, 1))
        s1 = both + jnp.where(lane[:rows] == 127, 0.0, pltpu.roll(v[0], 127, 1))
        return s0, s1

    def reorder(pairs, order):
        n = pairs[0][0].shape[0]
        rows = 8 * n * len(pairs)
        wide = jnp.concatenate(
            [jnp.concatenate([v.reshape(8 * n, 128) for v in pair], axis=1) for pair in pairs], axis=0
        )
        high = wide.astype(jnp.bfloat16)
        rest = wide - high.astype(jnp.float32)
        mid = rest.astype(jnp.bfloat16)
        low = (rest - mid.astype(jnp.float32)).astype(jnp.bfloat16)
        out = jnp.dot(jnp.concatenate([high, mid, low], axis=0), order, preferred_element_type=jnp.float32)
        out = out[:rows] + (out[rows:2 * rows] + out[2 * rows:])
        return [
            [out[8 * n * i:8 * n * (i + 1), 128 * h:128 * (h + 1)].reshape(n, 8, 128) for h in range(2)]
            for i in range(len(pairs))
        ]

    at_i = lax.broadcasted_iota(jnp.int32, (256, 256), 0)
    at_j = lax.broadcasted_iota(jnp.int32, (256, 256), 1)
    to_stored = jnp.where(at_i == 2 * (at_j & 127) + (at_j >> 7), 1.0, 0.0).astype(jnp.bfloat16)
    to_natural = jnp.where(at_j == 2 * (at_i & 127) + (at_i >> 7), 1.0, 0.0).astype(jnp.bfloat16)
    for f, halves in enumerate(
        reorder([[F[f, xt, S:S + BZ, MID:MID + 8, :] for xt in range(2)] for f in range(2)], to_stored)
    ):
        for xt in range(2):
            F[f, xt, S:S + BZ, MID:MID + 8, :] = halves[xt]

    off_rows = pl.ds(pl.multiple_of(LO + 16 * sib, 8), 8)
    sib_rows = pl.ds(pl.multiple_of(LO + 16 * gx, 8), 8)
    near = (gz - 1, gz + 1)

    def bands(k, f):
        return (pl.ds(S + BZ, S - f), pl.ds(f, S - f))[k]

    def edges(k, f):
        return (pl.ds(S, S - f), pl.ds(BZ + f, S - f))[k]

    def remote(f, src_planes, dst_planes, dst_rows, send, recv, to):
        return pltpu.make_async_remote_copy(
            src_ref=F.at[f, :, src_planes, own_rows, :], dst_ref=F.at[f, :, dst_planes, dst_rows, :],
            send_sem=send, recv_sem=recv, device_id=to, device_id_type=MESH,
        )

    def z_copy(k, f):
        return remote(f, edges(k, f), bands(k, f), own_rows, zs_sem.at[k, f], zr_sem.at[k, f], (near[k], gy, gx))

    def corner(k, f):
        return remote(
            f, edges(k, f), bands(k, f), off_rows, cs_sem.at[k, f], cr_sem.at[k, f], (near[k], off_gy, sib)
        )

    def forward(k, f):
        return remote(f, bands(k, f), bands(k, f), sib_rows, fs_sem.at[k, f], fr_sem.at[k, f], (gz, gy, sib))

    def off_forward(k):
        f = 1
        return remote(f, bands(k, f), bands(k, f), off_rows, cs_sem.at[k, f], cr_sem.at[k, f], (gz, off_gy, sib))

    def y_off(f):
        return remote(f, own_z, own_z, off_rows, ys_sem.at[0, f], yr_sem.at[0, f], (gz, off_gy, sib))

    def y_sib(f):
        return remote(f, own_z, own_z, sib_rows, ys_sem.at[1, f], yr_sem.at[1, f], (gz, gy, sib))

    def exchange_start():
        for k in range(2):
            @pl.when(to_z[k])
            def _(k=k):
                for f in (1, 0):
                    z_copy(k, f).start()

        @pl.when(has_off)
        def _():
            for f in range(2):
                y_off(f).start()
        for k in range(2):
            @pl.when(to_z[k] & has_off)
            def _(k=k):
                corner(k, 0).start()
        for f in range(2):
            y_sib(f).start()

    def exchange_finish():
        for f in (1, 0):
            for k in range(2):
                @pl.when(from_z[k])
                def _(k=k, f=f):
                    z_copy(k, f).wait_recv()
                    if f == 1:
                        @pl.when(has_off)
                        def _():
                            off_forward(k).start()
                    forward(k, f).start()
        for f in range(2):
            y_sib(f).wait_recv()
        for k in range(2):
            @pl.when(from_z[k])
            def _(k=k):
                for f in range(2):
                    forward(k, f).wait_recv()

    def exchange_last():
        @pl.when(has_off)
        def _():
            for f in range(2):
                y_off(f).wait_recv()
        for k in range(2):
            @pl.when(from_z[k] & has_off)
            def _(k=k):
                corner(k, 0).wait_recv()
                off_forward(k).wait_recv()

    def exchange_sent():
        for f in range(2):
            y_sib(f).wait_send()

        @pl.when(has_off)
        def _():
            for f in range(2):
                y_off(f).wait_send()
        for k in range(2):
            @pl.when(to_z[k])
            def _(k=k):
                for f in range(2):
                    z_copy(k, f).wait_send()

            @pl.when(to_z[k] & has_off)
            def _(k=k):
                corner(k, 0).wait_send()

            @pl.when(from_z[k])
            def _(k=k):
                for f in range(2):
                    forward(k, f).wait_send()

            @pl.when(from_z[k] & has_off)
            def _(k=k):
                off_forward(k).wait_send()

    def power_steps(read, write, degree, z0, z1, rows):
        r0, n = rows
        sums = {}

        def y_sum(z):
            if z not in sums:
                sums[z] = (
                    read(degree - 1, z, r0 - 1, n) + read(degree - 1, z, r0, n) + read(degree - 1, z, r0 + 1, n)
                )
            return sums[z]

        shared = None
        for z in range(z0, z1):
            if shared is None:
                shared = y_sum(z) + y_sum(z + 1)
                s0, s1 = x_sum(shared + y_sum(z - 1), n)
            else:
                s0, s1 = x_sum(shared + y_sum(z + 1), n)
                shared = None
            sums.pop(z - 1, None)
            mask = M[z, r0:r0 + n, :]
            box = jnp.stack([s0 * mask, s1 * mask])
            value = C[:, z, r0:r0 + n, :] * read(degree - 1, z, r0, n) - box
            if degree == 1:
                value = 0.5 * value
            else:
                value = value - read(degree - 2, z, r0, n)
            write(degree, z, r0, n, value)

    def reader(f, V):
        def read(degree, z, r, n):
            if degree == 0:
                return F[f, :, z, r:r + n, :]
            return V[degree - 1, :, z, r:r + n, :]
        return read

    def writer(V):
        def write(degree, z, r, n, value):
            V[degree - 1, :, z, r:r + n, :] = value
        return write

    read_p, read_r = reader(0, PV), reader(1, RV)
    write_p, write_r = writer(PV), writer(RV)

    def own(block, degree, xt):
        if degree == 0:
            return V0[block, xt]
        V = (PV, RV)[block]
        return V[degree - 1, xt, S:S + BZ, MID:MID + 8, :]

    lane8 = lax.broadcasted_iota(jnp.int32, (8, 128), 1)
    sub8 = lax.broadcasted_iota(jnp.int32, (8, 128), 0)

    def all_sublanes(v):
        v = v + pltpu.roll(v, 4, 0)
        v = v + pltpu.roll(v, 2, 0)
        return v + pltpu.roll(v, 1, 0)

    def exact_sum(pairs):
        while len(pairs) > 1:
            joined = []
            for (a, ea), (b, eb) in zip(pairs[::2], pairs[1::2]):
                t = a + b
                back = t - a
                err = (a - (t - back)) + (b - back)
                joined.append((t, err if ea is None else err + (ea + eb)))
            pairs = joined
        return pairs[0]

    def splat(v, j):
        return jnp.broadcast_to(v[j:j + 1, :], (8, 128))

    def by_row(values):
        out = jnp.zeros((8, 128), jnp.float32)
        for j, value in enumerate(values):
            if value:
                out = jnp.where(sub8 == j, value, out)
        return out

    diag_c = (by_row([CENTER] * S), by_row([CENTER] * (S - 1)))
    from_low = (by_row([0.0, HALF] + [0.5 * HALF] * (S - 1)), by_row([0.0, HALF] + [0.5 * HALF] * (S - 2)))
    from_high = (by_row([0.5 * HALF] * (S - 1)), by_row([0.5 * HALF] * (S - 2)))

    def combine(c, xt):
        total = None
        for block in range(2):
            for degree in range(S + 1 - block):
                half, row = place(degree + block * (S + 1))
                term = splat(c[half], row)[None] * own(block, degree, xt)
                total = term if total is None else total + term
        return total

    def outer(t, carry):
        par = t % 2
        exchange_start()

        @pl.when(t > 0)
        def _():
            for xt in range(2):
                X[xt] = X[xt] + combine([XC[h] for h in range(PARTS)], xt)
        exchange_finish()

        @pl.when(t == 0)
        def _():
            exchange_last()
            exchange_sent()
            for z in range(NZE):
                C[:, z, LO:HI + 8, :] = (2.0 / HALF) * (
                    F[1, :, z, LO:HI + 8, :] + (27.0 - CENTER)
                )
                F[1, :, z, LO:HI + 8, :] = F[0, :, z, LO:HI + 8, :]

        for f in range(2):
            V0[f] = F[f, :, S:S + BZ, MID:MID + 8, :]
        def early_rows(core, m):
            n = 8 * ((2 * m + 7) // 8)
            return (MID + m - n if core else MID + 8 - m, n)

        def late_rows(core, m):
            return (MID + m if core else MID - m, 8)

        def powers(rows, core):
            for degree in range(1, S + 1):
                for f, (read, write) in enumerate(((read_p, write_p), (read_r, write_r))):
                    m = S - f - degree
                    if m >= 0 and rows(core, m)[1]:
                        power_steps(read, write, degree, degree + f, NZE - degree - f, rows(core, m))

        for core in range(2):
            @pl.when(gx == core)
            def _(core=core):
                powers(early_rows, core)

                @pl.when(t > 0)
                def _():
                    exchange_last()
                powers(late_rows, core)

        parts = [None] * (NPP + NPR + NRR)

        def add(k, a, b):
            s = jnp.sum(a * b, axis=0)
            parts[k] = s if parts[k] is None else parts[k] + s

        for xt in range(2):
            p, r = own(0, 0, xt), own(1, 0, xt)
            for i in range(S + 1):
                p_next = own(0, i + 1, xt) if i < S else None
                r_next = own(1, i + 1, xt) if i < S - 1 else None
                add(2 * i, p, p)
                if i < S:
                    add(2 * i + 1, p, p_next)
                    add(NPP + 2 * i, p, r)
                    add(NPP + 2 * i + 1, p_next, r)
                    add(NPP + NPR + 2 * i, r, r)
                if i < S - 1:
                    add(NPP + NPR + 2 * i + 1, r, r_next)
                p, r = p_next, r_next
        picked = jnp.zeros((8, 128), jnp.float32)
        for k, part in enumerate(parts):
            picked = jnp.where(lane8 == k, jnp.sum(part, axis=1, keepdims=True), picked)
        local = jnp.sum(picked, axis=0, keepdims=True)

        me1 = 2 * pz + gx
        me2 = 4 * py + gy
        @pl.when(t > 0)
        def _():
            exchange_sent()
        S1[par, me1] = local
        for to in line:
            pltpu.make_async_remote_copy(
                src_ref=S1.at[par, me1], dst_ref=S1.at[par, me1],
                send_sem=g1_s.at[par], recv_sem=g1_r.at[par],
                device_id=to, device_id_type=MESH,
            ).start()
        whole1 = pltpu.make_async_copy(S1.at[par, pl.ds(0, 15)], S1.at[par, pl.ds(0, 15)], g1_r.at[par])
        whole1.wait()
        S2[par, me2] = jnp.concatenate(exact_sum([(S1[par, i], None) for i in range(16)]), axis=0)
        for to in plane:
            pltpu.make_async_remote_copy(
                src_ref=S2.at[par, me2], dst_ref=S2.at[par, me2],
                send_sem=g2_s.at[par], recv_sem=g2_r.at[par],
                device_id=to, device_id_type=MESH,
            ).start()
        whole2 = pltpu.make_async_copy(S2.at[par, pl.ds(0, 15)], S2.at[par, pl.ds(0, 15)], g2_r.at[par])
        whole2.wait()
        high, low = exact_sum([(S2[par, i, 0:1], S2[par, i, 1:2]) for i in range(16)])
        lead = high.astype(jnp.bfloat16).astype(jnp.float32)
        rest = (high - lead) + low
        lead, rest = jnp.broadcast_to(lead, (8, 128)), jnp.broadcast_to(rest, (8, 128))
        pltpu.make_async_copy(S1.at[par, pl.ds(0, 15)], S1.at[par, pl.ds(0, 15)], g1_s.at[par]).wait()
        pltpu.make_async_copy(S2.at[par, pl.ds(0, 15)], S2.at[par, pl.ds(0, 15)], g2_s.at[par]).wait()

        columns = 2 * S + 1

        def lanes(v):
            return jnp.broadcast_to(jnp.sum(v, axis=1, keepdims=True), (8, 128))

        table = [
            [lanes(w_ref[j, half] * lead) + lanes(w_ref[j, half] * rest) for half in range(PARTS)]
            for j in range(columns)
        ]

        def form(u, v, top_p, top_r):
            used = list(range(top_p + 1)) + [S + 1 + j for j in range(top_r + 1)]
            total = None
            for half in sorted({place(j)[0] for j in used}):
                terms = [table[j][half] * splat(v[place(j)[0]], place(j)[1]) for j in used]
                while len(terms) > 1:
                    terms = [
                        terms[i] + terms[i + 1] if i + 1 < len(terms) else terms[i] for i in range(0, len(terms), 2)
                    ]
                part = terms[0] * u[half]
                total = part if total is None else total + part
            return all_sublanes(total)

        unit = jnp.where(sub8 == 0, 1.0, 0.0)
        none = jnp.zeros((8, 128), jnp.float32)
        p_c, r_c, x_c = ([unit] + [none] * (PARTS - 1), [none, unit] + [none] * (PARTS - 2), [none] * PARTS)
        norm = form(r_c, r_c, -1, 0)
        for step in range(S):
            q = [
                diag_c[h] * p_c[h] + from_low[h] * pltpu.roll(p_c[h], 1, 0) + from_high[h] * pltpu.roll(p_c[h], 7, 0)
                for h in range(2)
            ]
            if PARTS == 3:
                q.append(jnp.where(sub8 == 0, 0.5 * HALF * splat(p_c[0], 7), 0.0))
            length = norm / form(p_c, q, step + 1, step)
            r_next = [r_c[h] - length * q[h] for h in range(PARTS)]
            norm_next = form(r_next, r_next, step + 1, min(step, S - 1))
            ratio = norm_next / norm
            new = (
                [x_c[h] + length * p_c[h] for h in range(PARTS)] + r_next
                + [r_next[h] + ratio * p_c[h] for h in range(PARTS)] + [norm_next]
            )
            count = sum(inner > step for inner in INNER)
            if count < len(INNER):
                keep = jnp.full((8, 128), t, jnp.int32) < count
                new = [jnp.where(keep, a, b) for a, b in zip(new, x_c + r_c + p_c + [norm])]
            x_c, r_c, p_c, norm = new[:PARTS], new[PARTS:2 * PARTS], new[2 * PARTS:3 * PARTS], new[-1]

        for xt in range(2):
            F[0, xt, S:S + BZ, MID:MID + 8, :] = combine(p_c, xt)
            F[1, xt, S:S + BZ, MID:MID + 8, :] = combine(r_c, xt)
        for h in range(PARTS):
            XC[h] = x_c[h]
        return carry

    lax.fori_loop(0, len(INNER), outer, 0)

    def back(f, src):
        return pltpu.make_async_remote_copy(
            src_ref=src, dst_ref=land.at[f],
            send_sem=io_s.at[2 + f], recv_sem=io_r.at[2 + f],
            device_id=(gz, gy, sib), device_id_type=MESH,
        )

    (halves,) = reorder([[F[1, xt, S:S + BZ, MID:MID + 8, :] for xt in range(2)]], to_natural)
    for xt in range(2):
        F[1, xt, S:S + BZ, MID:MID + 8, :] = halves[xt]
    res_back = back(1, F.at[1, sib, own_z, own_rows, :])
    res_back.start()
    (halves,) = reorder([[X[xt] + combine([XC[h] for h in range(PARTS)], xt) for xt in range(2)]], to_natural)
    for xt in range(2):
        X[xt] = halves[xt]
    sol_back = back(0, X.at[sib])
    sol_back.start()
    res_ref[:, mine, :] = F[1, gx, S:S + BZ, MID:MID + 8, :]
    sol_ref[:, mine, :] = X[gx]
    for f, (cp, out) in enumerate(((sol_back, sol_ref), (res_back, res_ref))):
        cp.wait()
        out[:, other, :] = land[f]


def solution(mesh):
    table = weights()

    def local(right_side, diagonal):
        f32 = jnp.float32
        dma = pltpu.SemaphoreType.DMA
        field = (2, NZE, ROWS, 128)
        return pl.pallas_call(
            kernel,
            out_shape=(jax.ShapeDtypeStruct(right_side.shape, f32),) * 2,
            in_specs=[pl.BlockSpec(memory_space=pltpu.HBM)] * 3,
            out_specs=(pl.BlockSpec(memory_space=pltpu.VMEM),) * 2,
            scratch_shapes=[
                pltpu.VMEM((2,) + field, f32),
                pltpu.VMEM((S,) + field, f32),
                pltpu.VMEM((S - 1,) + field, f32),
                pltpu.VMEM(field, f32),
                pltpu.VMEM((NZE, ROWS, 128), f32),
                pltpu.VMEM((2, 2, BZ, 8, 128), f32),
                pltpu.VMEM((2, BZ, 8, 128), f32),
                pltpu.VMEM((PARTS, 8, 128), f32),
                pltpu.VMEM((2, BZ, 8, 128), f32),
                pltpu.VMEM((2, 16, 1, 128), f32),
                pltpu.VMEM((2, 16, 2, 128), f32),
                pltpu.VMEM(table.shape, f32),
                dma((5,)), dma((2, 2)), dma((2, 2)), dma((2, 2)), dma((2, 2)), dma((2, 2)), dma((2, 2)), dma((2, 2)), dma((2, 2)),
                dma((4,)), dma((4,)), dma((2,)), dma((2,)), dma((2,)), dma((2,)),
            ],
            compiler_params=pltpu.CompilerParams(collective_id=0, has_side_effects=True, vmem_limit_bytes=48 * 2**20),
        )(*(pltpu.with_memory_space_constraint(v, pltpu.HBM) for v in (right_side, diagonal, jnp.asarray(table))))

    spec = P("gz", "gy", "gx")
    return jax.shard_map(
        local, mesh=mesh, in_specs=(spec, spec), out_specs=(spec, spec), check_vma=False
    )
```

```python
import functools

import jax
import jax.numpy as jnp
import numpy as np
from jax import lax
from jax.experimental import pallas as pl
from jax.experimental.pallas import tpu as pltpu
from jax.sharding import PartitionSpec as P

S = 8
INNER = (8, 8, 7, 7)
MESH = pl.DeviceIdType.MESH

CENTER = 19.0
HALF = 19.0

BZ = 8
NZE = BZ + 2 * S
ROWS = 40
LO, MID, HI = 8, 16, 24

NPP, NPR, NRR = 2 * S + 1, 2 * S, 2 * S - 1

PARTS = 3 if S == 8 else 2


def place(i):
    if i > S:
        return 1, i - S - 1
    return (0, i) if i < 8 else (2, i - 8)


def weights():
    columns = 2 * S + 1
    total = NPP + NPR + NRR

    def moment(offset, m):
        v = np.zeros(total)
        if m < 2:
            v[offset + m] = 1.0
        else:
            v[offset + m] = 2.0
            v[offset + m % 2] -= 1.0
        return v

    gram = np.zeros((columns, columns, total))
    for i in range(columns):
        for j in range(columns):
            di, dj = (i if i <= S else i - S - 1), (j if j <= S else j - S - 1)
            kinds = (i > S) + (j > S)
            offset = (0, NPP, NPP + NPR)[kinds]
            gram[i, j] = (moment(offset, di + dj) + moment(offset, abs(di - dj))) / 2
    out = np.zeros((columns, PARTS, 8, 128), np.float32)
    for j in range(columns):
        for i in range(columns):
            half, row = place(i)
            out[j, half, row, :total] = gram[i, j]
    return out


def kernel(
    rhs_ref, diag_ref, w_hbm, sol_ref, res_ref,
    F, PV, RV, C, M, V0, X, XC, land, S1, S2, w_ref,
    in_sem, zs_sem, zr_sem, ys_sem, yr_sem, cs_sem, cr_sem, fs_sem, fr_sem, io_s, io_r, g1_s, g1_r, g2_s, g2_r,
):
    gz = lax.axis_index("gz")
    gy = lax.axis_index("gy")
    gx = lax.axis_index("gx")
    nz = lax.axis_size("gz")
    ny = lax.axis_size("gy")
    yv = 2 * gy + gx
    nyv = 2 * ny
    sib = 1 - gx
    nzp = 8
    py = gz // nzp
    pz = gz % nzp

    own_rows = pl.ds(MID, 8)
    own_z = pl.ds(S, BZ)
    mine = pl.ds(pl.multiple_of(8 * gx, 8), 8)
    other = pl.ds(pl.multiple_of(8 * sib, 8), 8)

    loads = []
    for f, ref in enumerate((rhs_ref, diag_ref)):
        loads.append(pltpu.make_async_copy(ref.at[:, other, :], land.at[f], in_sem.at[f]))
    for f, ref in enumerate((rhs_ref, diag_ref)):
        loads.append(pltpu.make_async_copy(ref.at[:, mine, :], F.at[f, gx, own_z, own_rows, :], in_sem.at[2 + f]))
    loads.append(pltpu.make_async_copy(w_hbm, w_ref, in_sem.at[4]))
    for cp in loads:
        cp.start()

    plane = [
        (((py + dy) % 4) * nzp + pz, (gy + dx) % 4, gx)
        for dy in (2, 1, 3, 0) for dx in (2, 1, 3, 0) if dy or dx
    ]
    line = [(py * nzp + (pz + dz) % nzp, gy, (gx + dc) % 2) for dz in (4, 3, 5, 2, 6, 1, 7, 0) for dc in range(2) if dz or dc]
    off_gy = gy + 2 * gx - 1
    has_off = (off_gy >= 0) & (off_gy < ny)
    to_z = (gz > 0, gz < nz - 1)
    from_z = (gz < nz - 1, gz > 0)

    barrier = pltpu.get_barrier_semaphore()
    for to in plane + line:
        pl.semaphore_signal(barrier, inc=1, device_id=to, device_id_type=MESH)
    @pl.when(has_off)
    def _():
        pl.semaphore_signal(barrier, inc=1, device_id=(gz, off_gy, sib), device_id_type=MESH)
    for k, dz in enumerate((-1, 1)):
        @pl.when(to_z[k])
        def _(dz=dz):
            pl.semaphore_signal(barrier, inc=1, device_id=(gz + dz, gy, gx), device_id_type=MESH)

        @pl.when(to_z[k] & has_off)
        def _(dz=dz):
            pl.semaphore_signal(barrier, inc=1, device_id=(gz + dz, off_gy, sib), device_id_type=MESH)

    @pl.when(gz == 0)
    def _():
        F[:, :, 0:S, :, :] = jnp.zeros((2, 2, S, ROWS, 128), jnp.float32)

    @pl.when(gz == nz - 1)
    def _():
        F[:, :, S + BZ:NZE, :, :] = jnp.zeros((2, 2, S, ROWS, 128), jnp.float32)

    @pl.when(yv == 0)
    def _():
        F[:, :, :, LO:MID, :] = jnp.zeros((2, 2, NZE, 8, 128), jnp.float32)

    @pl.when(yv == nyv - 1)
    def _():
        F[:, :, :, HI:HI + 8, :] = jnp.zeros((2, 2, NZE, 8, 128), jnp.float32)

    X[...] = jnp.zeros(X.shape, jnp.float32)

    row = lax.broadcasted_iota(jnp.int32, (ROWS, 128), 0) + (8 * yv - MID)
    row_in = jnp.where((row >= 0) & (row < 8 * nyv), 2.0 / HALF, 0.0)
    for z in range(NZE):
        at = gz * BZ + (z - S)
        M[z] = row_in * jnp.where((at >= 0) & (at < nz * BZ), 1.0, 0.0)

    nz_near = jnp.where(gz > 0, 1, 0) + jnp.where(gz < nz - 1, 1, 0)
    pl.semaphore_wait(barrier, len(plane) + len(line) + nz_near + jnp.where(has_off, nz_near + 1, 0))
    swaps = []
    for f in range(2):
        loads[f].wait()
        cp = pltpu.make_async_remote_copy(
            src_ref=land.at[f],
            dst_ref=F.at[f, gx, own_z, own_rows, :],
            send_sem=io_s.at[f], recv_sem=io_r.at[f],
            device_id=(gz, gy, sib), device_id_type=MESH,
        )
        cp.start()
        swaps.append(cp)
    for cp in loads[2:] + swaps:
        cp.wait()

    lane = lax.broadcasted_iota(jnp.int32, (24, 128), 1)

    def x_sum(v, rows):
        both = v[0] + v[1]
        s0 = both + jnp.where(lane[:rows] == 0, 0.0, pltpu.roll(v[1], 1, 1))
        s1 = both + jnp.where(lane[:rows] == 127, 0.0, pltpu.roll(v[0], 127, 1))
        return s0, s1

    def reorder(pairs, order):
        n = pairs[0][0].shape[0]
        rows = 8 * n * len(pairs)
        wide = jnp.concatenate(
            [jnp.concatenate([v.reshape(8 * n, 128) for v in pair], axis=1) for pair in pairs], axis=0
        )
        high = wide.astype(jnp.bfloat16)
        rest = wide - high.astype(jnp.float32)
        mid = rest.astype(jnp.bfloat16)
        low = (rest - mid.astype(jnp.float32)).astype(jnp.bfloat16)
        out = jnp.dot(jnp.concatenate([high, mid, low], axis=0), order, preferred_element_type=jnp.float32)
        out = out[:rows] + (out[rows:2 * rows] + out[2 * rows:])
        return [
            [out[8 * n * i:8 * n * (i + 1), 128 * h:128 * (h + 1)].reshape(n, 8, 128) for h in range(2)]
            for i in range(len(pairs))
        ]

    at_i = lax.broadcasted_iota(jnp.int32, (256, 256), 0)
    at_j = lax.broadcasted_iota(jnp.int32, (256, 256), 1)
    to_stored = jnp.where(at_i == 2 * (at_j & 127) + (at_j >> 7), 1.0, 0.0).astype(jnp.bfloat16)
    to_natural = jnp.where(at_j == 2 * (at_i & 127) + (at_i >> 7), 1.0, 0.0).astype(jnp.bfloat16)
    for f, halves in enumerate(
        reorder([[F[f, xt, S:S + BZ, MID:MID + 8, :] for xt in range(2)] for f in range(2)], to_stored)
    ):
        for xt in range(2):
            F[f, xt, S:S + BZ, MID:MID + 8, :] = halves[xt]

    off_rows = pl.ds(pl.multiple_of(LO + 16 * sib, 8), 8)
    sib_rows = pl.ds(pl.multiple_of(LO + 16 * gx, 8), 8)
    near = (gz - 1, gz + 1)

    def bands(k, f):
        return (pl.ds(S + BZ, S - f), pl.ds(f, S - f))[k]

    def edges(k, f):
        return (pl.ds(S, S - f), pl.ds(BZ + f, S - f))[k]

    def remote(f, src_planes, dst_planes, dst_rows, send, recv, to):
        return pltpu.make_async_remote_copy(
            src_ref=F.at[f, :, src_planes, own_rows, :], dst_ref=F.at[f, :, dst_planes, dst_rows, :],
            send_sem=send, recv_sem=recv, device_id=to, device_id_type=MESH,
        )

    def z_copy(k, f):
        return remote(f, edges(k, f), bands(k, f), own_rows, zs_sem.at[k, f], zr_sem.at[k, f], (near[k], gy, gx))

    def corner(k, f):
        return remote(
            f, edges(k, f), bands(k, f), off_rows, cs_sem.at[k, f], cr_sem.at[k, f], (near[k], off_gy, sib)
        )

    def forward(k, f):
        return remote(f, bands(k, f), bands(k, f), sib_rows, fs_sem.at[k, f], fr_sem.at[k, f], (gz, gy, sib))

    def off_forward(k):
        f = 1
        return remote(f, bands(k, f), bands(k, f), off_rows, cs_sem.at[k, f], cr_sem.at[k, f], (gz, off_gy, sib))

    def y_off(f):
        return remote(f, own_z, own_z, off_rows, ys_sem.at[0, f], yr_sem.at[0, f], (gz, off_gy, sib))

    def y_sib(f):
        return remote(f, own_z, own_z, sib_rows, ys_sem.at[1, f], yr_sem.at[1, f], (gz, gy, sib))

    def exchange_start(f):
        for k in range(2):
            @pl.when(to_z[k])
            def _(k=k):
                z_copy(k, f).start()

        @pl.when(has_off)
        def _():
            y_off(f).start()
        if f == 0:
            for k in range(2):
                @pl.when(to_z[k] & has_off)
                def _(k=k):
                    corner(k, 0).start()
        y_sib(f).start()

    def exchange_finish():
        for f in (1, 0):
            for k in range(2):
                @pl.when(from_z[k])
                def _(k=k, f=f):
                    z_copy(k, f).wait_recv()
                    if f == 1:
                        @pl.when(has_off)
                        def _():
                            off_forward(k).start()
                    forward(k, f).start()
        for f in range(2):
            y_sib(f).wait_recv()
        for k in range(2):
            @pl.when(from_z[k])
            def _(k=k):
                for f in range(2):
                    forward(k, f).wait_recv()

    def exchange_last():
        @pl.when(has_off)
        def _():
            for f in range(2):
                y_off(f).wait_recv()
        for k in range(2):
            @pl.when(from_z[k] & has_off)
            def _(k=k):
                corner(k, 0).wait_recv()
                off_forward(k).wait_recv()

    def exchange_sent():
        for f in range(2):
            y_sib(f).wait_send()

        @pl.when(has_off)
        def _():
            for f in range(2):
                y_off(f).wait_send()
        for k in range(2):
            @pl.when(to_z[k])
            def _(k=k):
                for f in range(2):
                    z_copy(k, f).wait_send()

            @pl.when(to_z[k] & has_off)
            def _(k=k):
                corner(k, 0).wait_send()

            @pl.when(from_z[k])
            def _(k=k):
                for f in range(2):
                    forward(k, f).wait_send()

            @pl.when(from_z[k] & has_off)
            def _(k=k):
                off_forward(k).wait_send()

    def power_steps(read, write, degree, z0, z1, rows):
        r0, n = rows
        sums = {}

        def y_sum(z):
            if z not in sums:
                sums[z] = (
                    read(degree - 1, z, r0 - 1, n) + read(degree - 1, z, r0, n) + read(degree - 1, z, r0 + 1, n)
                )
            return sums[z]

        shared = None
        for z in range(z0, z1):
            if shared is None:
                shared = y_sum(z) + y_sum(z + 1)
                s0, s1 = x_sum(shared + y_sum(z - 1), n)
            else:
                s0, s1 = x_sum(shared + y_sum(z + 1), n)
                shared = None
            sums.pop(z - 1, None)
            mask = M[z, r0:r0 + n, :]
            box = jnp.stack([s0 * mask, s1 * mask])
            value = C[:, z, r0:r0 + n, :] * read(degree - 1, z, r0, n) - box
            if degree == 1:
                value = 0.5 * value
            else:
                value = value - read(degree - 2, z, r0, n)
            write(degree, z, r0, n, value)

    def reader(f, V):
        def read(degree, z, r, n):
            if degree == 0:
                return F[f, :, z, r:r + n, :]
            return V[degree - 1, :, z, r:r + n, :]
        return read

    def writer(V):
        def write(degree, z, r, n, value):
            V[degree - 1, :, z, r:r + n, :] = value
        return write

    read_p, read_r = reader(0, PV), reader(1, RV)
    write_p, write_r = writer(PV), writer(RV)

    def own(block, degree, xt):
        if degree == 0:
            return V0[block, xt]
        V = (PV, RV)[block]
        return V[degree - 1, xt, S:S + BZ, MID:MID + 8, :]

    lane8 = lax.broadcasted_iota(jnp.int32, (8, 128), 1)
    sub8 = lax.broadcasted_iota(jnp.int32, (8, 128), 0)

    def all_sublanes(v):
        v = v + pltpu.roll(v, 4, 0)
        v = v + pltpu.roll(v, 2, 0)
        return v + pltpu.roll(v, 1, 0)

    def exact_sum(pairs):
        while len(pairs) > 1:
            joined = []
            for (a, ea), (b, eb) in zip(pairs[::2], pairs[1::2]):
                t = a + b
                back = t - a
                err = (a - (t - back)) + (b - back)
                joined.append((t, err if ea is None else err + (ea + eb)))
            pairs = joined
        return pairs[0]

    def splat(v, j):
        return jnp.broadcast_to(v[j:j + 1, :], (8, 128))

    def by_row(values):
        out = jnp.zeros((8, 128), jnp.float32)
        for j, value in enumerate(values):
            if value:
                out = jnp.where(sub8 == j, value, out)
        return out

    diag_c = (by_row([CENTER] * S), by_row([CENTER] * (S - 1)))
    from_low = (by_row([0.0, HALF] + [0.5 * HALF] * (S - 1)), by_row([0.0, HALF] + [0.5 * HALF] * (S - 2)))
    from_high = (by_row([0.5 * HALF] * (S - 1)), by_row([0.5 * HALF] * (S - 2)))

    def combine(c, xt):
        total = None
        for block in range(2):
            for degree in range(S + 1 - block):
                half, row = place(degree + block * (S + 1))
                term = splat(c[half], row)[None] * own(block, degree, xt)
                total = term if total is None else total + term
        return total

    def outer(t, carry):
        par = t % 2
        @pl.when(t > 0)
        def _():
            for xt in range(2):
                X[xt] = X[xt] + combine([XC[h] for h in range(PARTS)], xt)
        exchange_finish()

        @pl.when(t == 0)
        def _():
            exchange_last()
            exchange_sent()
            for z in range(NZE):
                C[:, z, LO:HI + 8, :] = (2.0 / HALF) * (
                    F[1, :, z, LO:HI + 8, :] + (27.0 - CENTER)
                )
                F[1, :, z, LO:HI + 8, :] = F[0, :, z, LO:HI + 8, :]

        for f in range(2):
            V0[f] = F[f, :, S:S + BZ, MID:MID + 8, :]
        def early_rows(core, m):
            n = 8 * ((2 * m + 7) // 8)
            return (MID + m - n if core else MID + 8 - m, n)

        def late_rows(core, m):
            return (MID + m if core else MID - m, 8)

        def powers(rows, core):
            for degree in range(1, S + 1):
                for f, (read, write) in enumerate(((read_p, write_p), (read_r, write_r))):
                    m = S - f - degree
                    if m >= 0 and rows(core, m)[1]:
                        power_steps(read, write, degree, degree + f, NZE - degree - f, rows(core, m))

        for core in range(2):
            @pl.when(gx == core)
            def _(core=core):
                powers(early_rows, core)

                @pl.when(t > 0)
                def _():
                    exchange_last()
                powers(late_rows, core)

        parts = [None] * (NPP + NPR + NRR)

        def add(k, a, b):
            s = jnp.sum(a * b, axis=0)
            parts[k] = s if parts[k] is None else parts[k] + s

        for xt in range(2):
            p, r = own(0, 0, xt), own(1, 0, xt)
            for i in range(S + 1):
                p_next = own(0, i + 1, xt) if i < S else None
                r_next = own(1, i + 1, xt) if i < S - 1 else None
                add(2 * i, p, p)
                if i < S:
                    add(2 * i + 1, p, p_next)
                    add(NPP + 2 * i, p, r)
                    add(NPP + 2 * i + 1, p_next, r)
                    add(NPP + NPR + 2 * i, r, r)
                if i < S - 1:
                    add(NPP + NPR + 2 * i + 1, r, r_next)
                p, r = p_next, r_next
        picked = jnp.zeros((8, 128), jnp.float32)
        for k, part in enumerate(parts):
            picked = jnp.where(lane8 == k, jnp.sum(part, axis=1, keepdims=True), picked)
        local = jnp.sum(picked, axis=0, keepdims=True)

        me1 = 2 * pz + gx
        me2 = 4 * py + gy
        @pl.when(t > 0)
        def _():
            exchange_sent()
        S1[par, me1] = local
        for to in line:
            pltpu.make_async_remote_copy(
                src_ref=S1.at[par, me1], dst_ref=S1.at[par, me1],
                send_sem=g1_s.at[par], recv_sem=g1_r.at[par],
                device_id=to, device_id_type=MESH,
            ).start()
        whole1 = pltpu.make_async_copy(S1.at[par, pl.ds(0, 15)], S1.at[par, pl.ds(0, 15)], g1_r.at[par])
        whole1.wait()
        S2[par, me2] = jnp.concatenate(exact_sum([(S1[par, i], None) for i in range(16)]), axis=0)
        for to in plane:
            pltpu.make_async_remote_copy(
                src_ref=S2.at[par, me2], dst_ref=S2.at[par, me2],
                send_sem=g2_s.at[par], recv_sem=g2_r.at[par],
                device_id=to, device_id_type=MESH,
            ).start()
        whole2 = pltpu.make_async_copy(S2.at[par, pl.ds(0, 15)], S2.at[par, pl.ds(0, 15)], g2_r.at[par])
        whole2.wait()
        high, low = exact_sum([(S2[par, i, 0:1], S2[par, i, 1:2]) for i in range(16)])
        lead = high.astype(jnp.bfloat16).astype(jnp.float32)
        rest = (high - lead) + low
        lead, rest = jnp.broadcast_to(lead, (8, 128)), jnp.broadcast_to(rest, (8, 128))
        pltpu.make_async_copy(S1.at[par, pl.ds(0, 15)], S1.at[par, pl.ds(0, 15)], g1_s.at[par]).wait()
        pltpu.make_async_copy(S2.at[par, pl.ds(0, 15)], S2.at[par, pl.ds(0, 15)], g2_s.at[par]).wait()

        columns = 2 * S + 1

        def lanes(v):
            return jnp.broadcast_to(jnp.sum(v, axis=1, keepdims=True), (8, 128))

        table = [
            [lanes(w_ref[j, half] * lead) + lanes(w_ref[j, half] * rest) for half in range(PARTS)]
            for j in range(columns)
        ]

        def form(u, v, top_p, top_r):
            used = list(range(top_p + 1)) + [S + 1 + j for j in range(top_r + 1)]
            total = None
            for half in sorted({place(j)[0] for j in used}):
                terms = [table[j][half] * splat(v[place(j)[0]], place(j)[1]) for j in used]
                while len(terms) > 1:
                    terms = [
                        terms[i] + terms[i + 1] if i + 1 < len(terms) else terms[i] for i in range(0, len(terms), 2)
                    ]
                part = terms[0] * u[half]
                total = part if total is None else total + part
            return all_sublanes(total)

        unit = jnp.where(sub8 == 0, 1.0, 0.0)
        none = jnp.zeros((8, 128), jnp.float32)
        p_c, r_c, x_c = ([unit] + [none] * (PARTS - 1), [none, unit] + [none] * (PARTS - 2), [none] * PARTS)
        norm = form(r_c, r_c, -1, 0)
        for step in range(S):
            q = [
                diag_c[h] * p_c[h] + from_low[h] * pltpu.roll(p_c[h], 1, 0) + from_high[h] * pltpu.roll(p_c[h], 7, 0)
                for h in range(2)
            ]
            if PARTS == 3:
                q.append(jnp.where(sub8 == 0, 0.5 * HALF * splat(p_c[0], 7), 0.0))
            length = norm / form(p_c, q, step + 1, step)
            r_next = [r_c[h] - length * q[h] for h in range(PARTS)]
            norm_next = form(r_next, r_next, step + 1, min(step, S - 1))
            ratio = norm_next / norm
            new = (
                [x_c[h] + length * p_c[h] for h in range(PARTS)] + r_next
                + [r_next[h] + ratio * p_c[h] for h in range(PARTS)] + [norm_next]
            )
            count = sum(inner > step for inner in INNER)
            if count < len(INNER):
                keep = jnp.full((8, 128), t, jnp.int32) < count
                new = [jnp.where(keep, a, b) for a, b in zip(new, x_c + r_c + p_c + [norm])]
            x_c, r_c, p_c, norm = new[:PARTS], new[PARTS:2 * PARTS], new[2 * PARTS:3 * PARTS], new[-1]

        for xt in range(2):
            F[1, xt, S:S + BZ, MID:MID + 8, :] = combine(r_c, xt)

        @pl.when(t < len(INNER) - 1)
        def _():
            exchange_start(1)
            for xt in range(2):
                F[0, xt, S:S + BZ, MID:MID + 8, :] = combine(p_c, xt)
            exchange_start(0)
        for h in range(PARTS):
            XC[h] = x_c[h]
        return carry

    exchange_start(1)
    exchange_start(0)
    lax.fori_loop(0, len(INNER), outer, 0)

    def back(f, src):
        return pltpu.make_async_remote_copy(
            src_ref=src, dst_ref=land.at[f],
            send_sem=io_s.at[2 + f], recv_sem=io_r.at[2 + f],
            device_id=(gz, gy, sib), device_id_type=MESH,
        )

    (halves,) = reorder([[F[1, xt, S:S + BZ, MID:MID + 8, :] for xt in range(2)]], to_natural)
    for xt in range(2):
        F[1, xt, S:S + BZ, MID:MID + 8, :] = halves[xt]
    res_back = back(1, F.at[1, sib, own_z, own_rows, :])
    res_back.start()
    (halves,) = reorder([[X[xt] + combine([XC[h] for h in range(PARTS)], xt) for xt in range(2)]], to_natural)
    for xt in range(2):
        X[xt] = halves[xt]
    sol_back = back(0, X.at[sib])
    sol_back.start()
    res_ref[:, mine, :] = F[1, gx, S:S + BZ, MID:MID + 8, :]
    sol_ref[:, mine, :] = X[gx]
    for f, (cp, out) in enumerate(((sol_back, sol_ref), (res_back, res_ref))):
        cp.wait()
        out[:, other, :] = land[f]


def solution(mesh):
    table = weights()

    def local(right_side, diagonal):
        f32 = jnp.float32
        dma = pltpu.SemaphoreType.DMA
        field = (2, NZE, ROWS, 128)
        return pl.pallas_call(
            kernel,
            out_shape=(jax.ShapeDtypeStruct(right_side.shape, f32),) * 2,
            in_specs=[pl.BlockSpec(memory_space=pltpu.HBM)] * 3,
            out_specs=(pl.BlockSpec(memory_space=pltpu.VMEM),) * 2,
            scratch_shapes=[
                pltpu.VMEM((2,) + field, f32),
                pltpu.VMEM((S,) + field, f32),
                pltpu.VMEM((S - 1,) + field, f32),
                pltpu.VMEM(field, f32),
                pltpu.VMEM((NZE, ROWS, 128), f32),
                pltpu.VMEM((2, 2, BZ, 8, 128), f32),
                pltpu.VMEM((2, BZ, 8, 128), f32),
                pltpu.VMEM((PARTS, 8, 128), f32),
                pltpu.VMEM((2, BZ, 8, 128), f32),
                pltpu.VMEM((2, 16, 1, 128), f32),
                pltpu.VMEM((2, 16, 2, 128), f32),
                pltpu.VMEM(table.shape, f32),
                dma((5,)), dma((2, 2)), dma((2, 2)), dma((2, 2)), dma((2, 2)), dma((2, 2)), dma((2, 2)), dma((2, 2)), dma((2, 2)),
                dma((4,)), dma((4,)), dma((2,)), dma((2,)), dma((2,)), dma((2,)),
            ],
            compiler_params=pltpu.CompilerParams(collective_id=0, has_side_effects=True, vmem_limit_bytes=48 * 2**20),
        )(*(pltpu.with_memory_space_constraint(v, pltpu.HBM) for v in (right_side, diagonal, jnp.asarray(table))))

    spec = P("gz", "gy", "gx")
    return jax.shard_map(
        local, mesh=mesh, in_specs=(spec, spec), out_specs=(spec, spec), check_vma=False
    )
```

```python
import functools

import jax
import jax.numpy as jnp
import numpy as np
from jax import lax
from jax.experimental import pallas as pl
from jax.experimental.pallas import tpu as pltpu
from jax.sharding import PartitionSpec as P

S = 8
INNER = (8, 8, 7, 7)
MESH = pl.DeviceIdType.MESH

CENTER = 19.0
HALF = 19.0

BZ = 8
NZE = BZ + 2 * S
ROWS = 40
LO, MID, HI = 8, 16, 24

NPP, NPR, NRR = 2 * S + 1, 2 * S, 2 * S - 1

PARTS = 3 if S == 8 else 2


def place(i):
    if i > S:
        return 1, i - S - 1
    return (0, i) if i < 8 else (2, i - 8)


def weights():
    columns = 2 * S + 1
    total = NPP + NPR + NRR

    def moment(offset, m):
        v = np.zeros(total)
        if m < 2:
            v[offset + m] = 1.0
        else:
            v[offset + m] = 2.0
            v[offset + m % 2] -= 1.0
        return v

    gram = np.zeros((columns, columns, total))
    for i in range(columns):
        for j in range(columns):
            di, dj = (i if i <= S else i - S - 1), (j if j <= S else j - S - 1)
            kinds = (i > S) + (j > S)
            offset = (0, NPP, NPP + NPR)[kinds]
            gram[i, j] = (moment(offset, di + dj) + moment(offset, abs(di - dj))) / 2
    out = np.zeros((columns, PARTS, 8, 128), np.float32)
    for j in range(columns):
        for i in range(columns):
            half, row = place(i)
            out[j, half, row, :total] = gram[i, j]
    return out


def kernel(
    rhs_ref, diag_ref, w_hbm, sol_ref, res_ref,
    F, PV, RV, C, M, V0, X, XC, land, S1, S2, w_ref,
    in_sem, zs_sem, zr_sem, ys_sem, yr_sem, cs_sem, cr_sem, fs_sem, fr_sem, io_s, io_r, g1_s, g1_r, g2_s, g2_r,
):
    gz = lax.axis_index("gz")
    gy = lax.axis_index("gy")
    gx = lax.axis_index("gx")
    nz = lax.axis_size("gz")
    ny = lax.axis_size("gy")
    yv = 2 * gy + gx
    nyv = 2 * ny
    sib = 1 - gx
    nzp = 8
    py = gz // nzp
    pz = gz % nzp

    own_rows = pl.ds(MID, 8)
    own_z = pl.ds(S, BZ)
    mine = pl.ds(pl.multiple_of(8 * gx, 8), 8)
    other = pl.ds(pl.multiple_of(8 * sib, 8), 8)

    loads = []
    for f, ref in enumerate((rhs_ref, diag_ref)):
        loads.append(pltpu.make_async_copy(ref.at[:, other, :], land.at[f], in_sem.at[f]))
    for f, ref in enumerate((rhs_ref, diag_ref)):
        loads.append(pltpu.make_async_copy(ref.at[:, mine, :], F.at[f, gx, own_z, own_rows, :], in_sem.at[2 + f]))
    loads.append(pltpu.make_async_copy(w_hbm, w_ref, in_sem.at[4]))
    for cp in loads:
        cp.start()

    plane = [
        (((py + dy) % 4) * nzp + pz, (gy + dx) % 4, gx)
        for dy in (2, 1, 3, 0) for dx in (2, 1, 3, 0) if dy or dx
    ]
    line = [(py * nzp + (pz + dz) % nzp, gy, (gx + dc) % 2) for dz in (4, 3, 5, 2, 6, 1, 7, 0) for dc in range(2) if dz or dc]
    off_gy = gy + 2 * gx - 1
    has_off = (off_gy >= 0) & (off_gy < ny)
    to_z = (gz > 0, gz < nz - 1)
    from_z = (gz < nz - 1, gz > 0)

    barrier = pltpu.get_barrier_semaphore()
    for to in plane + line:
        pl.semaphore_signal(barrier, inc=1, device_id=to, device_id_type=MESH)
    @pl.when(has_off)
    def _():
        pl.semaphore_signal(barrier, inc=1, device_id=(gz, off_gy, sib), device_id_type=MESH)
    for k, dz in enumerate((-1, 1)):
        @pl.when(to_z[k])
        def _(dz=dz):
            pl.semaphore_signal(barrier, inc=1, device_id=(gz + dz, gy, gx), device_id_type=MESH)

        @pl.when(to_z[k] & has_off)
        def _(dz=dz):
            pl.semaphore_signal(barrier, inc=1, device_id=(gz + dz, off_gy, sib), device_id_type=MESH)

    @pl.when(gz == 0)
    def _():
        F[:, :, 0:S, :, :] = jnp.zeros((2, 2, S, ROWS, 128), jnp.float32)

    @pl.when(gz == nz - 1)
    def _():
        F[:, :, S + BZ:NZE, :, :] = jnp.zeros((2, 2, S, ROWS, 128), jnp.float32)

    @pl.when(yv == 0)
    def _():
        F[:, :, :, LO:MID, :] = jnp.zeros((2, 2, NZE, 8, 128), jnp.float32)

    @pl.when(yv == nyv - 1)
    def _():
        F[:, :, :, HI:HI + 8, :] = jnp.zeros((2, 2, NZE, 8, 128), jnp.float32)

    X[...] = jnp.zeros(X.shape, jnp.float32)

    row = lax.broadcasted_iota(jnp.int32, (ROWS, 128), 0) + (8 * yv - MID)
    row_in = jnp.where((row >= 0) & (row < 8 * nyv), 2.0 / HALF, 0.0)
    for z in range(NZE):
        at = gz * BZ + (z - S)
        M[z] = row_in * jnp.where((at >= 0) & (at < nz * BZ), 1.0, 0.0)

    nz_near = jnp.where(gz > 0, 1, 0) + jnp.where(gz < nz - 1, 1, 0)
    pl.semaphore_wait(barrier, len(plane) + len(line) + nz_near + jnp.where(has_off, nz_near + 1, 0))
    swaps = []
    for f in range(2):
        loads[f].wait()
        cp = pltpu.make_async_remote_copy(
            src_ref=land.at[f],
            dst_ref=F.at[f, gx, own_z, own_rows, :],
            send_sem=io_s.at[f], recv_sem=io_r.at[f],
            device_id=(gz, gy, sib), device_id_type=MESH,
        )
        cp.start()
        swaps.append(cp)
    for cp in loads[2:] + swaps:
        cp.wait()

    lane = lax.broadcasted_iota(jnp.int32, (24, 128), 1)

    def x_sum(v, rows):
        both = v[0] + v[1]
        s0 = both + jnp.where(lane[:rows] == 0, 0.0, pltpu.roll(v[1], 1, 1))
        s1 = both + jnp.where(lane[:rows] == 127, 0.0, pltpu.roll(v[0], 127, 1))
        return s0, s1

    def reorder(pairs, order):
        n = pairs[0][0].shape[0]
        rows = 8 * n * len(pairs)
        wide = jnp.concatenate(
            [jnp.concatenate([v.reshape(8 * n, 128) for v in pair], axis=1) for pair in pairs], axis=0
        )
        high = wide.astype(jnp.bfloat16)
        rest = wide - high.astype(jnp.float32)
        mid = rest.astype(jnp.bfloat16)
        low = (rest - mid.astype(jnp.float32)).astype(jnp.bfloat16)
        out = jnp.dot(jnp.concatenate([high, mid, low], axis=0), order, preferred_element_type=jnp.float32)
        out = out[:rows] + (out[rows:2 * rows] + out[2 * rows:])
        return [
            [out[8 * n * i:8 * n * (i + 1), 128 * h:128 * (h + 1)].reshape(n, 8, 128) for h in range(2)]
            for i in range(len(pairs))
        ]

    at_i = lax.broadcasted_iota(jnp.int32, (256, 256), 0)
    at_j = lax.broadcasted_iota(jnp.int32, (256, 256), 1)
    to_stored = jnp.where(at_i == 2 * (at_j & 127) + (at_j >> 7), 1.0, 0.0).astype(jnp.bfloat16)
    to_natural = jnp.where(at_j == 2 * (at_i & 127) + (at_i >> 7), 1.0, 0.0).astype(jnp.bfloat16)
    for f, halves in enumerate(
        reorder([[F[f, xt, S:S + BZ, MID:MID + 8, :] for xt in range(2)] for f in range(2)], to_stored)
    ):
        for xt in range(2):
            F[f, xt, S:S + BZ, MID:MID + 8, :] = halves[xt]

    off_rows = pl.ds(pl.multiple_of(LO + 16 * sib, 8), 8)
    sib_rows = pl.ds(pl.multiple_of(LO + 16 * gx, 8), 8)
    near = (gz - 1, gz + 1)

    def bands(k, f):
        return (pl.ds(S + BZ, S - f), pl.ds(f, S - f))[k]

    def edges(k, f):
        return (pl.ds(S, S - f), pl.ds(BZ + f, S - f))[k]

    def remote(f, src_planes, dst_planes, dst_rows, send, recv, to):
        return pltpu.make_async_remote_copy(
            src_ref=F.at[f, :, src_planes, own_rows, :], dst_ref=F.at[f, :, dst_planes, dst_rows, :],
            send_sem=send, recv_sem=recv, device_id=to, device_id_type=MESH,
        )

    def z_copy(k, f):
        return remote(f, edges(k, f), bands(k, f), own_rows, zs_sem.at[k, f], zr_sem.at[k, f], (near[k], gy, gx))

    def corner(k, f):
        return remote(
            f, edges(k, f), bands(k, f), off_rows, cs_sem.at[k, f], cr_sem.at[k, f], (near[k], off_gy, sib)
        )

    def forward(k, f):
        return remote(f, bands(k, f), bands(k, f), sib_rows, fs_sem.at[k, f], fr_sem.at[k, f], (gz, gy, sib))

    def off_forward(k):
        f = 1
        return remote(f, bands(k, f), bands(k, f), off_rows, cs_sem.at[k, f], cr_sem.at[k, f], (gz, off_gy, sib))

    def y_off(f):
        return remote(f, own_z, own_z, off_rows, ys_sem.at[0, f], yr_sem.at[0, f], (gz, off_gy, sib))

    def y_sib(f):
        return remote(f, own_z, own_z, sib_rows, ys_sem.at[1, f], yr_sem.at[1, f], (gz, gy, sib))

    def exchange_start(f):
        for k in range(2):
            @pl.when(to_z[k])
            def _(k=k):
                z_copy(k, f).start()

        @pl.when(has_off)
        def _():
            y_off(f).start()
        if f == 0:
            for k in range(2):
                @pl.when(to_z[k] & has_off)
                def _(k=k):
                    corner(k, 0).start()
        y_sib(f).start()

    def exchange_finish():
        for f in (1, 0):
            for k in range(2):
                @pl.when(from_z[k])
                def _(k=k, f=f):
                    z_copy(k, f).wait_recv()
                    if f == 1:
                        @pl.when(has_off)
                        def _():
                            off_forward(k).start()
                    forward(k, f).start()
        for f in range(2):
            y_sib(f).wait_recv()
        for k in range(2):
            @pl.when(from_z[k])
            def _(k=k):
                for f in range(2):
                    forward(k, f).wait_recv()

    def exchange_last():
        @pl.when(has_off)
        def _():
            for f in range(2):
                y_off(f).wait_recv()
        for k in range(2):
            @pl.when(from_z[k] & has_off)
            def _(k=k):
                corner(k, 0).wait_recv()
                off_forward(k).wait_recv()

    def exchange_sent():
        for f in range(2):
            y_sib(f).wait_send()

        @pl.when(has_off)
        def _():
            for f in range(2):
                y_off(f).wait_send()
        for k in range(2):
            @pl.when(to_z[k])
            def _(k=k):
                for f in range(2):
                    z_copy(k, f).wait_send()

            @pl.when(to_z[k] & has_off)
            def _(k=k):
                corner(k, 0).wait_send()

            @pl.when(from_z[k])
            def _(k=k):
                for f in range(2):
                    forward(k, f).wait_send()

            @pl.when(from_z[k] & has_off)
            def _(k=k):
                off_forward(k).wait_send()

    def power_steps(read, write, degree, z0, z1, rows):
        r0, n = rows
        sums = {}

        def y_sum(z):
            if z not in sums:
                sums[z] = (
                    read(degree - 1, z, r0 - 1, n) + read(degree - 1, z, r0, n) + read(degree - 1, z, r0 + 1, n)
                )
            return sums[z]

        shared = None
        for z in range(z0, z1):
            if shared is None:
                shared = y_sum(z) + y_sum(z + 1)
                s0, s1 = x_sum(shared + y_sum(z - 1), n)
            else:
                s0, s1 = x_sum(shared + y_sum(z + 1), n)
                shared = None
            sums.pop(z - 1, None)
            mask = M[z, r0:r0 + n, :]
            box = jnp.stack([s0 * mask, s1 * mask])
            value = C[:, z, r0:r0 + n, :] * read(degree - 1, z, r0, n) - box
            if degree == 1:
                value = 0.5 * value
            else:
                value = value - read(degree - 2, z, r0, n)
            write(degree, z, r0, n, value)

    def reader(f, V):
        def read(degree, z, r, n):
            if degree == 0:
                return F[f, :, z, r:r + n, :]
            return V[degree - 1, :, z, r:r + n, :]
        return read

    def writer(V):
        def write(degree, z, r, n, value):
            V[degree - 1, :, z, r:r + n, :] = value
        return write

    read_p, read_r = reader(0, PV), reader(1, RV)
    write_p, write_r = writer(PV), writer(RV)

    def own(block, degree, xt):
        if degree == 0:
            return V0[block, xt]
        V = (PV, RV)[block]
        return V[degree - 1, xt, S:S + BZ, MID:MID + 8, :]

    lane8 = lax.broadcasted_iota(jnp.int32, (8, 128), 1)
    sub8 = lax.broadcasted_iota(jnp.int32, (8, 128), 0)

    def all_sublanes(v):
        v = v + pltpu.roll(v, 4, 0)
        v = v + pltpu.roll(v, 2, 0)
        return v + pltpu.roll(v, 1, 0)

    def exact_sum(pairs):
        while len(pairs) > 1:
            joined = []
            for (a, ea), (b, eb) in zip(pairs[::2], pairs[1::2]):
                t = a + b
                back = t - a
                err = (a - (t - back)) + (b - back)
                joined.append((t, err if ea is None else err + (ea + eb)))
            pairs = joined
        return pairs[0]

    def splat(v, j):
        return jnp.broadcast_to(v[j:j + 1, :], (8, 128))

    def by_row(values):
        out = jnp.zeros((8, 128), jnp.float32)
        for j, value in enumerate(values):
            if value:
                out = jnp.where(sub8 == j, value, out)
        return out

    diag_c = (by_row([CENTER] * S), by_row([CENTER] * (S - 1)))
    from_low = (by_row([0.0, HALF] + [0.5 * HALF] * (S - 1)), by_row([0.0, HALF] + [0.5 * HALF] * (S - 2)))
    from_high = (by_row([0.5 * HALF] * (S - 1)), by_row([0.5 * HALF] * (S - 2)))

    def combine(c, xt):
        total = None
        for block in range(2):
            for degree in range(S + 1 - block):
                half, row = place(degree + block * (S + 1))
                term = splat(c[half], row)[None] * own(block, degree, xt)
                total = term if total is None else total + term
        return total

    def outer(t, carry):
        par = t % 2
        @pl.when(t > 0)
        def _():
            for xt in range(2):
                X[xt] = X[xt] + combine([XC[h] for h in range(PARTS)], xt)
        exchange_finish()

        @pl.when(t == 0)
        def _():
            exchange_last()
            exchange_sent()
            for z in range(NZE):
                C[:, z, LO:HI + 8, :] = (2.0 / HALF) * (
                    F[1, :, z, LO:HI + 8, :] + (27.0 - CENTER)
                )
                F[1, :, z, LO:HI + 8, :] = F[0, :, z, LO:HI + 8, :]

        for f in range(2):
            V0[f] = F[f, :, S:S + BZ, MID:MID + 8, :]
        def early_rows(core, m):
            n = 8 * ((2 * m + 7) // 8)
            return (MID + m - n if core else MID + 8 - m, n)

        def late_rows(core, m):
            return (MID + m if core else MID - m, 8)

        def powers(rows, core, fields=(0, 1)):
            for degree in range(1, S + 1):
                for f in fields:
                    read, write = ((read_p, write_p), (read_r, write_r))[f]
                    m = S - f - degree
                    if m >= 0 and rows(core, m)[1]:
                        power_steps(read, write, degree, degree + f, NZE - degree - f, rows(core, m))

        for core in range(2):
            @pl.when((gx == core) & (t > 0))
            def _(core=core):
                powers(early_rows, core)
                exchange_last()
                powers(late_rows, core)

        @pl.when(t == 0)
        def _():
            for degree in range(1, S + 1):
                m = S - degree
                rows = (LO, 24) if m > 4 else (MID - 4, 16) if m else (MID, 8)
                power_steps(read_p, write_p, degree, degree, NZE - degree, rows)
            for degree in range(1, S):
                RV[degree - 1, :, S:S + BZ, MID:MID + 8, :] = PV[degree - 1, :, S:S + BZ, MID:MID + 8, :]

        parts = [None] * (NPP + NPR + NRR)

        def add(k, a, b):
            s = jnp.sum(a * b, axis=0)
            parts[k] = s if parts[k] is None else parts[k] + s

        for xt in range(2):
            p, r = own(0, 0, xt), own(1, 0, xt)
            for i in range(S + 1):
                p_next = own(0, i + 1, xt) if i < S else None
                r_next = own(1, i + 1, xt) if i < S - 1 else None
                add(2 * i, p, p)
                if i < S:
                    add(2 * i + 1, p, p_next)
                    add(NPP + 2 * i, p, r)
                    add(NPP + 2 * i + 1, p_next, r)
                    add(NPP + NPR + 2 * i, r, r)
                if i < S - 1:
                    add(NPP + NPR + 2 * i + 1, r, r_next)
                p, r = p_next, r_next
        picked = jnp.zeros((8, 128), jnp.float32)
        for k, part in enumerate(parts):
            picked = jnp.where(lane8 == k, jnp.sum(part, axis=1, keepdims=True), picked)
        local = jnp.sum(picked, axis=0, keepdims=True)

        me1 = 2 * pz + gx
        me2 = 4 * py + gy
        @pl.when(t > 0)
        def _():
            exchange_sent()
        S1[par, me1] = local
        for to in line:
            pltpu.make_async_remote_copy(
                src_ref=S1.at[par, me1], dst_ref=S1.at[par, me1],
                send_sem=g1_s.at[par], recv_sem=g1_r.at[par],
                device_id=to, device_id_type=MESH,
            ).start()
        whole1 = pltpu.make_async_copy(S1.at[par, pl.ds(0, 15)], S1.at[par, pl.ds(0, 15)], g1_r.at[par])
        whole1.wait()
        S2[par, me2] = jnp.concatenate(exact_sum([(S1[par, i], None) for i in range(16)]), axis=0)
        for to in plane:
            pltpu.make_async_remote_copy(
                src_ref=S2.at[par, me2], dst_ref=S2.at[par, me2],
                send_sem=g2_s.at[par], recv_sem=g2_r.at[par],
                device_id=to, device_id_type=MESH,
            ).start()
        whole2 = pltpu.make_async_copy(S2.at[par, pl.ds(0, 15)], S2.at[par, pl.ds(0, 15)], g2_r.at[par])
        whole2.wait()
        high, low = exact_sum([(S2[par, i, 0:1], S2[par, i, 1:2]) for i in range(16)])
        lead = high.astype(jnp.bfloat16).astype(jnp.float32)
        rest = (high - lead) + low
        lead, rest = jnp.broadcast_to(lead, (8, 128)), jnp.broadcast_to(rest, (8, 128))
        pltpu.make_async_copy(S1.at[par, pl.ds(0, 15)], S1.at[par, pl.ds(0, 15)], g1_s.at[par]).wait()
        pltpu.make_async_copy(S2.at[par, pl.ds(0, 15)], S2.at[par, pl.ds(0, 15)], g2_s.at[par]).wait()

        columns = 2 * S + 1

        def lanes(v):
            return jnp.broadcast_to(jnp.sum(v, axis=1, keepdims=True), (8, 128))

        table = [
            [lanes(w_ref[j, half] * lead) + lanes(w_ref[j, half] * rest) for half in range(PARTS)]
            for j in range(columns)
        ]

        def form(u, v, top_p, top_r):
            used = list(range(top_p + 1)) + [S + 1 + j for j in range(top_r + 1)]
            total = None
            for half in sorted({place(j)[0] for j in used}):
                terms = [table[j][half] * splat(v[place(j)[0]], place(j)[1]) for j in used]
                while len(terms) > 1:
                    terms = [
                        terms[i] + terms[i + 1] if i + 1 < len(terms) else terms[i] for i in range(0, len(terms), 2)
                    ]
                part = terms[0] * u[half]
                total = part if total is None else total + part
            return all_sublanes(total)

        unit = jnp.where(sub8 == 0, 1.0, 0.0)
        none = jnp.zeros((8, 128), jnp.float32)
        p_c, r_c, x_c = ([unit] + [none] * (PARTS - 1), [none, unit] + [none] * (PARTS - 2), [none] * PARTS)
        norm = form(r_c, r_c, -1, 0)
        for step in range(S):
            q = [
                diag_c[h] * p_c[h] + from_low[h] * pltpu.roll(p_c[h], 1, 0) + from_high[h] * pltpu.roll(p_c[h], 7, 0)
                for h in range(2)
            ]
            if PARTS == 3:
                q.append(jnp.where(sub8 == 0, 0.5 * HALF * splat(p_c[0], 7), 0.0))
            length = norm / form(p_c, q, step + 1, step)
            r_next = [r_c[h] - length * q[h] for h in range(PARTS)]
            norm_next = form(r_next, r_next, step + 1, min(step, S - 1))
            ratio = norm_next / norm
            new = (
                [x_c[h] + length * p_c[h] for h in range(PARTS)] + r_next
                + [r_next[h] + ratio * p_c[h] for h in range(PARTS)] + [norm_next]
            )
            count = sum(inner > step for inner in INNER)
            if count < len(INNER):
                keep = jnp.full((8, 128), t, jnp.int32) < count
                new = [jnp.where(keep, a, b) for a, b in zip(new, x_c + r_c + p_c + [norm])]
            x_c, r_c, p_c, norm = new[:PARTS], new[PARTS:2 * PARTS], new[2 * PARTS:3 * PARTS], new[-1]

        for xt in range(2):
            F[1, xt, S:S + BZ, MID:MID + 8, :] = combine(r_c, xt)

        @pl.when(t < len(INNER) - 1)
        def _():
            exchange_start(1)
            for xt in range(2):
                F[0, xt, S:S + BZ, MID:MID + 8, :] = combine(p_c, xt)
            exchange_start(0)
        for h in range(PARTS):
            XC[h] = x_c[h]
        return carry

    exchange_start(1)
    exchange_start(0)
    lax.fori_loop(0, len(INNER), outer, 0)

    def back(f, src):
        return pltpu.make_async_remote_copy(
            src_ref=src, dst_ref=land.at[f],
            send_sem=io_s.at[2 + f], recv_sem=io_r.at[2 + f],
            device_id=(gz, gy, sib), device_id_type=MESH,
        )

    (halves,) = reorder([[F[1, xt, S:S + BZ, MID:MID + 8, :] for xt in range(2)]], to_natural)
    for xt in range(2):
        F[1, xt, S:S + BZ, MID:MID + 8, :] = halves[xt]
    res_back = back(1, F.at[1, sib, own_z, own_rows, :])
    res_back.start()
    (halves,) = reorder([[X[xt] + combine([XC[h] for h in range(PARTS)], xt) for xt in range(2)]], to_natural)
    for xt in range(2):
        X[xt] = halves[xt]
    sol_back = back(0, X.at[sib])
    sol_back.start()
    res_ref[:, mine, :] = F[1, gx, S:S + BZ, MID:MID + 8, :]
    sol_ref[:, mine, :] = X[gx]
    for f, (cp, out) in enumerate(((sol_back, sol_ref), (res_back, res_ref))):
        cp.wait()
        out[:, other, :] = land[f]


def solution(mesh):
    table = weights()

    def local(right_side, diagonal):
        f32 = jnp.float32
        dma = pltpu.SemaphoreType.DMA
        field = (2, NZE, ROWS, 128)
        return pl.pallas_call(
            kernel,
            out_shape=(jax.ShapeDtypeStruct(right_side.shape, f32),) * 2,
            in_specs=[pl.BlockSpec(memory_space=pltpu.HBM)] * 3,
            out_specs=(pl.BlockSpec(memory_space=pltpu.VMEM),) * 2,
            scratch_shapes=[
                pltpu.VMEM((2,) + field, f32),
                pltpu.VMEM((S,) + field, f32),
                pltpu.VMEM((S - 1,) + field, f32),
                pltpu.VMEM(field, f32),
                pltpu.VMEM((NZE, ROWS, 128), f32),
                pltpu.VMEM((2, 2, BZ, 8, 128), f32),
                pltpu.VMEM((2, BZ, 8, 128), f32),
                pltpu.VMEM((PARTS, 8, 128), f32),
                pltpu.VMEM((2, BZ, 8, 128), f32),
                pltpu.VMEM((2, 16, 1, 128), f32),
                pltpu.VMEM((2, 16, 2, 128), f32),
                pltpu.VMEM(table.shape, f32),
                dma((5,)), dma((2, 2)), dma((2, 2)), dma((2, 2)), dma((2, 2)), dma((2, 2)), dma((2, 2)), dma((2, 2)), dma((2, 2)),
                dma((4,)), dma((4,)), dma((2,)), dma((2,)), dma((2,)), dma((2,)),
            ],
            compiler_params=pltpu.CompilerParams(collective_id=0, has_side_effects=True, vmem_limit_bytes=48 * 2**20),
        )(*(pltpu.with_memory_space_constraint(v, pltpu.HBM) for v in (right_side, diagonal, jnp.asarray(table))))

    spec = P("gz", "gy", "gx")
    return jax.shard_map(
        local, mesh=mesh, in_specs=(spec, spec), out_specs=(spec, spec), check_vma=False
    )
```

```python
import functools

import jax
import jax.numpy as jnp
import numpy as np
from jax import lax
from jax.experimental import pallas as pl
from jax.experimental.pallas import tpu as pltpu
from jax.sharding import PartitionSpec as P

S = 8
INNER = (8, 8, 7, 7)
MESH = pl.DeviceIdType.MESH

CENTER = 19.0
HALF = 19.0

BZ = 8
NZE = BZ + 2 * S
ROWS = 40
LO, MID, HI = 8, 16, 24

NPP, NPR, NRR = 2 * S + 1, 2 * S, 2 * S - 1

PARTS = 3 if S == 8 else 2


def place(i):
    if i > S:
        return 1, i - S - 1
    return (0, i) if i < 8 else (2, i - 8)


def weights():
    columns = 2 * S + 1
    total = NPP + NPR + NRR

    def moment(offset, m):
        v = np.zeros(total)
        if m < 2:
            v[offset + m] = 1.0
        else:
            v[offset + m] = 2.0
            v[offset + m % 2] -= 1.0
        return v

    gram = np.zeros((columns, columns, total))
    for i in range(columns):
        for j in range(columns):
            di, dj = (i if i <= S else i - S - 1), (j if j <= S else j - S - 1)
            kinds = (i > S) + (j > S)
            offset = (0, NPP, NPP + NPR)[kinds]
            gram[i, j] = (moment(offset, di + dj) + moment(offset, abs(di - dj))) / 2
    out = np.zeros((columns, PARTS, 8, 128), np.float32)
    for j in range(columns):
        for i in range(columns):
            half, row = place(i)
            out[j, half, row, :total] = gram[i, j]
    return out


def kernel(
    rhs_ref, diag_ref, w_hbm, sol_ref, res_ref,
    F, PV, RV, C, M, V0, X, XC, land, S1, S2, w_ref,
    in_sem, zs_sem, zr_sem, ys_sem, yr_sem, cs_sem, cr_sem, fs_sem, fr_sem, io_s, io_r, g1_s, g1_r, g2_s, g2_r,
):
    gz = lax.axis_index("gz")
    gy = lax.axis_index("gy")
    gx = lax.axis_index("gx")
    nz = lax.axis_size("gz")
    ny = lax.axis_size("gy")
    yv = 2 * gy + gx
    nyv = 2 * ny
    sib = 1 - gx
    nzp = 8
    py = gz // nzp
    pz = gz % nzp

    own_rows = pl.ds(MID, 8)
    own_z = pl.ds(S, BZ)
    mine = pl.ds(pl.multiple_of(8 * gx, 8), 8)
    other = pl.ds(pl.multiple_of(8 * sib, 8), 8)

    loads = []
    for f, ref in enumerate((rhs_ref, diag_ref)):
        loads.append(pltpu.make_async_copy(ref.at[:, other, :], land.at[f], in_sem.at[f]))
    for f, ref in enumerate((rhs_ref, diag_ref)):
        loads.append(pltpu.make_async_copy(ref.at[:, mine, :], F.at[f, gx, own_z, own_rows, :], in_sem.at[2 + f]))
    loads.append(pltpu.make_async_copy(w_hbm, w_ref, in_sem.at[4]))
    for cp in loads:
        cp.start()

    plane = [
        (((py + dy) % 4) * nzp + pz, (gy + dx) % 4, gx)
        for dy in (2, 1, 3, 0) for dx in (2, 1, 3, 0) if dy or dx
    ]
    line = [(py * nzp + (pz + dz) % nzp, gy, (gx + dc) % 2) for dz in (4, 3, 5, 2, 6, 1, 7, 0) for dc in range(2) if dz or dc]
    off_gy = gy + 2 * gx - 1
    has_off = (off_gy >= 0) & (off_gy < ny)
    to_z = (gz > 0, gz < nz - 1)
    from_z = (gz < nz - 1, gz > 0)

    barrier = pltpu.get_barrier_semaphore()
    for to in plane + line:
        pl.semaphore_signal(barrier, inc=1, device_id=to, device_id_type=MESH)
    @pl.when(has_off)
    def _():
        pl.semaphore_signal(barrier, inc=1, device_id=(gz, off_gy, sib), device_id_type=MESH)
    for k, dz in enumerate((-1, 1)):
        @pl.when(to_z[k])
        def _(dz=dz):
            pl.semaphore_signal(barrier, inc=1, device_id=(gz + dz, gy, gx), device_id_type=MESH)

        @pl.when(to_z[k] & has_off)
        def _(dz=dz):
            pl.semaphore_signal(barrier, inc=1, device_id=(gz + dz, off_gy, sib), device_id_type=MESH)

    @pl.when(gz == 0)
    def _():
        F[:, :, 0:S, :, :] = jnp.zeros((2, 2, S, ROWS, 128), jnp.float32)

    @pl.when(gz == nz - 1)
    def _():
        F[:, :, S + BZ:NZE, :, :] = jnp.zeros((2, 2, S, ROWS, 128), jnp.float32)

    @pl.when(yv == 0)
    def _():
        F[:, :, :, LO:MID, :] = jnp.zeros((2, 2, NZE, 8, 128), jnp.float32)

    @pl.when(yv == nyv - 1)
    def _():
        F[:, :, :, HI:HI + 8, :] = jnp.zeros((2, 2, NZE, 8, 128), jnp.float32)

    X[...] = jnp.zeros(X.shape, jnp.float32)

    row = lax.broadcasted_iota(jnp.int32, (ROWS, 128), 0) + (8 * yv - MID)
    row_in = jnp.where((row >= 0) & (row < 8 * nyv), 2.0 / HALF, 0.0)
    for z in range(NZE):
        at = gz * BZ + (z - S)
        M[z] = row_in * jnp.where((at >= 0) & (at < nz * BZ), 1.0, 0.0)

    nz_near = jnp.where(gz > 0, 1, 0) + jnp.where(gz < nz - 1, 1, 0)
    pl.semaphore_wait(barrier, len(plane) + len(line) + nz_near + jnp.where(has_off, nz_near + 1, 0))
    swaps = []
    for f in range(2):
        loads[f].wait()
        cp = pltpu.make_async_remote_copy(
            src_ref=land.at[f],
            dst_ref=F.at[f, gx, own_z, own_rows, :],
            send_sem=io_s.at[f], recv_sem=io_r.at[f],
            device_id=(gz, gy, sib), device_id_type=MESH,
        )
        cp.start()
        swaps.append(cp)
    for cp in loads[2:] + swaps:
        cp.wait()

    lane = lax.broadcasted_iota(jnp.int32, (24, 128), 1)

    def x_sum(v, rows):
        both = v[0] + v[1]
        s0 = both + jnp.where(lane[:rows] == 0, 0.0, pltpu.roll(v[1], 1, 1))
        s1 = both + jnp.where(lane[:rows] == 127, 0.0, pltpu.roll(v[0], 127, 1))
        return s0, s1

    def reorder(pairs, order):
        n = pairs[0][0].shape[0]
        rows = 8 * n * len(pairs)
        wide = jnp.concatenate(
            [jnp.concatenate([v.reshape(8 * n, 128) for v in pair], axis=1) for pair in pairs], axis=0
        )
        high = wide.astype(jnp.bfloat16)
        rest = wide - high.astype(jnp.float32)
        mid = rest.astype(jnp.bfloat16)
        low = (rest - mid.astype(jnp.float32)).astype(jnp.bfloat16)
        out = jnp.dot(jnp.concatenate([high, mid, low], axis=0), order, preferred_element_type=jnp.float32)
        out = out[:rows] + (out[rows:2 * rows] + out[2 * rows:])
        return [
            [out[8 * n * i:8 * n * (i + 1), 128 * h:128 * (h + 1)].reshape(n, 8, 128) for h in range(2)]
            for i in range(len(pairs))
        ]

    at_i = lax.broadcasted_iota(jnp.int32, (256, 256), 0)
    at_j = lax.broadcasted_iota(jnp.int32, (256, 256), 1)
    to_stored = jnp.where(at_i == 2 * (at_j & 127) + (at_j >> 7), 1.0, 0.0).astype(jnp.bfloat16)
    to_natural = jnp.where(at_j == 2 * (at_i & 127) + (at_i >> 7), 1.0, 0.0).astype(jnp.bfloat16)
    for f, halves in enumerate(
        reorder([[F[f, xt, S:S + BZ, MID:MID + 8, :] for xt in range(2)] for f in range(2)], to_stored)
    ):
        for xt in range(2):
            F[f, xt, S:S + BZ, MID:MID + 8, :] = halves[xt]

    off_rows = pl.ds(pl.multiple_of(LO + 16 * sib, 8), 8)
    sib_rows = pl.ds(pl.multiple_of(LO + 16 * gx, 8), 8)
    near = (jnp.maximum(gz - 1, 0), jnp.minimum(gz + 1, nz - 1))
    beyond = jnp.clip(off_gy, 0, ny - 1)

    def bands(k, f):
        return (pl.ds(S + BZ, S - f), pl.ds(f, S - f))[k]

    def edges(k, f):
        return (pl.ds(S, S - f), pl.ds(BZ + f, S - f))[k]

    def remote(f, src_planes, dst_planes, dst_rows, send, recv, to):
        return pltpu.make_async_remote_copy(
            src_ref=F.at[f, :, src_planes, own_rows, :], dst_ref=F.at[f, :, dst_planes, dst_rows, :],
            send_sem=send, recv_sem=recv, device_id=to, device_id_type=MESH,
        )

    def z_copy(k, f):
        return remote(f, edges(k, f), bands(k, f), own_rows, zs_sem.at[k, f], zr_sem.at[k, f], (near[k], gy, gx))

    def corner(k, f):
        return remote(
            f, edges(k, f), bands(k, f), off_rows, cs_sem.at[k, f], cr_sem.at[k, f], (near[k], beyond, sib)
        )

    def forward(k, f):
        return remote(f, bands(k, f), bands(k, f), sib_rows, fs_sem.at[k, f], fr_sem.at[k, f], (gz, gy, sib))

    def off_forward(k):
        f = 1
        return remote(f, bands(k, f), bands(k, f), off_rows, cs_sem.at[k, f], cr_sem.at[k, f], (gz, beyond, sib))

    def y_off(f):
        return remote(f, own_z, own_z, off_rows, ys_sem.at[0, f], yr_sem.at[0, f], (gz, beyond, sib))

    def y_sib(f):
        return remote(f, own_z, own_z, sib_rows, ys_sem.at[1, f], yr_sem.at[1, f], (gz, gy, sib))

    def exchange_start(f):
        for k in range(2):
            @pl.when(to_z[k])
            def _(k=k):
                z_copy(k, f).start()

        @pl.when(has_off)
        def _():
            y_off(f).start()
        if f == 0:
            for k in range(2):
                @pl.when(to_z[k] & has_off)
                def _(k=k):
                    corner(k, 0).start()
        y_sib(f).start()

    def exchange_finish():
        for f in (1, 0):
            for k in range(2):
                @pl.when(from_z[k])
                def _(k=k, f=f):
                    z_copy(k, f).wait_recv()
                    if f == 1:
                        @pl.when(has_off)
                        def _():
                            off_forward(k).start()
                    forward(k, f).start()
        for f in range(2):
            y_sib(f).wait_recv()
        for k in range(2):
            @pl.when(from_z[k])
            def _(k=k):
                for f in range(2):
                    forward(k, f).wait_recv()

    def exchange_last():
        @pl.when(has_off)
        def _():
            for f in range(2):
                y_off(f).wait_recv()
        for k in range(2):
            @pl.when(from_z[k] & has_off)
            def _(k=k):
                corner(k, 0).wait_recv()
                off_forward(k).wait_recv()

    def exchange_sent():
        for f in range(2):
            y_sib(f).wait_send()

        @pl.when(has_off)
        def _():
            for f in range(2):
                y_off(f).wait_send()
        for k in range(2):
            @pl.when(to_z[k])
            def _(k=k):
                for f in range(2):
                    z_copy(k, f).wait_send()

            @pl.when(to_z[k] & has_off)
            def _(k=k):
                corner(k, 0).wait_send()

            @pl.when(from_z[k])
            def _(k=k):
                for f in range(2):
                    forward(k, f).wait_send()

            @pl.when(from_z[k] & has_off)
            def _(k=k):
                off_forward(k).wait_send()

    def power_steps(read, write, degree, z0, z1, rows):
        r0, n = rows
        sums = {}

        def y_sum(z):
            if z not in sums:
                sums[z] = (
                    read(degree - 1, z, r0 - 1, n) + read(degree - 1, z, r0, n) + read(degree - 1, z, r0 + 1, n)
                )
            return sums[z]

        shared = None
        for z in range(z0, z1):
            if shared is None:
                shared = y_sum(z) + y_sum(z + 1)
                s0, s1 = x_sum(shared + y_sum(z - 1), n)
            else:
                s0, s1 = x_sum(shared + y_sum(z + 1), n)
                shared = None
            sums.pop(z - 1, None)
            mask = M[z, r0:r0 + n, :]
            box = jnp.stack([s0 * mask, s1 * mask])
            value = C[:, z, r0:r0 + n, :] * read(degree - 1, z, r0, n) - box
            if degree == 1:
                value = 0.5 * value
            else:
                value = value - read(degree - 2, z, r0, n)
            write(degree, z, r0, n, value)

    def reader(f, V):
        def read(degree, z, r, n):
            if degree == 0:
                return F[f, :, z, r:r + n, :]
            return V[degree - 1, :, z, r:r + n, :]
        return read

    def writer(V):
        def write(degree, z, r, n, value):
            V[degree - 1, :, z, r:r + n, :] = value
        return write

    read_p, read_r = reader(0, PV), reader(1, RV)
    write_p, write_r = writer(PV), writer(RV)

    def own(block, degree, xt):
        if degree == 0:
            return V0[block, xt]
        V = (PV, RV)[block]
        return V[degree - 1, xt, S:S + BZ, MID:MID + 8, :]

    lane8 = lax.broadcasted_iota(jnp.int32, (8, 128), 1)
    sub8 = lax.broadcasted_iota(jnp.int32, (8, 128), 0)

    def all_sublanes(v):
        v = v + pltpu.roll(v, 4, 0)
        v = v + pltpu.roll(v, 2, 0)
        return v + pltpu.roll(v, 1, 0)

    def exact_sum(pairs):
        while len(pairs) > 1:
            joined = []
            for (a, ea), (b, eb) in zip(pairs[::2], pairs[1::2]):
                t = a + b
                back = t - a
                err = (a - (t - back)) + (b - back)
                joined.append((t, err if ea is None else err + (ea + eb)))
            pairs = joined
        return pairs[0]

    def splat(v, j):
        return jnp.broadcast_to(v[j:j + 1, :], (8, 128))

    def by_row(values):
        out = jnp.zeros((8, 128), jnp.float32)
        for j, value in enumerate(values):
            if value:
                out = jnp.where(sub8 == j, value, out)
        return out

    diag_c = (by_row([CENTER] * S), by_row([CENTER] * (S - 1)))
    from_low = (by_row([0.0, HALF] + [0.5 * HALF] * (S - 1)), by_row([0.0, HALF] + [0.5 * HALF] * (S - 2)))
    from_high = (by_row([0.5 * HALF] * (S - 1)), by_row([0.5 * HALF] * (S - 2)))

    def combine(c, xt):
        total = None
        for block in range(2):
            for degree in range(S + 1 - block):
                half, row = place(degree + block * (S + 1))
                term = splat(c[half], row)[None] * own(block, degree, xt)
                total = term if total is None else total + term
        return total

    def outer(t, carry):
        par = t % 2
        @pl.when(t > 0)
        def _():
            for xt in range(2):
                X[xt] = X[xt] + combine([XC[h] for h in range(PARTS)], xt)
        exchange_finish()

        @pl.when(t == 0)
        def _():
            exchange_last()
            exchange_sent()
            for z in range(NZE):
                C[:, z, LO:HI + 8, :] = (2.0 / HALF) * (
                    F[1, :, z, LO:HI + 8, :] + (27.0 - CENTER)
                )
                F[1, :, z, LO:HI + 8, :] = F[0, :, z, LO:HI + 8, :]

        for f in range(2):
            V0[f] = F[f, :, S:S + BZ, MID:MID + 8, :]
        def early_rows(core, m):
            n = 8 * ((2 * m + 7) // 8)
            return (MID + m - n if core else MID + 8 - m, n)

        def late_rows(core, m):
            return (MID + m if core else MID - m, 8)

        def powers(rows, core, fields=(0, 1)):
            for degree in range(1, S + 1):
                for f in fields:
                    read, write = ((read_p, write_p), (read_r, write_r))[f]
                    m = S - f - degree
                    if m >= 0 and rows(core, m)[1]:
                        power_steps(read, write, degree, degree + f, NZE - degree - f, rows(core, m))

        for core in range(2):
            @pl.when((gx == core) & (t > 0))
            def _(core=core):
                powers(early_rows, core)
                exchange_last()
                powers(late_rows, core)

        @pl.when(t == 0)
        def _():
            for degree in range(1, S + 1):
                m = S - degree
                rows = (LO, 24) if m > 4 else (MID - 4, 16) if m else (MID, 8)
                power_steps(read_p, write_p, degree, degree, NZE - degree, rows)
            for degree in range(1, S):
                RV[degree - 1, :, S:S + BZ, MID:MID + 8, :] = PV[degree - 1, :, S:S + BZ, MID:MID + 8, :]

        parts = [None] * (NPP + NPR + NRR)

        def add(k, a, b):
            s = jnp.sum(a * b, axis=0)
            parts[k] = s if parts[k] is None else parts[k] + s

        for xt in range(2):
            p, r = own(0, 0, xt), own(1, 0, xt)
            for i in range(S + 1):
                p_next = own(0, i + 1, xt) if i < S else None
                r_next = own(1, i + 1, xt) if i < S - 1 else None
                add(2 * i, p, p)
                if i < S:
                    add(2 * i + 1, p, p_next)
                    add(NPP + 2 * i, p, r)
                    add(NPP + 2 * i + 1, p_next, r)
                    add(NPP + NPR + 2 * i, r, r)
                if i < S - 1:
                    add(NPP + NPR + 2 * i + 1, r, r_next)
                p, r = p_next, r_next
        picked = jnp.zeros((8, 128), jnp.float32)
        for k, part in enumerate(parts):
            picked = jnp.where(lane8 == k, jnp.sum(part, axis=1, keepdims=True), picked)
        local = jnp.sum(picked, axis=0, keepdims=True)

        me1 = 2 * pz + gx
        me2 = 4 * py + gy
        @pl.when(t > 0)
        def _():
            exchange_sent()
        S1[par, me1] = local
        for to in line:
            pltpu.make_async_remote_copy(
                src_ref=S1.at[par, me1], dst_ref=S1.at[par, me1],
                send_sem=g1_s.at[par], recv_sem=g1_r.at[par],
                device_id=to, device_id_type=MESH,
            ).start()
        whole1 = pltpu.make_async_copy(S1.at[par, pl.ds(0, 15)], S1.at[par, pl.ds(0, 15)], g1_r.at[par])
        whole1.wait()
        S2[par, me2] = jnp.concatenate(exact_sum([(S1[par, i], None) for i in range(16)]), axis=0)
        for to in plane:
            pltpu.make_async_remote_copy(
                src_ref=S2.at[par, me2], dst_ref=S2.at[par, me2],
                send_sem=g2_s.at[par], recv_sem=g2_r.at[par],
                device_id=to, device_id_type=MESH,
            ).start()
        whole2 = pltpu.make_async_copy(S2.at[par, pl.ds(0, 15)], S2.at[par, pl.ds(0, 15)], g2_r.at[par])
        whole2.wait()
        high, low = exact_sum([(S2[par, i, 0:1], S2[par, i, 1:2]) for i in range(16)])
        lead = high.astype(jnp.bfloat16).astype(jnp.float32)
        rest = (high - lead) + low
        lead, rest = jnp.broadcast_to(lead, (8, 128)), jnp.broadcast_to(rest, (8, 128))
        pltpu.make_async_copy(S1.at[par, pl.ds(0, 15)], S1.at[par, pl.ds(0, 15)], g1_s.at[par]).wait()
        pltpu.make_async_copy(S2.at[par, pl.ds(0, 15)], S2.at[par, pl.ds(0, 15)], g2_s.at[par]).wait()

        columns = 2 * S + 1

        def lanes(v):
            return jnp.broadcast_to(jnp.sum(v, axis=1, keepdims=True), (8, 128))

        table = [
            [lanes(w_ref[j, half] * lead) + lanes(w_ref[j, half] * rest) for half in range(PARTS)]
            for j in range(columns)
        ]

        def form(u, v, top_p, top_r):
            used = list(range(top_p + 1)) + [S + 1 + j for j in range(top_r + 1)]
            total = None
            for half in sorted({place(j)[0] for j in used}):
                terms = [table[j][half] * splat(v[place(j)[0]], place(j)[1]) for j in used]
                while len(terms) > 1:
                    terms = [
                        terms[i] + terms[i + 1] if i + 1 < len(terms) else terms[i] for i in range(0, len(terms), 2)
                    ]
                part = terms[0] * u[half]
                total = part if total is None else total + part
            return all_sublanes(total)

        unit = jnp.where(sub8 == 0, 1.0, 0.0)
        none = jnp.zeros((8, 128), jnp.float32)
        p_c, r_c, x_c = ([unit] + [none] * (PARTS - 1), [none, unit] + [none] * (PARTS - 2), [none] * PARTS)
        norm = form(r_c, r_c, -1, 0)
        for step in range(S):
            q = [
                diag_c[h] * p_c[h] + from_low[h] * pltpu.roll(p_c[h], 1, 0) + from_high[h] * pltpu.roll(p_c[h], 7, 0)
                for h in range(2)
            ]
            if PARTS == 3:
                q.append(jnp.where(sub8 == 0, 0.5 * HALF * splat(p_c[0], 7), 0.0))
            length = norm / form(p_c, q, step + 1, step)
            r_next = [r_c[h] - length * q[h] for h in range(PARTS)]
            norm_next = form(r_next, r_next, step + 1, min(step, S - 1))
            ratio = norm_next / norm
            new = (
                [x_c[h] + length * p_c[h] for h in range(PARTS)] + r_next
                + [r_next[h] + ratio * p_c[h] for h in range(PARTS)] + [norm_next]
            )
            count = sum(inner > step for inner in INNER)
            if count < len(INNER):
                keep = jnp.full((8, 128), t, jnp.int32) < count
                new = [jnp.where(keep, a, b) for a, b in zip(new, x_c + r_c + p_c + [norm])]
            x_c, r_c, p_c, norm = new[:PARTS], new[PARTS:2 * PARTS], new[2 * PARTS:3 * PARTS], new[-1]

        for xt in range(2):
            F[1, xt, S:S + BZ, MID:MID + 8, :] = combine(r_c, xt)

        @pl.when(t < len(INNER) - 1)
        def _():
            exchange_start(1)
            for xt in range(2):
                F[0, xt, S:S + BZ, MID:MID + 8, :] = combine(p_c, xt)
            exchange_start(0)
        for h in range(PARTS):
            XC[h] = x_c[h]
        return carry

    exchange_start(1)
    exchange_start(0)
    lax.fori_loop(0, len(INNER), outer, 0)

    def back(f, src):
        return pltpu.make_async_remote_copy(
            src_ref=src, dst_ref=land.at[f],
            send_sem=io_s.at[2 + f], recv_sem=io_r.at[2 + f],
            device_id=(gz, gy, sib), device_id_type=MESH,
        )

    (halves,) = reorder([[F[1, xt, S:S + BZ, MID:MID + 8, :] for xt in range(2)]], to_natural)
    for xt in range(2):
        F[1, xt, S:S + BZ, MID:MID + 8, :] = halves[xt]
    res_back = back(1, F.at[1, sib, own_z, own_rows, :])
    res_back.start()
    (halves,) = reorder([[X[xt] + combine([XC[h] for h in range(PARTS)], xt) for xt in range(2)]], to_natural)
    for xt in range(2):
        X[xt] = halves[xt]
    sol_back = back(0, X.at[sib])
    sol_back.start()
    res_ref[:, mine, :] = F[1, gx, S:S + BZ, MID:MID + 8, :]
    sol_ref[:, mine, :] = X[gx]
    for f, (cp, out) in enumerate(((sol_back, sol_ref), (res_back, res_ref))):
        cp.wait()
        out[:, other, :] = land[f]


def solution(mesh):
    table = weights()

    def local(right_side, diagonal):
        f32 = jnp.float32
        dma = pltpu.SemaphoreType.DMA
        field = (2, NZE, ROWS, 128)
        return pl.pallas_call(
            kernel,
            out_shape=(jax.ShapeDtypeStruct(right_side.shape, f32),) * 2,
            in_specs=[pl.BlockSpec(memory_space=pltpu.HBM)] * 3,
            out_specs=(pl.BlockSpec(memory_space=pltpu.VMEM),) * 2,
            scratch_shapes=[
                pltpu.VMEM((2,) + field, f32),
                pltpu.VMEM((S,) + field, f32),
                pltpu.VMEM((S - 1,) + field, f32),
                pltpu.VMEM(field, f32),
                pltpu.VMEM((NZE, ROWS, 128), f32),
                pltpu.VMEM((2, 2, BZ, 8, 128), f32),
                pltpu.VMEM((2, BZ, 8, 128), f32),
                pltpu.VMEM((PARTS, 8, 128), f32),
                pltpu.VMEM((2, BZ, 8, 128), f32),
                pltpu.VMEM((2, 16, 1, 128), f32),
                pltpu.VMEM((2, 16, 2, 128), f32),
                pltpu.VMEM(table.shape, f32),
                dma((5,)), dma((2, 2)), dma((2, 2)), dma((2, 2)), dma((2, 2)), dma((2, 2)), dma((2, 2)), dma((2, 2)), dma((2, 2)),
                dma((4,)), dma((4,)), dma((2,)), dma((2,)), dma((2,)), dma((2,)),
            ],
            compiler_params=pltpu.CompilerParams(collective_id=0, has_side_effects=True, vmem_limit_bytes=48 * 2**20),
        )(*(pltpu.with_memory_space_constraint(v, pltpu.HBM) for v in (right_side, diagonal, jnp.asarray(table))))

    spec = P("gz", "gy", "gx")
    return jax.shard_map(
        local, mesh=mesh, in_specs=(spec, spec), out_specs=(spec, spec), check_vma=False
    )
```
